32 devices in a mesh: left: 8 (over y, x, core), right: 4 (over z).
Axes of the slice: x: 2, y: 2, z: 4, core: 2. Of those that a mesh axis runs over, the one named last changes fastest.
Arguments:
- tracer: float32 [2, 1024, 256, 128], P(None, None, 'left', 'right'), may hold values from -6 to 6
- symbol_x: float32 [1024], replicated, may hold values from 0.3 to 3
- symbol_y: float32 [256], replicated, may hold values from 0.3 to 3
- symbol_z: float32 [128], replicated, may hold values from 0.3 to 3
Outputs:
- modes: float32 [2, 1024, 256, 128], P(None, 'left', 'right')
The draws below stay inside these ranges and needn't reach their ends.
All inputs are finite; a program needn't handle non-finite values.
Results may differ from the reference program's by a relative error of at most 0.00007.
Values sent between devices are 32-bit elements; how exact they have to be, the bound alone decides.
A program may use at most 256 MiB of HBM per device.

```python
import jax
import jax.numpy as jnp
from jax import lax

GRID_X = 1024
GRID_Y = 256
GRID_Z = 128
FIELDS = 2


def level_of(stream_key, extent, shards, least, largest):
    def one(position, parts):
        draws = jax.random.uniform(jax.random.fold_in(jax.random.fold_in(stream_key, 6), position), (parts,), jnp.float32, least / len(shards), largest / len(shards))
        return jnp.repeat(jnp.exp(draws), extent[position] // parts).reshape((-1,) + (1,) * (len(extent) - position - 1))

    gain = one(*shards[0])
    for cut in shards[1:]:
        gain = gain * one(*cut)
    return gain


def normal_values(own_key, extent, scale, reach, shards=(), dtype=jnp.bfloat16):
    loudness = level_of(own_key, extent, shards, -0.22, 0.18) if shards else 1.0
    entries = jax.random.normal(own_key, extent, jnp.float32) * scale * loudness
    return jnp.minimum(jnp.maximum(entries, -reach), reach).astype(dtype)


def setup_inputs(seed: int = 0) -> dict:
    splits = jax.random.split(jax.random.key(seed), 5)
    return {
        "tracer": normal_values(splits[0], (FIELDS, GRID_X, GRID_Y, GRID_Z), 1.0, 6.0, ((2, 8), (3, 4)), jnp.float32),
        "symbol_x": jnp.clip(jax.random.uniform(splits[1], (GRID_X,), jnp.float32, 0.3, 3.0), 0.3, 3.0),
        "symbol_y": jnp.clip(jax.random.uniform(splits[2], (GRID_Y,), jnp.float32, 0.3, 3.0), 0.3, 3.0),
        "symbol_z": jnp.clip(jax.random.uniform(splits[3], (GRID_Z,), jnp.float32, 0.3, 3.0), 0.3, 3.0),
    }


def transform_table(count):
    rank = jnp.arange(count)
    angle = 2.0 * jnp.pi / count * (rank[:, None] * rank[None, :] % count).astype(jnp.float32)
    return (jnp.cos(angle) + jnp.sin(angle)) * count ** (-0.5)

def transform_dim(values, dim):
    moved = jnp.tensordot(values, transform_table(values.shape[dim]), axes=([dim], [0]), precision=lax.Precision.HIGHEST)
    return jnp.moveaxis(moved, -1, dim)

def reference(tracer, symbol_x, symbol_y, symbol_z):
    modes = tracer
    modes = transform_dim(modes, 1)
    modes = transform_dim(modes, 2)
    modes = transform_dim(modes, 3)
    symbol = symbol_x[:, None, None] + symbol_y[None, :, None] + symbol_z[None, None, :]
    modes = modes * lax.rsqrt(symbol)
    return modes
```

```python
import functools
import math

import jax
import jax.numpy as jnp
import numpy as np
from jax import lax
from jax.experimental import pallas as pl
from jax.experimental.pallas import tpu as pltpu
from jax.sharding import PartitionSpec as P

MESH = pl.DeviceIdType.MESH
NEAR_BYTES = 20 * 2**20
DEPTH = 8
BAND = 16
LANES = 128
SLOTS = 3
NEAR_LIMIT = 50 * 2**20
SUB = 2
LAG = 2


def transform_table(count):
    inner = 1 << ((count.bit_length() - 1) // 2)
    outer = count // inner
    column = np.arange(count)

    def angle(row):
        return 2.0 * np.pi / count * (row[:, None] * column[None, :] % count)

    low = angle(np.arange(inner))
    high = angle(np.arange(outer) * inner)
    scale = count ** (-0.5)
    cos_low = jnp.asarray(np.cos(low), jnp.float32)[None]
    sin_low = jnp.asarray(np.sin(low), jnp.float32)[None]
    plus = jnp.asarray((np.cos(high) + np.sin(high)) * scale, jnp.float32)[:, None]
    minus = jnp.asarray((np.cos(high) - np.sin(high)) * scale, jnp.float32)[:, None]
    return (cos_low * plus + sin_low * minus).reshape(count, count)


def factors_of(count):
    inner = 1 << ((count.bit_length() - 1) // 2)
    outer = count // inner
    column = np.arange(count)

    def angle(row):
        return 2.0 * np.pi / count * (row[:, None] * column[None, :] % count)

    low = angle(np.arange(inner))
    high = angle(np.arange(outer) * inner)
    scale = count ** (-0.5)
    low = jnp.asarray(np.stack([np.cos(low), np.sin(low)]), jnp.float32)
    high = jnp.asarray(np.stack([np.cos(high) + np.sin(high), np.cos(high) - np.sin(high)]) * scale, jnp.float32)
    return low, high


def halves_of(table):
    upper = lax.reduce_precision(table, 8, 7)
    return jnp.stack([upper.astype(jnp.bfloat16), (table - upper).astype(jnp.bfloat16)])


def small_table(count):
    rank = np.arange(count)
    angle = 2.0 * np.pi / count * (rank[:, None] * rank[None, :] % count)
    table = ((np.cos(angle) + np.sin(angle)) * count ** (-0.5)).astype(np.float32)
    upper = table.astype(jnp.bfloat16)
    return jnp.asarray(np.stack([upper, (table - upper.astype(np.float32)).astype(jnp.bfloat16)]))


def split(values):
    upper = values.astype(jnp.bfloat16)
    return upper, (values - upper.astype(jnp.float32)).astype(jnp.bfloat16)


def product(a, b):
    dot = functools.partial(jnp.dot, preferred_element_type=jnp.float32)
    return dot(a[0], b[0]) + (dot(a[0], b[1]) + dot(a[1], b[0]))


def landed(ref, sem):
    pltpu.make_async_copy(ref, ref, sem).wait()


def far_kernel(lefts, rights, near, data, hx, hy, hz, base, sym_y, out, *rest):
    (first, second, dbuf, lines, send_a, send_b, obuf,
     d_sem, sa_sem, ra_sem, y_sem, sb_sem, rb_sem, z_sem, o_sem, *staging) = rest
    fields, share_y, share_z, _ = data.shape
    size_y, size_z = hy.shape[1], hz.shape[1]
    share_x = base.shape[0]
    bands = out.shape[1]
    pieces = share_z // DEPTH
    chunks = fields * pieces
    rows = share_y * DEPTH
    flat = DEPTH * BAND
    out_y = bands * BAND
    left, right = lax.axis_index("left"), lax.axis_index("right")

    def load(i):
        source = data.at[i // pieces, :, pl.ds(lax.rem(i, pieces) * DEPTH, DEPTH), :]
        return pltpu.make_async_copy(source, dbuf.at[lax.rem(i, 2)], d_sem.at[lax.rem(i, 2)])

    load(0).start()

    barrier = pltpu.get_barrier_semaphore()
    for k in range(1, lefts):
        pl.semaphore_signal(barrier, inc=1, device_id=(lax.rem(left + k, lefts), right), device_id_type=MESH)
    for k in range(1, rights):
        pl.semaphore_signal(barrier, inc=1, device_id=(left, lax.rem(right + k, rights)), device_id_type=MESH)
    pl.semaphore_wait(barrier, lefts + rights - 2)

    def copy_a(i, to):
        slot = lax.rem(i, SLOTS)
        return pltpu.make_async_remote_copy(
            src_ref=send_a.at[slot, to],
            dst_ref=first.at[i, pl.ds(left * rows, rows)],
            send_sem=sa_sem.at[slot, to],
            recv_sem=ra_sem.at[i, left],
            device_id=(to, right),
            device_id_type=MESH,
        )

    def copy_b(i, to, band):
        spot = right * share_z + lax.rem(i, pieces) * DEPTH
        return pltpu.make_async_remote_copy(
            src_ref=send_b.at[i, to, band],
            dst_ref=second.at[i // pieces, band, pl.ds(spot * BAND, flat)],
            send_sem=sb_sem.at[i, to, band],
            recv_sem=rb_sem.at[i, right, band],
            device_id=(left, to),
            device_id_type=MESH,
        )

    def sent_a(i):
        for k in range(1, lefts):
            copy_a(i, lax.rem(left + k, lefts)).wait_send()

    def x_step(i):
        load(i).wait()

        @pl.when(i + 1 < chunks)
        def _():
            load(i + 1).start()

        @pl.when(i >= SLOTS)
        def _():
            sent_a(i - SLOTS)

        slot = lax.rem(i, SLOTS)
        lines[0], lines[1] = split(dbuf[lax.rem(i, 2)].reshape(rows, hx.shape[1]))

        def tile(j, carry):
            cols = pl.ds(pl.multiple_of(j * 2 * share_x, 2 * share_x), 2 * share_x)
            got = product((lines[0], lines[1]), (hx[0, :, cols], hx[1, :, cols]))
            send_a[slot, 2 * j] = got[:, :share_x]
            send_a[slot, 2 * j + 1] = got[:, share_x:]
            return carry

        lax.fori_loop(0, lefts // 2, tile, 0)
        for k in range(1, lefts):
            copy_a(i, lax.rem(left + k, lefts)).start()
        pltpu.make_async_copy(
            send_a.at[slot, left], first.at[i, pl.ds(left * rows, rows)], ra_sem.at[i, left]
        ).start()

    def y_step(i):
        for k in range(lefts):
            landed(first.at[i, pl.ds(k * rows, rows)], ra_sem.at[i, k])
        if near:
            block = first.at[i]
        else:
            block = staging[0]
            fetch = pltpu.make_async_copy(first.at[i], block, y_sem)
            fetch.start()
            fetch.wait()
        for z in range(0, DEPTH, 2):
            pair = jnp.concatenate(
                [block[pl.ds(z, size_y, stride=DEPTH), :], block[pl.ds(z + 1, size_y, stride=DEPTH), :]], axis=1
            )
            got = product((hy[0], hy[1]), split(pair))
            for to in range(rights):
                for band in range(bands):
                    top = to * out_y + band * BAND
                    for half in range(2):
                        send_b[i, to, band, (z + half) * BAND:(z + half + 1) * BAND, :] = (
                            got[top:top + BAND, half * share_x:(half + 1) * share_x]
                        )
        for band in range(bands):
            for k in range(rights):
                to = jnp.where(right < rights // 2, rights - 1 - k, k)

                @pl.when(to != right)
                def _():
                    copy_b(i, to, band).start()

            spot = right * share_z + lax.rem(i, pieces) * DEPTH
            pltpu.make_async_copy(
                send_b.at[i, right, band],
                second.at[i // pieces, band, pl.ds(spot * BAND, flat)],
                rb_sem.at[i, right, band],
            ).start()

    def step(i, carry):
        @pl.when(i < chunks)
        def _():
            x_step(i)

        @pl.when(i >= 1)
        def _():
            y_step(i - 1)

        return carry

    lax.fori_loop(0, chunks + 1, step, 0)

    def put(n):
        slot = lax.rem(n, 2)
        return pltpu.make_async_copy(obuf.at[slot], out.at[n // bands, lax.rem(n, bands)], o_sem.at[slot])

    def z_step(n, carry):
        field, band = n // bands, lax.rem(n, bands)
        slot = lax.rem(n, 2)

        def arrive(p, carry):
            for k in range(rights):
                spot = k * share_z + p * DEPTH
                landed(second.at[field, band, pl.ds(spot * BAND, flat)], rb_sem.at[field * pieces + p, k, band])
            return carry

        lax.fori_loop(0, pieces, arrive, 0)
        if near:
            block = second.at[field, band]
        else:
            block = staging[1]
            fetch = pltpu.make_async_copy(second.at[field, band], block, z_sem)
            fetch.start()
            fetch.wait()

        @pl.when(n >= 2)
        def _():
            put(n - 2).wait()

        def line(y, carry):
            plane = block[pl.ds(y, size_z, stride=BAND), :].T
            got = product(split(plane), (hz[0], hz[1]))
            got = got * lax.rsqrt(base[...] + sym_y[right * out_y + band * BAND + y])
            for t in range(size_z // LANES):
                obuf[slot, t, pl.ds(y, share_x, stride=BAND), :] = got[:, t * LANES:(t + 1) * LANES]
            return carry

        lax.fori_loop(0, BAND, line, 0, unroll=2)
        put(n).start()
        return carry

    steps = fields * bands
    lax.fori_loop(0, steps, z_step, 0)

    def drain_a(i, carry):
        sent_a(i)
        return carry

    lax.fori_loop(max(chunks - SLOTS, 0), chunks, drain_a, 0)

    def drain_b(i, carry):
        for k in range(1, rights):
            for band in range(bands):
                copy_b(i, lax.rem(right + k, rights), band).wait_send()
        return carry

    lax.fori_loop(0, chunks, drain_b, 0)
    for n in range(max(steps - 2, 0), steps):
        put(n).wait()


def stacked(halves):
    upper, lower = halves[0], halves[1]
    return jnp.concatenate(
        [jnp.concatenate([upper, lower], axis=1), jnp.concatenate([upper, jnp.zeros_like(lower)], axis=1)], axis=0
    )


def near_kernel(lefts, rights, data, low_in, high_in, hy_in, hz_in, sym_x, sym_z, sym_y, out, *rest):
    (first, second, dbuf, low, high, hx, hy, hz, lines, send_a, send_b, base,
     d_sem, t_sem, sa_sem, ra_sem, sb_sem, rb_sem, sc_sem, rc_sem) = rest
    fields, share_y, share_z, size_x = data.shape
    size_y = hy.shape[1]
    share_x, size_z = base.shape
    bands = out.shape[1]
    pieces = share_z // DEPTH
    chunks = fields * pieces
    subs = DEPTH // SUB
    line_subs = pieces * subs
    out_y = bands * BAND
    half = rights // 2
    left, right = lax.axis_index("left"), lax.axis_index("right")

    def load(i):
        slot = lax.rem(i, 2)
        planes = pl.ds(lax.rem(i, pieces) * DEPTH, DEPTH)
        return [pltpu.make_async_copy(
            data.at[i // pieces, :, planes, pl.ds(c * LANES, LANES)],
            dbuf.at[slot, c].reshape(share_y, DEPTH, LANES),
            d_sem.at[slot, c],
        ) for c in range(size_x // LANES)]

    def fetch(i):
        for copy in load(i):
            copy.start()

    tables = [pltpu.make_async_copy(a, b, t_sem.at[n]) for n, (a, b) in enumerate(
        [(low_in, low), (high_in, high), (hy_in, hy), (hz_in, hz)])]
    tables[0].start()
    tables[1].start()
    fetch(0)
    tables[2].start()
    tables[3].start()

    barrier = pltpu.get_barrier_semaphore()
    for k in range(1, lefts):
        pl.semaphore_signal(barrier, inc=1, device_id=(lax.rem(left + k, lefts), right), device_id_type=MESH)
    for k in range(1, rights):
        pl.semaphore_signal(barrier, inc=1, device_id=(left, lax.rem(right + k, rights)), device_id_type=MESH)

    column = jnp.broadcast_to(sym_x[pl.ds(left, 1), :], (size_z, share_x)).T
    base[...] = column + sym_z[...]

    pl.semaphore_wait(barrier, lefts + rights - 2)

    def copy_a(i, sub, to):
        slot = lax.rem(i, SLOTS)
        return pltpu.make_async_remote_copy(
            src_ref=send_a.at[slot, to, pl.ds(sub * SUB, SUB)],
            dst_ref=first.at[i, pl.ds(sub * SUB, SUB), pl.ds(left * share_y, share_y), :],
            send_sem=sa_sem.at[slot, sub, to],
            recv_sem=ra_sem.at[i, sub, left],
            device_id=(to, right),
            device_id_type=MESH,
        )

    def copy_b(p, to):
        field, spot = p // line_subs, lax.rem(p, line_subs) * SUB
        return pltpu.make_async_remote_copy(
            src_ref=send_b.at[field, to, :, pl.ds(spot * BAND, SUB * BAND), :],
            dst_ref=second.at[field, :, pl.ds((right * share_z + spot) * BAND, SUB * BAND), :],
            send_sem=sb_sem.at[p, to],
            recv_sem=rb_sem.at[p, right],
            device_id=(left, to),
            device_id_type=MESH,
        )

    def copy_c(band, to):
        return pltpu.make_async_remote_copy(
            src_ref=send_b.at[fields - 1, to, band],
            dst_ref=second.at[fields - 1, band, pl.ds(right * share_z * BAND, share_z * BAND), :],
            send_sem=sc_sem.at[band, to],
            recv_sem=rc_sem.at[band, right],
            device_id=(left, to),
            device_id_type=MESH,
        )

    lower = right < half
    rank = jnp.where(lower, right, rights - 1 - right)
    end = rank == 0

    def mirrored(t):
        return jnp.where(lower, t, rights - 1 - t)

    def crossing(k):
        return mirrored(jnp.where(end, rights - 1 - k, half + k))

    def beside(k):
        return mirrored(lax.rem(rank + 1 + k, half))

    def sent_a(i):
        for sub in range(subs):
            for k in range(1, lefts):
                copy_a(i, sub, lax.rem(left + k, lefts)).wait_send()

    def widen(cols):
        for top in range(size_x // low.shape[1]):
            made = low[0, :, cols] * high[0, top:top + 1, cols] + low[1, :, cols] * high[1, top:top + 1, cols]
            rows = pl.ds(top * low.shape[1], low.shape[1])
            hx[0, rows, cols], hx[1, rows, cols] = split(made)

    def x_step(i, opening):
        slot = lax.rem(i, SLOTS)
        for copy in load(i):
            copy.wait()

        if not opening:
            @pl.when(i >= SLOTS)
            def _():
                sent_a(i - SLOTS)

        here = dbuf.at[lax.rem(i, 2)]
        for c in range(size_x // LANES):
            cols = pl.ds(c * LANES, LANES)
            for z in range(DEPTH):
                rows = pl.ds(z * share_y, share_y)
                lines[0, rows, cols], lines[1, rows, cols] = split(here[c, pl.ds(z, share_y, stride=DEPTH), :])

        @pl.when(i + 2 < chunks)
        def _():
            fetch(i + 2)

        def tile(j, carry):
            pair = left // 2 ^ (lefts // 2 - 1 - j) if lefts & (lefts - 1) == 0 else j
            cols = pl.ds(pl.multiple_of(pair * 2 * share_x, 2 * share_x), 2 * share_x)
            if opening:
                widen(cols)
            got = product((lines[0], lines[1]), (hx[0, :, cols], hx[1, :, cols]))
            for core in range(2):
                to = 2 * pair + core
                send_a[slot, to] = got[:, core * share_x:(core + 1) * share_x].reshape(DEPTH, share_y, share_x)

                @pl.when(to != left)
                def _():
                    copy_a(i, 0, to).start()
            return carry

        lax.fori_loop(0, lefts // 2, tile, 0)
        for sub in range(1, subs):
            for k in range(lefts - 1, 0, -1):
                copy_a(i, sub, left ^ k if lefts & (lefts - 1) == 0 else lax.rem(left + k, lefts)).start()
        first[i, :, pl.ds(pl.multiple_of(left * share_y, share_y), share_y), :] = send_a[slot, left]

    def y_step(i, sub, p):
        for k in range(1, lefts):
            who = lax.rem(left + k, lefts)
            landed(first.at[i, pl.ds(sub * SUB, SUB), pl.ds(who * share_y, share_y), :], ra_sem.at[i, sub, who])
        field = i // pieces
        for z in range(0, SUB, 2):
            pair = jnp.concatenate([first[i, sub * SUB + z], first[i, sub * SUB + z + 1]], axis=1)
            got = product((hy[0], hy[1]), split(pair))
            spot = (lax.rem(i, pieces) * DEPTH + sub * SUB + z) * BAND
            for to in range(rights):
                for band in range(bands):
                    top = to * out_y + band * BAND
                    for side in range(2):
                        rows = pl.ds(pl.multiple_of(spot + side * BAND, BAND), BAND)
                        send_b[field, to, band, rows, :] = got[top:top + BAND, side * share_x:(side + 1) * share_x]
        for k in range(half):
            @pl.when(jnp.logical_not(end))
            def _():
                copy_b(p, crossing(k)).start()
        for k in range(half - 1):
            copy_b(p, beside(k)).start()
        spot = (lax.rem(i, pieces) * DEPTH + sub * SUB) * BAND
        for band in range(bands):
            mine = send_b[field, right, band, pl.ds(pl.multiple_of(spot, BAND), SUB * BAND), :]
            there = pl.multiple_of(right * share_z * BAND + spot, BAND)
            second[field, band, pl.ds(there, SUB * BAND), :] = mine

    held = (fields - 1) * line_subs

    def late(q):
        for k in range(half):
            copy_b(q, crossing(k)).start()

    fetch(1)
    tables[0].wait()
    tables[1].wait()
    x_step(0, True)

    def step(i, carry):
        @pl.when(i + 1 < chunks)
        def _():
            x_step(i + 1, False)

        @pl.when(i == 0)
        def _():
            tables[2].wait()
            tables[3].wait()

        def part(sub, carry):
            p = i * subs + sub
            y_step(i, sub, p)

            @pl.when(jnp.logical_and(end, jnp.logical_and(lax.rem(p, LAG) == 0, p // LAG < held)))
            def _():
                late(p // LAG)

            return carry

        lax.fori_loop(0, subs, part, 0)
        return carry

    lax.fori_loop(0, chunks, step, 0)

    @pl.when(end)
    def _():
        def more(q, carry):
            late(q)
            return carry

        lax.fori_loop(min((chunks * subs + LAG - 1) // LAG, held), held, more, 0)
        for band in range(bands):
            for k in range(half):
                copy_c(band, crossing(k)).start()

    def by_band(who):
        if who not in (0, rights - 1):
            return False
        return right >= half if who < half else right < half

    def arrive(p, carry):
        for who in range(rights):
            awaited = right != who
            if by_band(who) is not False:
                awaited = jnp.logical_and(awaited, jnp.logical_not(jnp.logical_and(by_band(who), p >= held)))

            @pl.when(awaited)
            def _():
                field, spot = p // line_subs, lax.rem(p, line_subs) * SUB
                ref = second.at[field, :, pl.ds((who * share_z + spot) * BAND, SUB * BAND), :]
                landed(ref, rb_sem.at[p, who])
        return carry

    def z_step(n, carry):
        field, band = n // bands, lax.rem(n, bands)

        @pl.when(band == 0)
        def _():
            lax.fori_loop(field * line_subs, (field + 1) * line_subs, arrive, 0)

        @pl.when(field == fields - 1)
        def _():
            for who in (0, rights - 1):
                @pl.when(by_band(who))
                def _():
                    ref = second.at[field, band, pl.ds(who * share_z * BAND, share_z * BAND), :]
                    landed(ref, rc_sem.at[band, who])

        table = hz[...]

        def line(y, carry):
            plane = second[field, band, pl.ds(y, size_z, stride=BAND), :].T
            got = jnp.dot(jnp.concatenate(split(plane), axis=1), table, preferred_element_type=jnp.float32)
            got = (got[:, :size_z] + got[:, size_z:]) * lax.rsqrt(base[...] + sym_y[right * out_y + band * BAND + y])
            out[field, band, pl.ds(y, share_x, stride=BAND), :] = got
            return carry

        lax.fori_loop(0, BAND, line, 0, unroll=4)
        return carry

    lax.fori_loop(0, fields * bands, z_step, 0)

    def drain_a(i, carry):
        sent_a(i)
        return carry

    lax.fori_loop(max(chunks - SLOTS, 0), chunks, drain_a, 0)

    def drain_b(p, carry):
        for k in range(half - 1):
            copy_b(p, beside(k)).wait_send()

        @pl.when(jnp.logical_or(jnp.logical_not(end), p < held))
        def _():
            for k in range(half):
                copy_b(p, crossing(k)).wait_send()

        return carry

    lax.fori_loop(0, chunks * subs, drain_b, 0)

    @pl.when(end)
    def _():
        for band in range(bands):
            for k in range(half):
                copy_c(band, crossing(k)).wait_send()


def flush_kernel(ready, out, sem):
    fields, bands = ready.shape[:2]
    copies = []
    for n in range(fields * bands):
        field, band = n // bands, n % bands
        there = out.at[field, :, pl.ds(band * BAND, BAND), :]
        copies.append(pltpu.make_async_copy(ready.at[field, band], there, sem.at[n]))
    for copy in copies:
        copy.start()
    for copy in copies:
        copy.wait()


def near_local(lefts, rights, tracer, symbol_x, symbol_y, symbol_z):
    fields, size_x, share_y, share_z = tracer.shape
    size_y, size_z = symbol_y.shape[0], symbol_z.shape[0]
    share_x, out_y = size_x // lefts, size_y // rights
    bands = out_y // BAND
    chunks = fields * (share_z // DEPTH)
    parts = chunks * (DEPTH // SUB)
    data = jnp.transpose(tracer, (0, 2, 3, 1))
    low, high = factors_of(size_x)
    hy, hz = small_table(size_y), stacked(small_table(size_z))
    f32, bf16 = jnp.float32, jnp.bfloat16
    any_space = pl.BlockSpec(memory_space=pl.ANY)
    vmem = pl.BlockSpec(memory_space=pltpu.VMEM)
    dma = pltpu.SemaphoreType.DMA
    ready = pl.pallas_call(
        functools.partial(near_kernel, lefts, rights),
        name="modes",
        out_shape=pltpu.VMEM((fields, bands, share_x * BAND, size_z), f32),
        in_specs=[*[any_space] * 5, vmem, vmem, pl.BlockSpec(memory_space=pltpu.SMEM)],
        out_specs=vmem,
        scratch_shapes=[
            pltpu.VMEM((chunks, DEPTH, size_y, share_x), f32),
            pltpu.VMEM((fields, bands, size_z * BAND, share_x), f32),
            pltpu.VMEM((2, size_x // LANES, share_y * DEPTH, LANES), f32),
            pltpu.VMEM(low.shape, f32),
            pltpu.VMEM(high.shape, f32),
            pltpu.VMEM((2, size_x, size_x), bf16),
            pltpu.VMEM(hy.shape, bf16),
            pltpu.VMEM(hz.shape, bf16),
            pltpu.VMEM((2, share_y * DEPTH, size_x), bf16),
            pltpu.VMEM((SLOTS, lefts, DEPTH, share_y, share_x), f32),
            pltpu.VMEM((fields, rights, bands, share_z * BAND, share_x), f32),
            pltpu.VMEM((share_x, size_z), f32),
            dma((2, size_x // LANES)),
            dma((4,)),
            dma((SLOTS, DEPTH // SUB, lefts)),
            dma((chunks, DEPTH // SUB, lefts)),
            dma((parts, rights)),
            dma((parts, rights)),
            dma((bands, rights)),
            dma((bands, rights)),
        ],
        compiler_params=pltpu.CompilerParams(
            collective_id=0, has_side_effects=True, vmem_limit_bytes=NEAR_LIMIT
        ),
    )(data, low, high, hy, hz, symbol_x.reshape(lefts, share_x), symbol_z.reshape(1, size_z), symbol_y)
    return pl.pallas_call(
        flush_kernel,
        name="flush",
        out_shape=jax.ShapeDtypeStruct((fields, share_x, out_y, size_z), f32),
        in_specs=[vmem],
        out_specs=any_space,
        scratch_shapes=[dma((fields * bands,))],
        compiler_params=pltpu.CompilerParams(vmem_limit_bytes=2**21),
    )(ready.reshape(fields, bands, share_x, BAND, size_z))


def far_local(lefts, rights, tracer, symbol_x, symbol_y, symbol_z):
    fields, size_x, share_y, share_z = tracer.shape
    size_y, size_z = symbol_y.shape[0], symbol_z.shape[0]
    share_x, out_y = size_x // lefts, size_y // rights
    bands = out_y // BAND
    chunks = fields * (share_z // DEPTH)
    data = jnp.transpose(tracer, (0, 2, 3, 1))
    part_x = lax.dynamic_slice_in_dim(symbol_x, lax.axis_index("left") * share_x, share_x)
    base = part_x[:, None] + symbol_z[None, :]
    f32 = jnp.float32
    any_space = pl.BlockSpec(memory_space=pl.ANY)
    vmem = pl.BlockSpec(memory_space=pltpu.VMEM)
    landing = [(chunks, size_y * DEPTH, share_x), (fields, bands, size_z * BAND, share_x)]
    near = 4 * sum(map(math.prod, landing)) <= NEAR_BYTES
    staging = [] if near else [
        pltpu.VMEM((size_y * DEPTH, share_x), f32), pltpu.VMEM((size_z * BAND, share_x), f32)
    ]
    results = pl.pallas_call(
        functools.partial(far_kernel, lefts, rights, near),
        name="modes",
        out_shape=[
            jax.ShapeDtypeStruct((fields, bands, size_z // LANES, share_x * BAND, LANES), f32),
            *([] if near else [jax.ShapeDtypeStruct(shape, f32) for shape in landing]),
        ],
        in_specs=[any_space, vmem, vmem, vmem, vmem, pl.BlockSpec(memory_space=pltpu.SMEM)],
        out_specs=[any_space] * (1 if near else 3),
        scratch_shapes=[
            *([pltpu.VMEM(shape, f32) for shape in landing] if near else []),
            pltpu.VMEM((2, share_y, DEPTH, size_x), f32),
            pltpu.VMEM((2, share_y * DEPTH, size_x), jnp.bfloat16),
            pltpu.VMEM((SLOTS, lefts, share_y * DEPTH, share_x), f32),
            pltpu.VMEM((chunks, rights, bands, DEPTH * BAND, share_x), f32),
            pltpu.VMEM((2, size_z // LANES, share_x * BAND, LANES), f32),
            pltpu.SemaphoreType.DMA((2,)),
            pltpu.SemaphoreType.DMA((SLOTS, lefts)),
            pltpu.SemaphoreType.DMA((chunks, lefts)),
            pltpu.SemaphoreType.DMA,
            pltpu.SemaphoreType.DMA((chunks, rights, bands)),
            pltpu.SemaphoreType.DMA((chunks, rights, bands)),
            pltpu.SemaphoreType.DMA,
            pltpu.SemaphoreType.DMA((2,)),
            *staging,
        ],
        compiler_params=pltpu.CompilerParams(
            collective_id=0, has_side_effects=True, vmem_limit_bytes=60 * 2**20
        ),
    )(data, halves_of(transform_table(size_x)), small_table(size_y), small_table(size_z), base, symbol_y)
    out = results[0].reshape(fields, bands, size_z // LANES, share_x, BAND, LANES)
    return jnp.transpose(out, (0, 3, 1, 4, 2, 5)).reshape(fields, share_x, out_y, size_z)


def local(lefts, rights, tracer, symbol_x, symbol_y, symbol_z):
    fields, size_x, share_y, share_z = tracer.shape
    size_z, share_x = symbol_z.shape[0], size_x // lefts
    size = 4 * math.prod(tracer.shape)
    fits = size <= NEAR_BYTES // 2 and share_x == LANES and size_z == LANES and rights % 2 == 0
    run = near_local if fits else far_local
    return run(lefts, rights, tracer, symbol_x, symbol_y, symbol_z)


def solution(mesh):
    return jax.shard_map(
        functools.partial(local, mesh.shape["left"], mesh.shape["right"]),
        mesh=mesh,
        in_specs=(P(None, None, "left", "right"), P(), P(), P()),
        out_specs=P(None, "left", "right", None),
        check_vma=False,
    )
```

```python
import functools
import math

import jax
import jax.numpy as jnp
import numpy as np
from jax import lax
from jax.experimental import pallas as pl
from jax.experimental.pallas import tpu as pltpu
from jax.sharding import PartitionSpec as P

MESH = pl.DeviceIdType.MESH
NEAR_BYTES = 20 * 2**20
DEPTH = 8
BAND = 16
LANES = 128
SLOTS = 3
NEAR_LIMIT = 50 * 2**20
SUB = 2


def transform_table(count):
    inner = 1 << ((count.bit_length() - 1) // 2)
    outer = count // inner
    column = np.arange(count)

    def angle(row):
        return 2.0 * np.pi / count * (row[:, None] * column[None, :] % count)

    low = angle(np.arange(inner))
    high = angle(np.arange(outer) * inner)
    scale = count ** (-0.5)
    cos_low = jnp.asarray(np.cos(low), jnp.float32)[None]
    sin_low = jnp.asarray(np.sin(low), jnp.float32)[None]
    plus = jnp.asarray((np.cos(high) + np.sin(high)) * scale, jnp.float32)[:, None]
    minus = jnp.asarray((np.cos(high) - np.sin(high)) * scale, jnp.float32)[:, None]
    return (cos_low * plus + sin_low * minus).reshape(count, count)


def factors_of(count):
    inner = 1 << ((count.bit_length() - 1) // 2)
    outer = count // inner
    column = np.arange(count)

    def angle(row):
        return 2.0 * np.pi / count * (row[:, None] * column[None, :] % count)

    low = angle(np.arange(inner))
    high = angle(np.arange(outer) * inner)
    scale = count ** (-0.5)
    low = jnp.asarray(np.stack([np.cos(low), np.sin(low)]), jnp.float32)
    high = jnp.asarray(np.stack([np.cos(high) + np.sin(high), np.cos(high) - np.sin(high)]) * scale, jnp.float32)
    return low, high


def halves_of(table):
    upper = lax.reduce_precision(table, 8, 7)
    return jnp.stack([upper.astype(jnp.bfloat16), (table - upper).astype(jnp.bfloat16)])


def small_table(count):
    rank = np.arange(count)
    angle = 2.0 * np.pi / count * (rank[:, None] * rank[None, :] % count)
    table = ((np.cos(angle) + np.sin(angle)) * count ** (-0.5)).astype(np.float32)
    upper = table.astype(jnp.bfloat16)
    return jnp.asarray(np.stack([upper, (table - upper.astype(np.float32)).astype(jnp.bfloat16)]))


def split(values):
    upper = values.astype(jnp.bfloat16)
    return upper, (values - upper.astype(jnp.float32)).astype(jnp.bfloat16)


def product(a, b):
    dot = functools.partial(jnp.dot, preferred_element_type=jnp.float32)
    return dot(a[0], b[0]) + (dot(a[0], b[1]) + dot(a[1], b[0]))


def landed(ref, sem):
    pltpu.make_async_copy(ref, ref, sem).wait()


def far_kernel(lefts, rights, near, data, hx, hy, hz, base, sym_y, out, *rest):
    (first, second, dbuf, lines, send_a, send_b, obuf,
     d_sem, sa_sem, ra_sem, y_sem, sb_sem, rb_sem, z_sem, o_sem, *staging) = rest
    fields, share_y, share_z, _ = data.shape
    size_y, size_z = hy.shape[1], hz.shape[1]
    share_x = base.shape[0]
    bands = out.shape[1]
    pieces = share_z // DEPTH
    chunks = fields * pieces
    rows = share_y * DEPTH
    flat = DEPTH * BAND
    out_y = bands * BAND
    left, right = lax.axis_index("left"), lax.axis_index("right")

    def load(i):
        source = data.at[i // pieces, :, pl.ds(lax.rem(i, pieces) * DEPTH, DEPTH), :]
        return pltpu.make_async_copy(source, dbuf.at[lax.rem(i, 2)], d_sem.at[lax.rem(i, 2)])

    load(0).start()

    barrier = pltpu.get_barrier_semaphore()
    for k in range(1, lefts):
        pl.semaphore_signal(barrier, inc=1, device_id=(lax.rem(left + k, lefts), right), device_id_type=MESH)
    for k in range(1, rights):
        pl.semaphore_signal(barrier, inc=1, device_id=(left, lax.rem(right + k, rights)), device_id_type=MESH)
    pl.semaphore_wait(barrier, lefts + rights - 2)

    def copy_a(i, to):
        slot = lax.rem(i, SLOTS)
        return pltpu.make_async_remote_copy(
            src_ref=send_a.at[slot, to],
            dst_ref=first.at[i, pl.ds(left * rows, rows)],
            send_sem=sa_sem.at[slot, to],
            recv_sem=ra_sem.at[i, left],
            device_id=(to, right),
            device_id_type=MESH,
        )

    def copy_b(i, to, band):
        spot = right * share_z + lax.rem(i, pieces) * DEPTH
        return pltpu.make_async_remote_copy(
            src_ref=send_b.at[i, to, band],
            dst_ref=second.at[i // pieces, band, pl.ds(spot * BAND, flat)],
            send_sem=sb_sem.at[i, to, band],
            recv_sem=rb_sem.at[i, right, band],
            device_id=(left, to),
            device_id_type=MESH,
        )

    def sent_a(i):
        for k in range(1, lefts):
            copy_a(i, lax.rem(left + k, lefts)).wait_send()

    def x_step(i):
        load(i).wait()

        @pl.when(i + 1 < chunks)
        def _():
            load(i + 1).start()

        @pl.when(i >= SLOTS)
        def _():
            sent_a(i - SLOTS)

        slot = lax.rem(i, SLOTS)
        lines[0], lines[1] = split(dbuf[lax.rem(i, 2)].reshape(rows, hx.shape[1]))

        def tile(j, carry):
            cols = pl.ds(pl.multiple_of(j * 2 * share_x, 2 * share_x), 2 * share_x)
            got = product((lines[0], lines[1]), (hx[0, :, cols], hx[1, :, cols]))
            send_a[slot, 2 * j] = got[:, :share_x]
            send_a[slot, 2 * j + 1] = got[:, share_x:]
            return carry

        lax.fori_loop(0, lefts // 2, tile, 0)
        for k in range(1, lefts):
            copy_a(i, lax.rem(left + k, lefts)).start()
        pltpu.make_async_copy(
            send_a.at[slot, left], first.at[i, pl.ds(left * rows, rows)], ra_sem.at[i, left]
        ).start()

    def y_step(i):
        for k in range(lefts):
            landed(first.at[i, pl.ds(k * rows, rows)], ra_sem.at[i, k])
        if near:
            block = first.at[i]
        else:
            block = staging[0]
            fetch = pltpu.make_async_copy(first.at[i], block, y_sem)
            fetch.start()
            fetch.wait()
        for z in range(0, DEPTH, 2):
            pair = jnp.concatenate(
                [block[pl.ds(z, size_y, stride=DEPTH), :], block[pl.ds(z + 1, size_y, stride=DEPTH), :]], axis=1
            )
            got = product((hy[0], hy[1]), split(pair))
            for to in range(rights):
                for band in range(bands):
                    top = to * out_y + band * BAND
                    for half in range(2):
                        send_b[i, to, band, (z + half) * BAND:(z + half + 1) * BAND, :] = (
                            got[top:top + BAND, half * share_x:(half + 1) * share_x]
                        )
        for band in range(bands):
            for k in range(rights):
                to = jnp.where(right < rights // 2, rights - 1 - k, k)

                @pl.when(to != right)
                def _():
                    copy_b(i, to, band).start()

            spot = right * share_z + lax.rem(i, pieces) * DEPTH
            pltpu.make_async_copy(
                send_b.at[i, right, band],
                second.at[i // pieces, band, pl.ds(spot * BAND, flat)],
                rb_sem.at[i, right, band],
            ).start()

    def step(i, carry):
        @pl.when(i < chunks)
        def _():
            x_step(i)

        @pl.when(i >= 1)
        def _():
            y_step(i - 1)

        return carry

    lax.fori_loop(0, chunks + 1, step, 0)

    def put(n):
        slot = lax.rem(n, 2)
        return pltpu.make_async_copy(obuf.at[slot], out.at[n // bands, lax.rem(n, bands)], o_sem.at[slot])

    def z_step(n, carry):
        field, band = n // bands, lax.rem(n, bands)
        slot = lax.rem(n, 2)

        def arrive(p, carry):
            for k in range(rights):
                spot = k * share_z + p * DEPTH
                landed(second.at[field, band, pl.ds(spot * BAND, flat)], rb_sem.at[field * pieces + p, k, band])
            return carry

        lax.fori_loop(0, pieces, arrive, 0)
        if near:
            block = second.at[field, band]
        else:
            block = staging[1]
            fetch = pltpu.make_async_copy(second.at[field, band], block, z_sem)
            fetch.start()
            fetch.wait()

        @pl.when(n >= 2)
        def _():
            put(n - 2).wait()

        def line(y, carry):
            plane = block[pl.ds(y, size_z, stride=BAND), :].T
            got = product(split(plane), (hz[0], hz[1]))
            got = got * lax.rsqrt(base[...] + sym_y[right * out_y + band * BAND + y])
            for t in range(size_z // LANES):
                obuf[slot, t, pl.ds(y, share_x, stride=BAND), :] = got[:, t * LANES:(t + 1) * LANES]
            return carry

        lax.fori_loop(0, BAND, line, 0, unroll=2)
        put(n).start()
        return carry

    steps = fields * bands
    lax.fori_loop(0, steps, z_step, 0)

    def drain_a(i, carry):
        sent_a(i)
        return carry

    lax.fori_loop(max(chunks - SLOTS, 0), chunks, drain_a, 0)

    def drain_b(i, carry):
        for k in range(1, rights):
            for band in range(bands):
                copy_b(i, lax.rem(right + k, rights), band).wait_send()
        return carry

    lax.fori_loop(0, chunks, drain_b, 0)
    for n in range(max(steps - 2, 0), steps):
        put(n).wait()


def stacked(halves):
    upper, lower = halves[0], halves[1]
    return jnp.concatenate(
        [jnp.concatenate([upper, lower], axis=1), jnp.concatenate([upper, jnp.zeros_like(lower)], axis=1)], axis=0
    )


def near_kernel(lefts, rights, data, low_in, high_in, hy_in, hz_in, sym_x, sym_z, sym_y, out, *rest):
    (first, second, dbuf, low, high, hx, hy, hz, lines, send_a, send_b, base,
     d_sem, t_sem, sa_sem, ra_sem, sb_sem, rb_sem, rc_sem) = rest
    fields, share_y, share_z, size_x = data.shape
    size_y = hy.shape[1]
    share_x, size_z = base.shape
    bands = out.shape[1]
    pieces = share_z // DEPTH
    chunks = fields * pieces
    subs = DEPTH // SUB
    line_subs = pieces * subs
    out_y = bands * BAND
    half = rights // 2
    left, right = lax.axis_index("left"), lax.axis_index("right")

    def load(i):
        slot = lax.rem(i, 2)
        planes = pl.ds(lax.rem(i, pieces) * DEPTH, DEPTH)
        return [pltpu.make_async_copy(
            data.at[i // pieces, :, planes, pl.ds(c * LANES, LANES)],
            dbuf.at[slot, c].reshape(share_y, DEPTH, LANES),
            d_sem.at[slot],
        ) for c in range(size_x // LANES)]

    def fetch(i):
        for copy in load(i):
            copy.start()

    tables = [pltpu.make_async_copy(a, b, t_sem.at[n]) for n, (a, b) in enumerate(
        [(low_in, low), (high_in, high), (hy_in, hy), (hz_in, hz)])]
    tables[0].start()
    tables[1].start()
    fetch(0)
    tables[2].start()
    tables[3].start()

    barrier = pltpu.get_barrier_semaphore()
    for k in range(1, lefts):
        pl.semaphore_signal(barrier, inc=1, device_id=(lax.rem(left + k, lefts), right), device_id_type=MESH)
    for k in range(1, rights):
        pl.semaphore_signal(barrier, inc=1, device_id=(left, lax.rem(right + k, rights)), device_id_type=MESH)

    column = jnp.broadcast_to(sym_x[pl.ds(left, 1), :], (size_z, share_x)).T
    base[...] = column + sym_z[...]

    def copy_a(i, sub, to):
        return pltpu.make_async_remote_copy(
            src_ref=send_a.at[i, to, pl.ds(sub * SUB, SUB)],
            dst_ref=first.at[i, pl.ds(sub * SUB, SUB), pl.ds(left * share_y, share_y), :],
            send_sem=sa_sem,
            recv_sem=ra_sem.at[i, sub],
            device_id=(to, right),
            device_id_type=MESH,
        )

    def copy_b(p, to):
        field, spot = p // line_subs, lax.rem(p, line_subs) * SUB
        return pltpu.make_async_remote_copy(
            src_ref=send_b.at[field, to, :, pl.ds(spot * BAND, SUB * BAND), :],
            dst_ref=second.at[field, :, pl.ds((right * share_z + spot) * BAND, SUB * BAND), :],
            send_sem=sb_sem,
            recv_sem=rb_sem.at[field],
            device_id=(left, to),
            device_id_type=MESH,
        )

    def copy_c(band, to):
        return pltpu.make_async_remote_copy(
            src_ref=send_b.at[fields - 1, to, band],
            dst_ref=second.at[fields - 1, band, pl.ds(right * share_z * BAND, share_z * BAND), :],
            send_sem=sb_sem,
            recv_sem=rc_sem.at[band],
            device_id=(left, to),
            device_id_type=MESH,
        )

    held = (fields - 1) * line_subs
    lower = right < half
    rank = jnp.where(lower, right, rights - 1 - right)
    end = rank == 0

    def mirrored(t):
        return jnp.where(lower, t, rights - 1 - t)

    def crossing(k):
        return mirrored(jnp.where(end, rights - 1 - k, half + k))

    def beside(k):
        return mirrored(lax.rem(rank + 1 + k, half))

    def widen(cols):
        for top in range(size_x // low.shape[1]):
            made = low[0, :, cols] * high[0, top:top + 1, cols] + low[1, :, cols] * high[1, top:top + 1, cols]
            rows = pl.ds(top * low.shape[1], low.shape[1])
            hx[0, rows, cols], hx[1, rows, cols] = split(made)

    def partner(k):
        return left ^ k if lefts & (lefts - 1) == 0 else lax.rem(left + k, lefts)

    def x_tile(i, j, opening):
        pair = partner(lefts - 1 - 2 * j) // 2
        cols = pl.ds(pl.multiple_of(pair * 2 * share_x, 2 * share_x), 2 * share_x)
        if opening:
            widen(cols)
        got = product((lines[0], lines[1]), (hx[0, :, cols], hx[1, :, cols]))
        for core in range(2):
            send_a[i, 2 * pair + core] = got[:, core * share_x:(core + 1) * share_x].reshape(DEPTH, share_y, share_x)
        return pair

    def x_send(i, pair):
        for core in range(2):
            @pl.when(2 * pair + core != left)
            def _():
                copy_a(i, 0, 2 * pair + core).start()

    def x_step(i, opening):
        slot = lax.rem(i, 2)
        landed(dbuf.at[slot], d_sem.at[slot])
        for c in range(size_x // LANES):
            cols = pl.ds(c * LANES, LANES)
            for z in range(DEPTH):
                rows = pl.ds(z * share_y, share_y)
                lines[0, rows, cols], lines[1, rows, cols] = split(dbuf[slot, c, pl.ds(z, share_y, stride=DEPTH), :])

        @pl.when(i + 2 < chunks)
        def _():
            fetch(i + 2)

        if opening:
            pair = x_tile(i, 0, True)
            pl.semaphore_wait(barrier, lefts + rights - 2)
            x_send(i, pair)

        def tile(j, carry):
            x_send(i, x_tile(i, j, opening))
            return carry

        lax.fori_loop(1 if opening else 0, lefts // 2, tile, 0)
        for sub in range(1, subs):
            for k in range(lefts - 1, 0, -1):
                copy_a(i, sub, partner(k)).start()
        first[i, :, pl.ds(pl.multiple_of(left * share_y, share_y), share_y), :] = send_a[i, left]

    def y_step(i, sub, p):
        landed(first.at[i, pl.ds(sub * SUB, SUB), pl.ds(0, (lefts - 1) * share_y), :], ra_sem.at[i, sub])
        field = i // pieces
        for z in range(0, SUB, 2):
            pair = jnp.concatenate([first[i, sub * SUB + z], first[i, sub * SUB + z + 1]], axis=1)
            got = product((hy[0], hy[1]), split(pair))
            spot = (lax.rem(i, pieces) * DEPTH + sub * SUB + z) * BAND
            for to in range(rights):
                for band in range(bands):
                    top = to * out_y + band * BAND
                    for side in range(2):
                        rows = pl.ds(pl.multiple_of(spot + side * BAND, BAND), BAND)
                        send_b[field, to, band, rows, :] = got[top:top + BAND, side * share_x:(side + 1) * share_x]
        for k in range(half):
            @pl.when(jnp.logical_or(end, p < held))
            def _():
                copy_b(p, crossing(k)).start()
        for k in range(half - 1):
            copy_b(p, beside(k)).start()
        spot = (lax.rem(i, pieces) * DEPTH + sub * SUB) * BAND
        for band in range(bands):
            mine = send_b[field, right, band, pl.ds(pl.multiple_of(spot, BAND), SUB * BAND), :]
            there = pl.multiple_of(right * share_z * BAND + spot, BAND)
            second[field, band, pl.ds(there, SUB * BAND), :] = mine

    fetch(1)
    tables[0].wait()
    tables[1].wait()
    x_step(0, True)
    tables[2].wait()
    tables[3].wait()

    def step(i, carry):
        y_step(i, 0, i * subs)

        @pl.when(i + 1 < chunks)
        def _():
            x_step(i + 1, False)

        def part(sub, carry):
            y_step(i, sub, i * subs + sub)
            return carry

        lax.fori_loop(1, subs, part, 0)
        return carry

    lax.fori_loop(0, chunks, step, 0)

    @pl.when(jnp.logical_not(end))
    def _():
        for band in range(bands):
            for k in range(half):
                copy_c(band, crossing(k)).start()

    def z_step(n, carry):
        field, band = n // bands, lax.rem(n, bands)

        for sources, chosen in ((rights - 1, field < fields - 1), (half, field == fields - 1)):
            @pl.when(jnp.logical_and(band == 0, chosen))
            def _():
                landed(second.at[field, :, pl.ds(0, sources * share_z * BAND), :], rb_sem.at[field])

        @pl.when(field == fields - 1)
        def _():
            landed(second.at[field, band, pl.ds(0, (half - 1) * share_z * BAND), :], rc_sem.at[band])

        table = hz[...]

        def line(y, carry):
            plane = second[field, band, pl.ds(y, size_z, stride=BAND), :].T
            got = jnp.dot(jnp.concatenate(split(plane), axis=1), table, preferred_element_type=jnp.float32)
            got = (got[:, :size_z] + got[:, size_z:]) * lax.rsqrt(base[...] + sym_y[right * out_y + band * BAND + y])
            out[field, band, pl.ds(y, share_x, stride=BAND), :] = got
            return carry

        lax.fori_loop(0, BAND, line, 0, unroll=4)
        return carry

    lax.fori_loop(0, fields * bands, z_step, 0)

    landed(send_a.at[:, pl.ds(0, lefts - 1)], sa_sem)
    landed(send_b.at[:, pl.ds(0, rights - 1)], sb_sem)


def flush_kernel(ready, out, sem):
    fields, bands = ready.shape[:2]
    for n in range(fields * bands):
        field, band = n // bands, n % bands
        there = out.at[field, :, pl.ds(band * BAND, BAND), :]
        pltpu.make_async_copy(ready.at[field, band], there, sem).start()
    landed(out, sem)


def near_local(lefts, rights, tracer, symbol_x, symbol_y, symbol_z):
    fields, size_x, share_y, share_z = tracer.shape
    size_y, size_z = symbol_y.shape[0], symbol_z.shape[0]
    share_x, out_y = size_x // lefts, size_y // rights
    bands = out_y // BAND
    chunks = fields * (share_z // DEPTH)
    parts = chunks * (DEPTH // SUB)
    data = jnp.transpose(tracer, (0, 2, 3, 1))
    low, high = factors_of(size_x)
    hy, hz = small_table(size_y), stacked(small_table(size_z))
    f32, bf16 = jnp.float32, jnp.bfloat16
    any_space = pl.BlockSpec(memory_space=pl.ANY)
    vmem = pl.BlockSpec(memory_space=pltpu.VMEM)
    dma = pltpu.SemaphoreType.DMA
    ready = pl.pallas_call(
        functools.partial(near_kernel, lefts, rights),
        name="modes",
        out_shape=pltpu.VMEM((fields, bands, share_x * BAND, size_z), f32),
        in_specs=[*[any_space] * 5, vmem, vmem, pl.BlockSpec(memory_space=pltpu.SMEM)],
        out_specs=vmem,
        scratch_shapes=[
            pltpu.VMEM((chunks, DEPTH, size_y, share_x), f32),
            pltpu.VMEM((fields, bands, size_z * BAND, share_x), f32),
            pltpu.VMEM((2, size_x // LANES, share_y * DEPTH, LANES), f32),
            pltpu.VMEM(low.shape, f32),
            pltpu.VMEM(high.shape, f32),
            pltpu.VMEM((2, size_x, size_x), bf16),
            pltpu.VMEM(hy.shape, bf16),
            pltpu.VMEM(hz.shape, bf16),
            pltpu.VMEM((2, share_y * DEPTH, size_x), bf16),
            pltpu.VMEM((chunks, lefts, DEPTH, share_y, share_x), f32),
            pltpu.VMEM((fields, rights, bands, share_z * BAND, share_x), f32),
            pltpu.VMEM((share_x, size_z), f32),
            dma((2,)),
            dma((4,)),
            dma,
            dma((chunks, DEPTH // SUB)),
            dma,
            dma((fields,)),
            dma((bands,)),
        ],
        compiler_params=pltpu.CompilerParams(
            collective_id=0, has_side_effects=True, vmem_limit_bytes=NEAR_LIMIT
        ),
    )(data, low, high, hy, hz, symbol_x.reshape(lefts, share_x), symbol_z.reshape(1, size_z), symbol_y)
    return pl.pallas_call(
        flush_kernel,
        name="flush",
        out_shape=jax.ShapeDtypeStruct((fields, share_x, out_y, size_z), f32),
        in_specs=[vmem],
        out_specs=any_space,
        scratch_shapes=[dma],
        compiler_params=pltpu.CompilerParams(vmem_limit_bytes=2**21),
    )(ready.reshape(fields, bands, share_x, BAND, size_z))


def far_local(lefts, rights, tracer, symbol_x, symbol_y, symbol_z):
    fields, size_x, share_y, share_z = tracer.shape
    size_y, size_z = symbol_y.shape[0], symbol_z.shape[0]
    share_x, out_y = size_x // lefts, size_y // rights
    bands = out_y // BAND
    chunks = fields * (share_z // DEPTH)
    data = jnp.transpose(tracer, (0, 2, 3, 1))
    part_x = lax.dynamic_slice_in_dim(symbol_x, lax.axis_index("left") * share_x, share_x)
    base = part_x[:, None] + symbol_z[None, :]
    f32 = jnp.float32
    any_space = pl.BlockSpec(memory_space=pl.ANY)
    vmem = pl.BlockSpec(memory_space=pltpu.VMEM)
    landing = [(chunks, size_y * DEPTH, share_x), (fields, bands, size_z * BAND, share_x)]
    near = 4 * sum(map(math.prod, landing)) <= NEAR_BYTES
    staging = [] if near else [
        pltpu.VMEM((size_y * DEPTH, share_x), f32), pltpu.VMEM((size_z * BAND, share_x), f32)
    ]
    results = pl.pallas_call(
        functools.partial(far_kernel, lefts, rights, near),
        name="modes",
        out_shape=[
            jax.ShapeDtypeStruct((fields, bands, size_z // LANES, share_x * BAND, LANES), f32),
            *([] if near else [jax.ShapeDtypeStruct(shape, f32) for shape in landing]),
        ],
        in_specs=[any_space, vmem, vmem, vmem, vmem, pl.BlockSpec(memory_space=pltpu.SMEM)],
        out_specs=[any_space] * (1 if near else 3),
        scratch_shapes=[
            *([pltpu.VMEM(shape, f32) for shape in landing] if near else []),
            pltpu.VMEM((2, share_y, DEPTH, size_x), f32),
            pltpu.VMEM((2, share_y * DEPTH, size_x), jnp.bfloat16),
            pltpu.VMEM((SLOTS, lefts, share_y * DEPTH, share_x), f32),
            pltpu.VMEM((chunks, rights, bands, DEPTH * BAND, share_x), f32),
            pltpu.VMEM((2, size_z // LANES, share_x * BAND, LANES), f32),
            pltpu.SemaphoreType.DMA((2,)),
            pltpu.SemaphoreType.DMA((SLOTS, lefts)),
            pltpu.SemaphoreType.DMA((chunks, lefts)),
            pltpu.SemaphoreType.DMA,
            pltpu.SemaphoreType.DMA((chunks, rights, bands)),
            pltpu.SemaphoreType.DMA((chunks, rights, bands)),
            pltpu.SemaphoreType.DMA,
            pltpu.SemaphoreType.DMA((2,)),
            *staging,
        ],
        compiler_params=pltpu.CompilerParams(
            collective_id=0, has_side_effects=True, vmem_limit_bytes=60 * 2**20
        ),
    )(data, halves_of(transform_table(size_x)), small_table(size_y), small_table(size_z), base, symbol_y)
    out = results[0].reshape(fields, bands, size_z // LANES, share_x, BAND, LANES)
    return jnp.transpose(out, (0, 3, 1, 4, 2, 5)).reshape(fields, share_x, out_y, size_z)


def local(lefts, rights, tracer, symbol_x, symbol_y, symbol_z):
    fields, size_x, share_y, share_z = tracer.shape
    size_z, share_x = symbol_z.shape[0], size_x // lefts
    size = 4 * math.prod(tracer.shape)
    fits = size <= NEAR_BYTES // 2 and share_x == LANES and size_z == LANES and rights % 2 == 0
    run = near_local if fits else far_local
    return run(lefts, rights, tracer, symbol_x, symbol_y, symbol_z)


def solution(mesh):
    return jax.shard_map(
        functools.partial(local, mesh.shape["left"], mesh.shape["right"]),
        mesh=mesh,
        in_specs=(P(None, None, "left", "right"), P(), P(), P()),
        out_specs=P(None, "left", "right", None),
        check_vma=False,
    )
```

```python
import functools
import math

import jax
import jax.numpy as jnp
import numpy as np
from jax import lax
from jax.experimental import pallas as pl
from jax.experimental.pallas import tpu as pltpu
from jax.sharding import PartitionSpec as P

MESH = pl.DeviceIdType.MESH
NEAR_BYTES = 20 * 2**20
DEPTH = 8
BAND = 16
SUBLANES = 8
LANES = 128
SLOTS = 3
NEAR_LIMIT = 50 * 2**20
SUB = 2


def transform_table(count):
    inner = 1 << ((count.bit_length() - 1) // 2)
    outer = count // inner
    column = np.arange(count)

    def angle(row):
        return 2.0 * np.pi / count * (row[:, None] * column[None, :] % count)

    low = angle(np.arange(inner))
    high = angle(np.arange(outer) * inner)
    scale = count ** (-0.5)
    cos_low = jnp.asarray(np.cos(low), jnp.float32)[None]
    sin_low = jnp.asarray(np.sin(low), jnp.float32)[None]
    plus = jnp.asarray((np.cos(high) + np.sin(high)) * scale, jnp.float32)[:, None]
    minus = jnp.asarray((np.cos(high) - np.sin(high)) * scale, jnp.float32)[:, None]
    return (cos_low * plus + sin_low * minus).reshape(count, count)


def factors_of(count):
    inner = 1 << ((count.bit_length() - 1) // 2)
    outer = count // inner
    column = np.arange(count)

    def angle(row):
        return 2.0 * np.pi / count * (row[:, None] * column[None, :] % count)

    low = angle(np.arange(inner))
    high = angle(np.arange(outer) * inner)
    scale = count ** (-0.5)
    low = jnp.asarray(np.stack([np.cos(low), np.sin(low)]), jnp.float32)
    high = jnp.asarray(np.stack([np.cos(high) + np.sin(high), np.cos(high) - np.sin(high)]) * scale, jnp.float32)
    return low, high


def halves_of(table):
    upper = lax.reduce_precision(table, 8, 7)
    return jnp.stack([upper.astype(jnp.bfloat16), (table - upper).astype(jnp.bfloat16)])


def small_table(count):
    rank = np.arange(count)
    angle = 2.0 * np.pi / count * (rank[:, None] * rank[None, :] % count)
    table = ((np.cos(angle) + np.sin(angle)) * count ** (-0.5)).astype(np.float32)
    upper = table.astype(jnp.bfloat16)
    return jnp.asarray(np.stack([upper, (table - upper.astype(np.float32)).astype(jnp.bfloat16)]))


def split(values):
    upper = values.astype(jnp.bfloat16)
    return upper, (values - upper.astype(jnp.float32)).astype(jnp.bfloat16)


def product(a, b):
    dot = functools.partial(jnp.dot, preferred_element_type=jnp.float32)
    return dot(a[0], b[0]) + (dot(a[0], b[1]) + dot(a[1], b[0]))


def landed(ref, sem):
    pltpu.make_async_copy(ref, ref, sem).wait()


def far_kernel(lefts, rights, near, data, hx, hy, hz, base, sym_y, out, *rest):
    (first, second, dbuf, lines, send_a, send_b, obuf,
     d_sem, sa_sem, ra_sem, y_sem, sb_sem, rb_sem, z_sem, o_sem, *staging) = rest
    fields, share_y, share_z, _ = data.shape
    size_y, size_z = hy.shape[1], hz.shape[1]
    share_x = base.shape[0]
    bands = out.shape[1]
    pieces = share_z // DEPTH
    chunks = fields * pieces
    rows = share_y * DEPTH
    flat = DEPTH * BAND
    out_y = bands * BAND
    left, right = lax.axis_index("left"), lax.axis_index("right")

    def load(i):
        source = data.at[i // pieces, :, pl.ds(lax.rem(i, pieces) * DEPTH, DEPTH), :]
        return pltpu.make_async_copy(source, dbuf.at[lax.rem(i, 2)], d_sem.at[lax.rem(i, 2)])

    load(0).start()

    barrier = pltpu.get_barrier_semaphore()
    for k in range(1, lefts):
        pl.semaphore_signal(barrier, inc=1, device_id=(lax.rem(left + k, lefts), right), device_id_type=MESH)
    for k in range(1, rights):
        pl.semaphore_signal(barrier, inc=1, device_id=(left, lax.rem(right + k, rights)), device_id_type=MESH)
    pl.semaphore_wait(barrier, lefts + rights - 2)

    def copy_a(i, to):
        slot = lax.rem(i, SLOTS)
        return pltpu.make_async_remote_copy(
            src_ref=send_a.at[slot, to],
            dst_ref=first.at[i, pl.ds(left * rows, rows)],
            send_sem=sa_sem.at[slot, to],
            recv_sem=ra_sem.at[i, left],
            device_id=(to, right),
            device_id_type=MESH,
        )

    def copy_b(i, to, band):
        spot = right * share_z + lax.rem(i, pieces) * DEPTH
        return pltpu.make_async_remote_copy(
            src_ref=send_b.at[i, to, band],
            dst_ref=second.at[i // pieces, band, pl.ds(spot * BAND, flat)],
            send_sem=sb_sem.at[i, to, band],
            recv_sem=rb_sem.at[i, right, band],
            device_id=(left, to),
            device_id_type=MESH,
        )

    def sent_a(i):
        for k in range(1, lefts):
            copy_a(i, lax.rem(left + k, lefts)).wait_send()

    def x_step(i):
        load(i).wait()

        @pl.when(i + 1 < chunks)
        def _():
            load(i + 1).start()

        @pl.when(i >= SLOTS)
        def _():
            sent_a(i - SLOTS)

        slot = lax.rem(i, SLOTS)
        lines[0], lines[1] = split(dbuf[lax.rem(i, 2)].reshape(rows, hx.shape[1]))

        def tile(j, carry):
            cols = pl.ds(pl.multiple_of(j * 2 * share_x, 2 * share_x), 2 * share_x)
            got = product((lines[0], lines[1]), (hx[0, :, cols], hx[1, :, cols]))
            send_a[slot, 2 * j] = got[:, :share_x]
            send_a[slot, 2 * j + 1] = got[:, share_x:]
            return carry

        lax.fori_loop(0, lefts // 2, tile, 0)
        for k in range(1, lefts):
            copy_a(i, lax.rem(left + k, lefts)).start()
        pltpu.make_async_copy(
            send_a.at[slot, left], first.at[i, pl.ds(left * rows, rows)], ra_sem.at[i, left]
        ).start()

    def y_step(i):
        for k in range(lefts):
            landed(first.at[i, pl.ds(k * rows, rows)], ra_sem.at[i, k])
        if near:
            block = first.at[i]
        else:
            block = staging[0]
            fetch = pltpu.make_async_copy(first.at[i], block, y_sem)
            fetch.start()
            fetch.wait()
        for z in range(0, DEPTH, 2):
            pair = jnp.concatenate(
                [block[pl.ds(z, size_y, stride=DEPTH), :], block[pl.ds(z + 1, size_y, stride=DEPTH), :]], axis=1
            )
            got = product((hy[0], hy[1]), split(pair))
            for to in range(rights):
                for band in range(bands):
                    top = to * out_y + band * BAND
                    for half in range(2):
                        send_b[i, to, band, (z + half) * BAND:(z + half + 1) * BAND, :] = (
                            got[top:top + BAND, half * share_x:(half + 1) * share_x]
                        )
        for band in range(bands):
            for k in range(rights):
                to = jnp.where(right < rights // 2, rights - 1 - k, k)

                @pl.when(to != right)
                def _():
                    copy_b(i, to, band).start()

            spot = right * share_z + lax.rem(i, pieces) * DEPTH
            pltpu.make_async_copy(
                send_b.at[i, right, band],
                second.at[i // pieces, band, pl.ds(spot * BAND, flat)],
                rb_sem.at[i, right, band],
            ).start()

    def step(i, carry):
        @pl.when(i < chunks)
        def _():
            x_step(i)

        @pl.when(i >= 1)
        def _():
            y_step(i - 1)

        return carry

    lax.fori_loop(0, chunks + 1, step, 0)

    def put(n):
        slot = lax.rem(n, 2)
        return pltpu.make_async_copy(obuf.at[slot], out.at[n // bands, lax.rem(n, bands)], o_sem.at[slot])

    def z_step(n, carry):
        field, band = n // bands, lax.rem(n, bands)
        slot = lax.rem(n, 2)

        def arrive(p, carry):
            for k in range(rights):
                spot = k * share_z + p * DEPTH
                landed(second.at[field, band, pl.ds(spot * BAND, flat)], rb_sem.at[field * pieces + p, k, band])
            return carry

        lax.fori_loop(0, pieces, arrive, 0)
        if near:
            block = second.at[field, band]
        else:
            block = staging[1]
            fetch = pltpu.make_async_copy(second.at[field, band], block, z_sem)
            fetch.start()
            fetch.wait()

        @pl.when(n >= 2)
        def _():
            put(n - 2).wait()

        def line(y, carry):
            plane = block[pl.ds(y, size_z, stride=BAND), :].T
            got = product(split(plane), (hz[0], hz[1]))
            got = got * lax.rsqrt(base[...] + sym_y[right * out_y + band * BAND + y])
            for t in range(size_z // LANES):
                obuf[slot, t, pl.ds(y, share_x, stride=BAND), :] = got[:, t * LANES:(t + 1) * LANES]
            return carry

        lax.fori_loop(0, BAND, line, 0, unroll=2)
        put(n).start()
        return carry

    steps = fields * bands
    lax.fori_loop(0, steps, z_step, 0)

    def drain_a(i, carry):
        sent_a(i)
        return carry

    lax.fori_loop(max(chunks - SLOTS, 0), chunks, drain_a, 0)

    def drain_b(i, carry):
        for k in range(1, rights):
            for band in range(bands):
                copy_b(i, lax.rem(right + k, rights), band).wait_send()
        return carry

    lax.fori_loop(0, chunks, drain_b, 0)
    for n in range(max(steps - 2, 0), steps):
        put(n).wait()


def stacked(halves):
    upper, lower = halves[0], halves[1]
    return jnp.concatenate(
        [jnp.concatenate([upper, lower], axis=1), jnp.concatenate([upper, jnp.zeros_like(lower)], axis=1)], axis=0
    )


def near_kernel(lefts, rights, data, low_in, high_in, hy_in, hz_in, x_in, z_in, y_in, out, *rest):
    (first, second, dbuf, low, high, hx, hy, hz, lines, send_a, send_b, base,
     sym_x, sym_z, sym_y, d_sem, t_sem, sa_sem, ra_sem, rp_sem, sb_sem, rb_sem, rc_sem) = rest
    fields, share_y, share_z, size_x = data.shape
    size_y = hy.shape[1]
    share_x, size_z = base.shape
    bands = out.shape[1]
    pieces = share_z // DEPTH
    chunks = fields * pieces
    subs = DEPTH // SUB
    out_y = bands * BAND
    half = rights // 2
    left, right = lax.axis_index("left"), lax.axis_index("right")

    def load(i):
        slot = lax.rem(i, 2)
        planes = pl.ds(lax.rem(i, pieces) * DEPTH, DEPTH)
        return [pltpu.make_async_copy(
            data.at[i // pieces, :, planes, pl.ds(c * LANES, LANES)],
            dbuf.at[slot, c].reshape(share_y, DEPTH, LANES),
            d_sem.at[slot],
        ) for c in range(size_x // LANES)]

    def fetch(i):
        for copy in load(i):
            copy.start()

    tables = [pltpu.make_async_copy(a, b, t_sem.at[n]) for n, (a, b) in enumerate(
        [(low_in, low), (high_in, high), (hy_in, hy), (hz_in, hz), (x_in, sym_x), (z_in, sym_z), (y_in, sym_y)])]
    tables[0].start()
    tables[1].start()
    fetch(0)
    for table in tables[2:]:
        table.start()

    barrier = pltpu.get_barrier_semaphore()
    for k in range(1, lefts):
        pl.semaphore_signal(barrier, inc=1, device_id=(lax.rem(left + k, lefts), right), device_id_type=MESH)
    for k in range(1, rights):
        pl.semaphore_signal(barrier, inc=1, device_id=(left, lax.rem(right + k, rights)), device_id_type=MESH)

    def copy_a(i, z, count, to, sem):
        return pltpu.make_async_remote_copy(
            src_ref=send_a.at[i, to, pl.ds(z, count)],
            dst_ref=first.at[i, pl.ds(z, count), pl.ds(left * share_y, share_y), :],
            send_sem=sa_sem,
            recv_sem=sem,
            device_id=(to, right),
            device_id_type=MESH,
        )

    def copy_b(field, spot, count, to):
        return pltpu.make_async_remote_copy(
            src_ref=send_b.at[field, to, :, pl.ds(spot * BAND, count * BAND), :],
            dst_ref=second.at[field, :, pl.ds((right * share_z + spot) * BAND, count * BAND), :],
            send_sem=sb_sem,
            recv_sem=rb_sem.at[field],
            device_id=(left, to),
            device_id_type=MESH,
        )

    def copy_c(n, to):
        band, rows = n // 2, pl.ds(n % 2 * SUBLANES, SUBLANES)
        there = second.at[fields - 1, band].reshape(size_z, BAND, share_x)
        return pltpu.make_async_remote_copy(
            src_ref=send_b.at[fields - 1, to, band].reshape(share_z, BAND, share_x).at[:, rows, :],
            dst_ref=there.at[pl.ds(right * share_z, share_z), rows, :],
            send_sem=sb_sem,
            recv_sem=rc_sem.at[n],
            device_id=(left, to),
            device_id_type=MESH,
        )

    lower = right < half
    rank = jnp.where(lower, right, rights - 1 - right)
    end = rank == 0

    def mirrored(t):
        return jnp.where(lower, t, rights - 1 - t)

    def crossing(k):
        return mirrored(jnp.where(end, rights - 1 - k, half + k))

    def beside(k):
        return mirrored(lax.rem(rank + 1 + k, half))

    def widen(cols):
        for top in range(size_x // low.shape[1]):
            made = low[0, :, cols] * high[0, top:top + 1, cols] + low[1, :, cols] * high[1, top:top + 1, cols]
            rows = pl.ds(top * low.shape[1], low.shape[1])
            hx[0, rows, cols], hx[1, rows, cols] = split(made)

    def partner(k):
        return left ^ k if lefts & (lefts - 1) == 0 else lax.rem(left + k, lefts)

    def x_tile(i, j, z, count, opening):
        pair = partner(lefts - 1 - 2 * j) // 2
        cols = pl.ds(pl.multiple_of(pair * 2 * share_x, 2 * share_x), 2 * share_x)
        if opening:
            widen(cols)
        rows = pl.ds(z * share_y, count * share_y)
        got = product((lines[0, rows, :], lines[1, rows, :]), (hx[0, :, cols], hx[1, :, cols]))
        for core in range(2):
            part = got[:, core * share_x:(core + 1) * share_x].reshape(count, share_y, share_x)
            send_a[i, 2 * pair + core, z:z + count] = part
        return pair

    def x_split(i, planes):
        slot = lax.rem(i, 2)
        for c in range(size_x // LANES):
            cols = pl.ds(c * LANES, LANES)
            for z in planes:
                rows = pl.ds(z * share_y, share_y)
                lines[0, rows, cols], lines[1, rows, cols] = split(dbuf[slot, c, pl.ds(z, share_y, stride=DEPTH), :])

    def x_send(i, z, count, pair, sem):
        for core in range(2):
            @pl.when(2 * pair + core != left)
            def _():
                copy_a(i, z, count, 2 * pair + core, sem).start()

    def x_rest(i, subs_left):
        for sub in subs_left:
            for k in range(lefts - 1, 0, -1):
                copy_a(i, sub * SUB, SUB, partner(k), ra_sem.at[i, sub]).start()

    def x_own(i, z, count):
        mine = pl.ds(pl.multiple_of(left * share_y, share_y), share_y)
        first[i, z:z + count, mine, :] = send_a[i, left, z:z + count]

    def x_open():
        landed(dbuf.at[0], d_sem.at[0])
        x_split(0, range(SUB))
        pair = x_tile(0, 0, 0, SUB, True)
        pl.semaphore_wait(barrier, lefts + rights - 2)
        x_send(0, 0, 1, pair, rp_sem.at[0])

        def tile(j, carry):
            x_send(0, 0, 1, x_tile(0, j, 0, SUB, True), rp_sem.at[0])
            return carry

        lax.fori_loop(1, lefts // 2, tile, 0)
        for z in range(1, SUB):
            for k in range(lefts - 1, 0, -1):
                copy_a(0, z, 1, partner(k), rp_sem.at[z]).start()
        x_own(0, 0, SUB)
        x_split(0, range(SUB, DEPTH))

        def more(j, carry):
            x_send(0, SUB, SUB, x_tile(0, j, SUB, DEPTH - SUB, False), ra_sem.at[0, 1])
            return carry

        lax.fori_loop(0, lefts // 2, more, 0)
        x_rest(0, range(2, subs))
        x_own(0, SUB, DEPTH - SUB)
        fetch(2)

    def x_step(i):
        slot = lax.rem(i, 2)
        landed(dbuf.at[slot], d_sem.at[slot])
        x_split(i, range(DEPTH))

        @pl.when(i + 2 < chunks)
        def _():
            fetch(i + 2)

        def tile(j, carry):
            x_send(i, 0, SUB, x_tile(i, j, 0, DEPTH, False), ra_sem.at[i, 0])
            return carry

        lax.fori_loop(0, lefts // 2, tile, 0)
        x_rest(i, range(1, subs))
        x_own(i, 0, DEPTH)

    def y_step(i, z, count, sem):
        landed(first.at[i, pl.ds(z, count), pl.ds(0, (lefts - 1) * share_y), :], sem)
        field, spot = i // pieces, lax.rem(i, pieces) * DEPTH + z
        wide = jnp.concatenate([first[i, z + n] for n in range(count)], axis=1)
        got = product((hy[0], hy[1]), split(wide))
        for to in range(rights):
            for band in range(bands):
                top = to * out_y + band * BAND
                for n in range(count):
                    rows = pl.ds(pl.multiple_of((spot + n) * BAND, BAND), BAND)
                    send_b[field, to, band, rows, :] = got[top:top + BAND, n * share_x:(n + 1) * share_x]
        for k in range(half):
            @pl.when(jnp.logical_or(end, field < fields - 1))
            def _():
                copy_b(field, spot, count, crossing(k)).start()
        for k in range(half - 1):
            copy_b(field, spot, count, beside(k)).start()
        for band in range(bands):
            mine = send_b[field, right, band, pl.ds(pl.multiple_of(spot * BAND, BAND), count * BAND), :]
            there = pl.multiple_of((right * share_z + spot) * BAND, BAND)
            second[field, band, pl.ds(there, count * BAND), :] = mine

    fetch(1)
    tables[0].wait()
    tables[1].wait()
    x_open()
    tables[2].wait()
    tables[3].wait()
    for z in range(SUB):
        y_step(0, z, 1, rp_sem.at[z])

    def step(i, carry):
        @pl.when(i + 1 < chunks)
        def _():
            x_step(i + 1)

        def part(sub, carry):
            y_step(i, sub * SUB, SUB, ra_sem.at[i, sub])
            return carry

        lax.fori_loop(1, subs, part, 0)

        @pl.when(i + 1 < chunks)
        def _():
            y_step(i + 1, 0, SUB, ra_sem.at[i + 1, 0])

        return carry

    lax.fori_loop(0, chunks, step, 0)

    @pl.when(jnp.logical_not(end))
    def _():
        for n in range(2 * bands):
            for k in range(half):
                copy_c(n, crossing(k)).start()

    for table in tables[4:]:
        table.wait()
    column = jnp.broadcast_to(sym_x[pl.ds(left, 1), :], (size_z, share_x)).T
    base[...] = column + sym_z[...]

    def z_step(n, carry):
        field, part = n // (2 * bands), lax.rem(n, 2 * bands)
        band, top = part // 2, lax.rem(part, 2) * SUBLANES
        for sources, chosen in ((rights - 1, field < fields - 1), (half, field == fields - 1)):
            @pl.when(jnp.logical_and(part == 0, chosen))
            def _():
                landed(second.at[field, :, pl.ds(0, sources * share_z * BAND), :], rb_sem.at[field])

        @pl.when(field == fields - 1)
        def _():
            block = second.at[field, band].reshape(size_z, BAND, share_x)
            landed(block.at[pl.ds(0, (half - 1) * share_z), pl.ds(top, SUBLANES), :], rc_sem.at[part])

        table = hz[...]

        def line(step, carry):
            y = top + step
            plane = second[field, band, pl.ds(y, size_z, stride=BAND), :].T
            got = jnp.dot(jnp.concatenate(split(plane), axis=1), table, preferred_element_type=jnp.float32)
            got = (got[:, :size_z] + got[:, size_z:]) * lax.rsqrt(base[...] + sym_y[right * out_y + band * BAND + y])
            out[field, band, pl.ds(y, share_x, stride=BAND), :] = got
            return carry

        lax.fori_loop(0, SUBLANES, line, 0, unroll=4)
        return carry

    lax.fori_loop(0, fields * bands * 2, z_step, 0)
    landed(send_a.at[:, pl.ds(0, lefts - 1)], sa_sem)
    landed(send_b.at[:, pl.ds(0, rights - 1)], sb_sem)


def flush_kernel(ready, out, sem):
    fields, bands = ready.shape[:2]
    for n in range(fields * bands):
        field, band = n // bands, n % bands
        there = out.at[field, :, pl.ds(band * BAND, BAND), :]
        pltpu.make_async_copy(ready.at[field, band], there, sem).start()
    landed(out, sem)


def near_local(lefts, rights, tracer, symbol_x, symbol_y, symbol_z):
    fields, size_x, share_y, share_z = tracer.shape
    size_y, size_z = symbol_y.shape[0], symbol_z.shape[0]
    share_x, out_y = size_x // lefts, size_y // rights
    bands = out_y // BAND
    chunks = fields * (share_z // DEPTH)
    data = jnp.transpose(tracer, (0, 2, 3, 1))
    low, high = factors_of(size_x)
    hy, hz = small_table(size_y), stacked(small_table(size_z))
    f32, bf16 = jnp.float32, jnp.bfloat16
    any_space = pl.BlockSpec(memory_space=pl.ANY)
    vmem = pl.BlockSpec(memory_space=pltpu.VMEM)
    dma = pltpu.SemaphoreType.DMA
    ready = pl.pallas_call(
        functools.partial(near_kernel, lefts, rights),
        name="modes",
        out_shape=pltpu.VMEM((fields, bands, share_x * BAND, size_z), f32),
        in_specs=[any_space] * 8,
        out_specs=vmem,
        scratch_shapes=[
            pltpu.VMEM((chunks, DEPTH, size_y, share_x), f32),
            pltpu.VMEM((fields, bands, size_z * BAND, share_x), f32),
            pltpu.VMEM((2, size_x // LANES, share_y * DEPTH, LANES), f32),
            pltpu.VMEM(low.shape, f32),
            pltpu.VMEM(high.shape, f32),
            pltpu.VMEM((2, size_x, size_x), bf16),
            pltpu.VMEM(hy.shape, bf16),
            pltpu.VMEM(hz.shape, bf16),
            pltpu.VMEM((2, share_y * DEPTH, size_x), bf16),
            pltpu.VMEM((chunks, lefts, DEPTH, share_y, share_x), f32),
            pltpu.VMEM((fields, rights, bands, share_z * BAND, share_x), f32),
            pltpu.VMEM((share_x, size_z), f32),
            pltpu.VMEM((lefts, share_x), f32),
            pltpu.VMEM((1, size_z), f32),
            pltpu.SMEM((size_y,), f32),
            dma((2,)),
            dma((7,)),
            dma,
            dma((chunks, DEPTH // SUB)),
            dma((SUB,)),
            dma,
            dma((fields,)),
            dma((2 * bands,)),
        ],
        compiler_params=pltpu.CompilerParams(
            collective_id=0, has_side_effects=True, vmem_limit_bytes=NEAR_LIMIT
        ),
    )(data, low, high, hy, hz, symbol_x.reshape(lefts, share_x), symbol_z.reshape(1, size_z), symbol_y)
    return pl.pallas_call(
        flush_kernel,
        name="flush",
        out_shape=jax.ShapeDtypeStruct((fields, share_x, out_y, size_z), f32),
        in_specs=[vmem],
        out_specs=any_space,
        scratch_shapes=[dma],
        compiler_params=pltpu.CompilerParams(vmem_limit_bytes=2**21),
    )(ready.reshape(fields, bands, share_x, BAND, size_z))


def far_local(lefts, rights, tracer, symbol_x, symbol_y, symbol_z):
    fields, size_x, share_y, share_z = tracer.shape
    size_y, size_z = symbol_y.shape[0], symbol_z.shape[0]
    share_x, out_y = size_x // lefts, size_y // rights
    bands = out_y // BAND
    chunks = fields * (share_z // DEPTH)
    data = jnp.transpose(tracer, (0, 2, 3, 1))
    part_x = lax.dynamic_slice_in_dim(symbol_x, lax.axis_index("left") * share_x, share_x)
    base = part_x[:, None] + symbol_z[None, :]
    f32 = jnp.float32
    any_space = pl.BlockSpec(memory_space=pl.ANY)
    vmem = pl.BlockSpec(memory_space=pltpu.VMEM)
    landing = [(chunks, size_y * DEPTH, share_x), (fields, bands, size_z * BAND, share_x)]
    near = 4 * sum(map(math.prod, landing)) <= NEAR_BYTES
    staging = [] if near else [
        pltpu.VMEM((size_y * DEPTH, share_x), f32), pltpu.VMEM((size_z * BAND, share_x), f32)
    ]
    results = pl.pallas_call(
        functools.partial(far_kernel, lefts, rights, near),
        name="modes",
        out_shape=[
            jax.ShapeDtypeStruct((fields, bands, size_z // LANES, share_x * BAND, LANES), f32),
            *([] if near else [jax.ShapeDtypeStruct(shape, f32) for shape in landing]),
        ],
        in_specs=[any_space, vmem, vmem, vmem, vmem, pl.BlockSpec(memory_space=pltpu.SMEM)],
        out_specs=[any_space] * (1 if near else 3),
        scratch_shapes=[
            *([pltpu.VMEM(shape, f32) for shape in landing] if near else []),
            pltpu.VMEM((2, share_y, DEPTH, size_x), f32),
            pltpu.VMEM((2, share_y * DEPTH, size_x), jnp.bfloat16),
            pltpu.VMEM((SLOTS, lefts, share_y * DEPTH, share_x), f32),
            pltpu.VMEM((chunks, rights, bands, DEPTH * BAND, share_x), f32),
            pltpu.VMEM((2, size_z // LANES, share_x * BAND, LANES), f32),
            pltpu.SemaphoreType.DMA((2,)),
            pltpu.SemaphoreType.DMA((SLOTS, lefts)),
            pltpu.SemaphoreType.DMA((chunks, lefts)),
            pltpu.SemaphoreType.DMA,
            pltpu.SemaphoreType.DMA((chunks, rights, bands)),
            pltpu.SemaphoreType.DMA((chunks, rights, bands)),
            pltpu.SemaphoreType.DMA,
            pltpu.SemaphoreType.DMA((2,)),
            *staging,
        ],
        compiler_params=pltpu.CompilerParams(
            collective_id=0, has_side_effects=True, vmem_limit_bytes=60 * 2**20
        ),
    )(data, halves_of(transform_table(size_x)), small_table(size_y), small_table(size_z), base, symbol_y)
    out = results[0].reshape(fields, bands, size_z // LANES, share_x, BAND, LANES)
    return jnp.transpose(out, (0, 3, 1, 4, 2, 5)).reshape(fields, share_x, out_y, size_z)


def local(lefts, rights, tracer, symbol_x, symbol_y, symbol_z):
    fields, size_x, share_y, share_z = tracer.shape
    size_z, share_x = symbol_z.shape[0], size_x // lefts
    size = 4 * math.prod(tracer.shape)
    fits = size <= NEAR_BYTES // 2 and share_x == LANES and size_z == LANES and rights % 2 == 0
    run = near_local if fits else far_local
    return run(lefts, rights, tracer, symbol_x, symbol_y, symbol_z)


def solution(mesh):
    return jax.shard_map(
        functools.partial(local, mesh.shape["left"], mesh.shape["right"]),
        mesh=mesh,
        in_specs=(P(None, None, "left", "right"), P(), P(), P()),
        out_specs=P(None, "left", "right", None),
        check_vma=False,
    )
```

```python
import functools
import math

import jax
import jax.numpy as jnp
import numpy as np
from jax import lax
from jax.experimental import pallas as pl
from jax.experimental.pallas import tpu as pltpu
from jax.sharding import PartitionSpec as P

MESH = pl.DeviceIdType.MESH
NEAR_BYTES = 20 * 2**20
DEPTH = 8
BAND = 16
SUBLANES = 8
LANES = 128
SLOTS = 3
NEAR_LIMIT = 50 * 2**20
SUB = 2


def transform_table(count):
    inner = 1 << ((count.bit_length() - 1) // 2)
    outer = count // inner
    column = np.arange(count)

    def angle(row):
        return 2.0 * np.pi / count * (row[:, None] * column[None, :] % count)

    low = angle(np.arange(inner))
    high = angle(np.arange(outer) * inner)
    scale = count ** (-0.5)
    cos_low = jnp.asarray(np.cos(low), jnp.float32)[None]
    sin_low = jnp.asarray(np.sin(low), jnp.float32)[None]
    plus = jnp.asarray((np.cos(high) + np.sin(high)) * scale, jnp.float32)[:, None]
    minus = jnp.asarray((np.cos(high) - np.sin(high)) * scale, jnp.float32)[:, None]
    return (cos_low * plus + sin_low * minus).reshape(count, count)


def factors_of(count):
    inner = 1 << ((count.bit_length() - 1) // 2)
    outer = count // inner
    column = np.arange(count)

    def angle(row):
        return 2.0 * np.pi / count * (row[:, None] * column[None, :] % count)

    low = angle(np.arange(inner))
    high = angle(np.arange(outer) * inner)
    scale = count ** (-0.5)
    low = jnp.asarray(np.stack([np.cos(low), np.sin(low)]), jnp.float32)
    high = jnp.asarray(np.stack([np.cos(high) + np.sin(high), np.cos(high) - np.sin(high)]) * scale, jnp.float32)
    return low, high


def halves_of(table):
    upper = lax.reduce_precision(table, 8, 7)
    return jnp.stack([upper.astype(jnp.bfloat16), (table - upper).astype(jnp.bfloat16)])


def small_table(count):
    rank = np.arange(count)
    angle = 2.0 * np.pi / count * (rank[:, None] * rank[None, :] % count)
    table = ((np.cos(angle) + np.sin(angle)) * count ** (-0.5)).astype(np.float32)
    upper = table.astype(jnp.bfloat16)
    return jnp.asarray(np.stack([upper, (table - upper.astype(np.float32)).astype(jnp.bfloat16)]))


def split(values):
    upper = values.astype(jnp.bfloat16)
    return upper, (values - upper.astype(jnp.float32)).astype(jnp.bfloat16)


def product(a, b):
    dot = functools.partial(jnp.dot, preferred_element_type=jnp.float32)
    return dot(a[0], b[0]) + (dot(a[0], b[1]) + dot(a[1], b[0]))


def landed(ref, sem):
    pltpu.make_async_copy(ref, ref, sem).wait()


def far_kernel(lefts, rights, near, data, hx, hy, hz, base, sym_y, out, *rest):
    (first, second, dbuf, lines, send_a, send_b, obuf,
     d_sem, sa_sem, ra_sem, y_sem, sb_sem, rb_sem, z_sem, o_sem, *staging) = rest
    fields, share_y, share_z, _ = data.shape
    size_y, size_z = hy.shape[1], hz.shape[1]
    share_x = base.shape[0]
    bands = out.shape[1]
    pieces = share_z // DEPTH
    chunks = fields * pieces
    rows = share_y * DEPTH
    flat = DEPTH * BAND
    out_y = bands * BAND
    left, right = lax.axis_index("left"), lax.axis_index("right")

    def load(i):
        source = data.at[i // pieces, :, pl.ds(lax.rem(i, pieces) * DEPTH, DEPTH), :]
        return pltpu.make_async_copy(source, dbuf.at[lax.rem(i, 2)], d_sem.at[lax.rem(i, 2)])

    load(0).start()

    barrier = pltpu.get_barrier_semaphore()
    for k in range(1, lefts):
        pl.semaphore_signal(barrier, inc=1, device_id=(lax.rem(left + k, lefts), right), device_id_type=MESH)
    for k in range(1, rights):
        pl.semaphore_signal(barrier, inc=1, device_id=(left, lax.rem(right + k, rights)), device_id_type=MESH)
    pl.semaphore_wait(barrier, lefts + rights - 2)

    def copy_a(i, to):
        slot = lax.rem(i, SLOTS)
        return pltpu.make_async_remote_copy(
            src_ref=send_a.at[slot, to],
            dst_ref=first.at[i, pl.ds(left * rows, rows)],
            send_sem=sa_sem.at[slot, to],
            recv_sem=ra_sem.at[i, left],
            device_id=(to, right),
            device_id_type=MESH,
        )

    def copy_b(i, to, band):
        spot = right * share_z + lax.rem(i, pieces) * DEPTH
        return pltpu.make_async_remote_copy(
            src_ref=send_b.at[i, to, band],
            dst_ref=second.at[i // pieces, band, pl.ds(spot * BAND, flat)],
            send_sem=sb_sem.at[i, to, band],
            recv_sem=rb_sem.at[i, right, band],
            device_id=(left, to),
            device_id_type=MESH,
        )

    def sent_a(i):
        for k in range(1, lefts):
            copy_a(i, lax.rem(left + k, lefts)).wait_send()

    def x_step(i):
        load(i).wait()

        @pl.when(i + 1 < chunks)
        def _():
            load(i + 1).start()

        @pl.when(i >= SLOTS)
        def _():
            sent_a(i - SLOTS)

        slot = lax.rem(i, SLOTS)
        lines[0], lines[1] = split(dbuf[lax.rem(i, 2)].reshape(rows, hx.shape[1]))

        def tile(j, carry):
            cols = pl.ds(pl.multiple_of(j * 2 * share_x, 2 * share_x), 2 * share_x)
            got = product((lines[0], lines[1]), (hx[0, :, cols], hx[1, :, cols]))
            send_a[slot, 2 * j] = got[:, :share_x]
            send_a[slot, 2 * j + 1] = got[:, share_x:]
            return carry

        lax.fori_loop(0, lefts // 2, tile, 0)
        for k in range(1, lefts):
            copy_a(i, lax.rem(left + k, lefts)).start()
        pltpu.make_async_copy(
            send_a.at[slot, left], first.at[i, pl.ds(left * rows, rows)], ra_sem.at[i, left]
        ).start()

    def y_step(i):
        for k in range(lefts):
            landed(first.at[i, pl.ds(k * rows, rows)], ra_sem.at[i, k])
        if near:
            block = first.at[i]
        else:
            block = staging[0]
            fetch = pltpu.make_async_copy(first.at[i], block, y_sem)
            fetch.start()
            fetch.wait()
        for z in range(0, DEPTH, 2):
            pair = jnp.concatenate(
                [block[pl.ds(z, size_y, stride=DEPTH), :], block[pl.ds(z + 1, size_y, stride=DEPTH), :]], axis=1
            )
            got = product((hy[0], hy[1]), split(pair))
            for to in range(rights):
                for band in range(bands):
                    top = to * out_y + band * BAND
                    for half in range(2):
                        send_b[i, to, band, (z + half) * BAND:(z + half + 1) * BAND, :] = (
                            got[top:top + BAND, half * share_x:(half + 1) * share_x]
                        )
        for band in range(bands):
            for k in range(rights):
                to = jnp.where(right < rights // 2, rights - 1 - k, k)

                @pl.when(to != right)
                def _():
                    copy_b(i, to, band).start()

            spot = right * share_z + lax.rem(i, pieces) * DEPTH
            pltpu.make_async_copy(
                send_b.at[i, right, band],
                second.at[i // pieces, band, pl.ds(spot * BAND, flat)],
                rb_sem.at[i, right, band],
            ).start()

    def step(i, carry):
        @pl.when(i < chunks)
        def _():
            x_step(i)

        @pl.when(i >= 1)
        def _():
            y_step(i - 1)

        return carry

    lax.fori_loop(0, chunks + 1, step, 0)

    def put(n):
        slot = lax.rem(n, 2)
        return pltpu.make_async_copy(obuf.at[slot], out.at[n // bands, lax.rem(n, bands)], o_sem.at[slot])

    def z_step(n, carry):
        field, band = n // bands, lax.rem(n, bands)
        slot = lax.rem(n, 2)

        def arrive(p, carry):
            for k in range(rights):
                spot = k * share_z + p * DEPTH
                landed(second.at[field, band, pl.ds(spot * BAND, flat)], rb_sem.at[field * pieces + p, k, band])
            return carry

        lax.fori_loop(0, pieces, arrive, 0)
        if near:
            block = second.at[field, band]
        else:
            block = staging[1]
            fetch = pltpu.make_async_copy(second.at[field, band], block, z_sem)
            fetch.start()
            fetch.wait()

        @pl.when(n >= 2)
        def _():
            put(n - 2).wait()

        def line(y, carry):
            plane = block[pl.ds(y, size_z, stride=BAND), :].T
            got = product(split(plane), (hz[0], hz[1]))
            got = got * lax.rsqrt(base[...] + sym_y[right * out_y + band * BAND + y])
            for t in range(size_z // LANES):
                obuf[slot, t, pl.ds(y, share_x, stride=BAND), :] = got[:, t * LANES:(t + 1) * LANES]
            return carry

        lax.fori_loop(0, BAND, line, 0, unroll=2)
        put(n).start()
        return carry

    steps = fields * bands
    lax.fori_loop(0, steps, z_step, 0)

    def drain_a(i, carry):
        sent_a(i)
        return carry

    lax.fori_loop(max(chunks - SLOTS, 0), chunks, drain_a, 0)

    def drain_b(i, carry):
        for k in range(1, rights):
            for band in range(bands):
                copy_b(i, lax.rem(right + k, rights), band).wait_send()
        return carry

    lax.fori_loop(0, chunks, drain_b, 0)
    for n in range(max(steps - 2, 0), steps):
        put(n).wait()


def stacked(halves):
    upper, lower = halves[0], halves[1]
    return jnp.concatenate(
        [jnp.concatenate([upper, lower], axis=1), jnp.concatenate([upper, jnp.zeros_like(lower)], axis=1)], axis=0
    )


def near_kernel(lefts, rights, data, low_in, high_in, hy_in, hz_in, x_in, z_in, y_in, out, *rest):
    (first, second, dbuf, low, high, hx, hy, hz, lines, send_a, send_b, base,
     sym_x, sym_z, sym_y, raw_out, raw_in, guest_a, guest_first, guest_b,
     d_sem, t_sem, sa_sem, ra_sem, rp_sem, sb_sem, rb_sem, rc_sem, raw_sem, guest_sem) = rest
    fields, share_y, share_z, size_x = data.shape
    size_y = hy.shape[1]
    share_x, size_z = base.shape
    bands = out.shape[1]
    pieces = share_z // DEPTH
    chunks = fields * pieces
    subs = DEPTH // SUB
    out_y = bands * BAND
    half = rights // 2
    left, right = lax.axis_index("left"), lax.axis_index("right")

    def load(i):
        slot = lax.rem(i, 2)
        planes = pl.ds(lax.rem(i, pieces) * DEPTH, DEPTH)
        return [pltpu.make_async_copy(
            data.at[i // pieces, :, planes, pl.ds(c * LANES, LANES)],
            dbuf.at[slot, c].reshape(share_y, DEPTH, LANES),
            d_sem.at[slot],
        ) for c in range(size_x // LANES)]

    def fetch(i):
        for copy in load(i):
            copy.start()

    tables = [pltpu.make_async_copy(a, b, t_sem.at[n]) for n, (a, b) in enumerate(
        [(low_in, low), (high_in, high), (hy_in, hy), (hz_in, hz), (x_in, sym_x), (z_in, sym_z), (y_in, sym_y)])]
    tables[0].start()
    tables[1].start()
    fetch(0)
    for table in tables[2:]:
        table.start()

    barrier = pltpu.get_barrier_semaphore()
    for k in range(1, lefts):
        pl.semaphore_signal(barrier, inc=1, device_id=(lax.rem(left + k, lefts), right), device_id_type=MESH)
    for k in range(1, rights):
        pl.semaphore_signal(barrier, inc=1, device_id=(left, lax.rem(right + k, rights)), device_id_type=MESH)

    def copy_a(i, z, count, to, sem):
        return pltpu.make_async_remote_copy(
            src_ref=send_a.at[i, to, pl.ds(z, count)],
            dst_ref=first.at[i, pl.ds(z, count), pl.ds(left * share_y, share_y), :],
            send_sem=sa_sem,
            recv_sem=sem,
            device_id=(to, right),
            device_id_type=MESH,
        )

    def copy_b(field, spot, count, to, kind):
        return pltpu.make_async_remote_copy(
            src_ref=send_b.at[field, to, :, pl.ds(spot * BAND, count * BAND), :],
            dst_ref=second.at[field, :, pl.ds((right * share_z + spot) * BAND, count * BAND), :],
            send_sem=sb_sem.at[jnp.where(field == 0, kind, 2)],
            recv_sem=rb_sem.at[field],
            device_id=(left, to),
            device_id_type=MESH,
        )

    def copy_c(n, to):
        band, rows = n // 2, pl.ds(n % 2 * SUBLANES, SUBLANES)
        there = second.at[fields - 1, band].reshape(size_z, BAND, share_x)
        return pltpu.make_async_remote_copy(
            src_ref=send_b.at[fields - 1, to, band].reshape(share_z, BAND, share_x).at[:, rows, :],
            dst_ref=there.at[pl.ds(right * share_z, share_z), rows, :],
            send_sem=sb_sem.at[2],
            recv_sem=rc_sem.at[n],
            device_id=(left, to),
            device_id_type=MESH,
        )

    lower = right < half
    rank = jnp.where(lower, right, rights - 1 - right)
    end = rank == 0
    gate = rank == half - 1
    twin = rights - 1 - right
    guest_z = DEPTH - SUB

    def mirrored(t):
        return jnp.where(lower, t, rights - 1 - t)

    def crossing(k):
        return mirrored(jnp.where(end, rights - 1 - k, half + k))

    def beside(k):
        return mirrored(lax.rem(rank + 1 + k, half))

    def raw():
        return pltpu.make_async_remote_copy(
            src_ref=raw_out,
            dst_ref=raw_in,
            send_sem=raw_sem.at[0],
            recv_sem=raw_sem.at[1],
            device_id=(left, twin),
            device_id_type=MESH,
        )

    def copy_guest_a(to):
        return pltpu.make_async_remote_copy(
            src_ref=guest_a.at[to],
            dst_ref=guest_first.at[:, pl.ds(left * share_y, share_y), :],
            send_sem=guest_sem.at[0],
            recv_sem=guest_sem.at[1],
            device_id=(to, right),
            device_id_type=MESH,
        )

    def copy_guest_b(to):
        spot = (twin * share_z + guest_z) * BAND
        return pltpu.make_async_remote_copy(
            src_ref=guest_b.at[to],
            dst_ref=second.at[0, :, pl.ds(spot, SUB * BAND), :],
            send_sem=guest_sem.at[2],
            recv_sem=rb_sem.at[0],
            device_id=(left, to),
            device_id_type=MESH,
        )

    def widen(cols):
        for top in range(size_x // low.shape[1]):
            made = low[0, :, cols] * high[0, top:top + 1, cols] + low[1, :, cols] * high[1, top:top + 1, cols]
            rows = pl.ds(top * low.shape[1], low.shape[1])
            hx[0, rows, cols], hx[1, rows, cols] = split(made)

    def partner(k):
        return left ^ k if lefts & (lefts - 1) == 0 else lax.rem(left + k, lefts)

    def x_tile(sends, j, z, count, opening):
        pair = partner(lefts - 1 - 2 * j) // 2
        cols = pl.ds(pl.multiple_of(pair * 2 * share_x, 2 * share_x), 2 * share_x)
        if opening:
            widen(cols)
        rows = pl.ds(z * share_y, count * share_y)
        got = product((lines[0, rows, :], lines[1, rows, :]), (hx[0, :, cols], hx[1, :, cols]))
        for core in range(2):
            part = got[:, core * share_x:(core + 1) * share_x].reshape(count, share_y, share_x)
            sends[2 * pair + core, z:z + count] = part
        return pair

    def x_split(i, planes):
        slot = lax.rem(i, 2)
        for c in range(size_x // LANES):
            cols = pl.ds(c * LANES, LANES)
            for z in planes:
                rows = pl.ds(z * share_y, share_y)
                lines[0, rows, cols], lines[1, rows, cols] = split(dbuf[slot, c, pl.ds(z, share_y, stride=DEPTH), :])

    def x_send(i, z, count, pair, sem):
        for core in range(2):
            @pl.when(2 * pair + core != left)
            def _():
                copy_a(i, z, count, 2 * pair + core, sem).start()

    def x_rest(i, subs_left):
        for sub in subs_left:
            for k in range(lefts - 1, 0, -1):
                copy_a(i, sub * SUB, SUB, partner(k), ra_sem.at[i, sub]).start()

    def x_own(i, z, count):
        mine = pl.ds(pl.multiple_of(left * share_y, share_y), share_y)
        first[i, z:z + count, mine, :] = send_a[i, left, z:z + count]

    def x_open():
        landed(dbuf.at[0], d_sem.at[0])
        x_split(0, range(SUB))
        for c in range(size_x // LANES):
            for z in range(SUB):
                line = dbuf[0, c, pl.ds(guest_z + z, share_y, stride=DEPTH), :]
                raw_out[z * share_y:(z + 1) * share_y, c * LANES:(c + 1) * LANES] = line
        pair = x_tile(send_a.at[0], 0, 0, SUB, True)
        pl.semaphore_wait(barrier, lefts + rights - 2)

        @pl.when(gate)
        def _():
            raw().start()

        x_send(0, 0, 1, pair, rp_sem.at[0])

        def tile(j, carry):
            x_send(0, 0, 1, x_tile(send_a.at[0], j, 0, SUB, True), rp_sem.at[0])
            return carry

        lax.fori_loop(1, lefts // 2, tile, 0)
        for z in range(1, SUB):
            for k in range(lefts - 1, 0, -1):
                copy_a(0, z, 1, partner(k), rp_sem.at[z]).start()
        x_own(0, 0, SUB)
        x_split(0, range(SUB, DEPTH))

        def more(j, carry):
            x_send(0, SUB, SUB, x_tile(send_a.at[0], j, SUB, DEPTH - SUB, False), ra_sem.at[0, 1])
            return carry

        lax.fori_loop(0, lefts // 2, more, 0)
        x_rest(0, range(2, subs))
        x_own(0, SUB, DEPTH - SUB)
        fetch(2)

    def x_step(i):
        slot = lax.rem(i, 2)
        landed(dbuf.at[slot], d_sem.at[slot])
        x_split(i, range(DEPTH))

        @pl.when(i + 2 < chunks)
        def _():
            fetch(i + 2)

        def tile(j, carry):
            x_send(i, 0, SUB, x_tile(send_a.at[i], j, 0, DEPTH, False), ra_sem.at[i, 0])
            return carry

        lax.fori_loop(0, lefts // 2, tile, 0)
        x_rest(i, range(1, subs))
        x_own(i, 0, DEPTH)

    def y_values(ready, sends, spot, count):
        got = product((hy[0], hy[1]), split(jnp.concatenate([ready[n] for n in range(count)], axis=1)))
        for to in range(rights):
            for band in range(bands):
                top = to * out_y + band * BAND
                for n in range(count):
                    rows = pl.ds(pl.multiple_of((spot + n) * BAND, BAND), BAND)
                    sends[to, band, rows, :] = got[top:top + BAND, n * share_x:(n + 1) * share_x]

    def y_own(sends, spot, field, there, count):
        for band in range(bands):
            mine = sends[right, band, pl.ds(pl.multiple_of(spot * BAND, BAND), count * BAND), :]
            second[field, band, pl.ds(pl.multiple_of(there * BAND, BAND), count * BAND), :] = mine

    def y_step(i, z, count, sem):
        landed(first.at[i, pl.ds(z, count), pl.ds(0, (lefts - 1) * share_y), :], sem)
        field, spot = i // pieces, lax.rem(i, pieces) * DEPTH + z
        y_values(first.at[i, pl.ds(z, count)], send_b.at[field], spot, count)
        hosted = jnp.logical_and(gate, jnp.logical_and(i == 0, z == guest_z))
        direct = jnp.logical_or(end, jnp.logical_and(field < fields - 1, jnp.logical_not(hosted)))
        for k in range(half):
            @pl.when(direct)
            def _():
                copy_b(field, spot, count, crossing(k), 0).start()
        for k in range(half - 1):
            copy_b(field, spot, count, beside(k), 1).start()
        y_own(send_b.at[field], spot, field, right * share_z + spot, count)

    def guest_x():
        landed(raw_in, raw_sem.at[1])
        for c in range(size_x // LANES):
            cols = pl.ds(c * LANES, LANES)
            lines[0, pl.ds(0, SUB * share_y), cols], lines[1, pl.ds(0, SUB * share_y), cols] = split(raw_in[:, cols])

        def tile(j, carry):
            x_tile(guest_a, j, 0, SUB, False)
            return carry

        lax.fori_loop(0, lefts // 2, tile, 0)
        for k in range(lefts - 1, 0, -1):
            copy_guest_a(partner(k)).start()
        guest_first[:, pl.ds(pl.multiple_of(left * share_y, share_y), share_y), :] = guest_a[left]

    def guest_y():
        landed(guest_first.at[:, pl.ds(0, (lefts - 1) * share_y), :], guest_sem.at[1])
        y_values(guest_first, guest_b, 0, SUB)
        for k in range(half - 1):
            copy_guest_b(beside(k)).start()
        y_own(guest_b, 0, 0, twin * share_z + guest_z, SUB)

    fetch(1)
    tables[0].wait()
    tables[1].wait()
    x_open()
    tables[2].wait()
    tables[3].wait()
    for z in range(SUB):
        y_step(0, z, 1, rp_sem.at[z])

    def step(i, carry):
        @pl.when(i + 1 < chunks)
        def _():
            x_step(i + 1)

        @pl.when(jnp.logical_and(gate, i == min(1, chunks - 1)))
        def _():
            guest_x()

        def part(sub, carry):
            y_step(i, sub * SUB, SUB, ra_sem.at[i, sub])
            return carry

        lax.fori_loop(1, subs, part, 0)

        @pl.when(jnp.logical_and(gate, i == min(2, chunks - 1)))
        def _():
            guest_y()

        @pl.when(i + 1 < chunks)
        def _():
            y_step(i + 1, 0, SUB, ra_sem.at[i + 1, 0])

        return carry

    lax.fori_loop(0, chunks, step, 0)

    @pl.when(jnp.logical_not(end))
    def _():
        for n in range(2 * bands):
            for k in range(half):
                copy_c(n, crossing(k)).start()

    for table in tables[4:]:
        table.wait()
    column = jnp.broadcast_to(sym_x[pl.ds(left, 1), :], (size_z, share_x)).T
    base[...] = column + sym_z[...]

    def z_step(n, carry):
        field, part = n // (2 * bands), lax.rem(n, 2 * bands)
        band, top = part // 2, lax.rem(part, 2) * SUBLANES
        hosting = jnp.logical_and(gate, field == 0)
        everything = (rights - 1) * share_z
        for planes, chosen in (
            (everything - SUB, hosting),
            (everything, jnp.logical_and(field < fields - 1, jnp.logical_not(hosting))),
            (half * share_z, field == fields - 1),
        ):
            @pl.when(jnp.logical_and(part == 0, chosen))
            def _():
                landed(second.at[field, :, pl.ds(0, planes * BAND), :], rb_sem.at[field])

        @pl.when(field == fields - 1)
        def _():
            block = second.at[field, band].reshape(size_z, BAND, share_x)
            landed(block.at[pl.ds(0, (half - 1) * share_z), pl.ds(top, SUBLANES), :], rc_sem.at[part])

        table = hz[...]

        def line(step, carry):
            y = top + step
            plane = second[field, band, pl.ds(y, size_z, stride=BAND), :].T
            got = jnp.dot(jnp.concatenate(split(plane), axis=1), table, preferred_element_type=jnp.float32)
            got = (got[:, :size_z] + got[:, size_z:]) * lax.rsqrt(base[...] + sym_y[right * out_y + band * BAND + y])
            out[field, band, pl.ds(y, share_x, stride=BAND), :] = got
            return carry

        lax.fori_loop(0, SUBLANES, line, 0, unroll=4)
        return carry

    lax.fori_loop(0, fields * bands * 2, z_step, 0)
    landed(send_a.at[:, pl.ds(0, lefts - 1)], sa_sem)
    landed(send_b.at[0, pl.ds(0, half - 1)], sb_sem.at[1])
    landed(send_b.at[pl.ds(1, fields - 1), pl.ds(0, rights - 1)], sb_sem.at[2])

    @pl.when(gate)
    def _():
        landed(send_b.at[0, pl.ds(0, half), :, pl.ds(0, (share_z - SUB) * BAND), :], sb_sem.at[0])
        landed(raw_out, raw_sem.at[0])
        landed(guest_a.at[pl.ds(0, lefts - 1)], guest_sem.at[0])
        landed(guest_b.at[pl.ds(0, half - 1)], guest_sem.at[2])

    @pl.when(jnp.logical_not(gate))
    def _():
        landed(send_b.at[0, pl.ds(0, half)], sb_sem.at[0])


def flush_kernel(ready, out, sem):
    fields, bands = ready.shape[:2]
    for n in range(fields * bands):
        field, band = n // bands, n % bands
        there = out.at[field, :, pl.ds(band * BAND, BAND), :]
        pltpu.make_async_copy(ready.at[field, band], there, sem).start()
    landed(out, sem)


def near_local(lefts, rights, tracer, symbol_x, symbol_y, symbol_z):
    fields, size_x, share_y, share_z = tracer.shape
    size_y, size_z = symbol_y.shape[0], symbol_z.shape[0]
    share_x, out_y = size_x // lefts, size_y // rights
    bands = out_y // BAND
    chunks = fields * (share_z // DEPTH)
    data = jnp.transpose(tracer, (0, 2, 3, 1))
    low, high = factors_of(size_x)
    hy, hz = small_table(size_y), stacked(small_table(size_z))
    f32, bf16 = jnp.float32, jnp.bfloat16
    any_space = pl.BlockSpec(memory_space=pl.ANY)
    vmem = pl.BlockSpec(memory_space=pltpu.VMEM)
    dma = pltpu.SemaphoreType.DMA
    ready = pl.pallas_call(
        functools.partial(near_kernel, lefts, rights),
        name="modes",
        out_shape=pltpu.VMEM((fields, bands, share_x * BAND, size_z), f32),
        in_specs=[any_space] * 8,
        out_specs=vmem,
        scratch_shapes=[
            pltpu.VMEM((chunks, DEPTH, size_y, share_x), f32),
            pltpu.VMEM((fields, bands, size_z * BAND, share_x), f32),
            pltpu.VMEM((2, size_x // LANES, share_y * DEPTH, LANES), f32),
            pltpu.VMEM(low.shape, f32),
            pltpu.VMEM(high.shape, f32),
            pltpu.VMEM((2, size_x, size_x), bf16),
            pltpu.VMEM(hy.shape, bf16),
            pltpu.VMEM(hz.shape, bf16),
            pltpu.VMEM((2, share_y * DEPTH, size_x), bf16),
            pltpu.VMEM((chunks, lefts, DEPTH, share_y, share_x), f32),
            pltpu.VMEM((fields, rights, bands, share_z * BAND, share_x), f32),
            pltpu.VMEM((share_x, size_z), f32),
            pltpu.VMEM((lefts, share_x), f32),
            pltpu.VMEM((1, size_z), f32),
            pltpu.SMEM((size_y,), f32),
            pltpu.VMEM((SUB * share_y, size_x), f32),
            pltpu.VMEM((SUB * share_y, size_x), f32),
            pltpu.VMEM((lefts, SUB, share_y, share_x), f32),
            pltpu.VMEM((SUB, size_y, share_x), f32),
            pltpu.VMEM((rights, bands, SUB * BAND, share_x), f32),
            dma((2,)),
            dma((7,)),
            dma,
            dma((chunks, DEPTH // SUB)),
            dma((SUB,)),
            dma((3,)),
            dma((fields,)),
            dma((2 * bands,)),
            dma((2,)),
            dma((3,)),
        ],
        compiler_params=pltpu.CompilerParams(
            collective_id=0, has_side_effects=True, vmem_limit_bytes=NEAR_LIMIT
        ),
    )(data, low, high, hy, hz, symbol_x.reshape(lefts, share_x), symbol_z.reshape(1, size_z), symbol_y)
    return pl.pallas_call(
        flush_kernel,
        name="flush",
        out_shape=jax.ShapeDtypeStruct((fields, share_x, out_y, size_z), f32),
        in_specs=[vmem],
        out_specs=any_space,
        scratch_shapes=[dma],
        compiler_params=pltpu.CompilerParams(vmem_limit_bytes=2**21),
    )(ready.reshape(fields, bands, share_x, BAND, size_z))


def far_local(lefts, rights, tracer, symbol_x, symbol_y, symbol_z):
    fields, size_x, share_y, share_z = tracer.shape
    size_y, size_z = symbol_y.shape[0], symbol_z.shape[0]
    share_x, out_y = size_x // lefts, size_y // rights
    bands = out_y // BAND
    chunks = fields * (share_z // DEPTH)
    data = jnp.transpose(tracer, (0, 2, 3, 1))
    part_x = lax.dynamic_slice_in_dim(symbol_x, lax.axis_index("left") * share_x, share_x)
    base = part_x[:, None] + symbol_z[None, :]
    f32 = jnp.float32
    any_space = pl.BlockSpec(memory_space=pl.ANY)
    vmem = pl.BlockSpec(memory_space=pltpu.VMEM)
    landing = [(chunks, size_y * DEPTH, share_x), (fields, bands, size_z * BAND, share_x)]
    near = 4 * sum(map(math.prod, landing)) <= NEAR_BYTES
    staging = [] if near else [
        pltpu.VMEM((size_y * DEPTH, share_x), f32), pltpu.VMEM((size_z * BAND, share_x), f32)
    ]
    results = pl.pallas_call(
        functools.partial(far_kernel, lefts, rights, near),
        name="modes",
        out_shape=[
            jax.ShapeDtypeStruct((fields, bands, size_z // LANES, share_x * BAND, LANES), f32),
            *([] if near else [jax.ShapeDtypeStruct(shape, f32) for shape in landing]),
        ],
        in_specs=[any_space, vmem, vmem, vmem, vmem, pl.BlockSpec(memory_space=pltpu.SMEM)],
        out_specs=[any_space] * (1 if near else 3),
        scratch_shapes=[
            *([pltpu.VMEM(shape, f32) for shape in landing] if near else []),
            pltpu.VMEM((2, share_y, DEPTH, size_x), f32),
            pltpu.VMEM((2, share_y * DEPTH, size_x), jnp.bfloat16),
            pltpu.VMEM((SLOTS, lefts, share_y * DEPTH, share_x), f32),
            pltpu.VMEM((chunks, rights, bands, DEPTH * BAND, share_x), f32),
            pltpu.VMEM((2, size_z // LANES, share_x * BAND, LANES), f32),
            pltpu.SemaphoreType.DMA((2,)),
            pltpu.SemaphoreType.DMA((SLOTS, lefts)),
            pltpu.SemaphoreType.DMA((chunks, lefts)),
            pltpu.SemaphoreType.DMA,
            pltpu.SemaphoreType.DMA((chunks, rights, bands)),
            pltpu.SemaphoreType.DMA((chunks, rights, bands)),
            pltpu.SemaphoreType.DMA,
            pltpu.SemaphoreType.DMA((2,)),
            *staging,
        ],
        compiler_params=pltpu.CompilerParams(
            collective_id=0, has_side_effects=True, vmem_limit_bytes=60 * 2**20
        ),
    )(data, halves_of(transform_table(size_x)), small_table(size_y), small_table(size_z), base, symbol_y)
    out = results[0].reshape(fields, bands, size_z // LANES, share_x, BAND, LANES)
    return jnp.transpose(out, (0, 3, 1, 4, 2, 5)).reshape(fields, share_x, out_y, size_z)


def local(lefts, rights, tracer, symbol_x, symbol_y, symbol_z):
    fields, size_x, share_y, share_z = tracer.shape
    size_z, share_x = symbol_z.shape[0], size_x // lefts
    size = 4 * math.prod(tracer.shape)
    fits = size <= NEAR_BYTES // 2 and share_x == LANES and size_z == LANES and rights % 2 == 0
    fits = fits and rights > 2 and fields > 1
    run = near_local if fits else far_local
    return run(lefts, rights, tracer, symbol_x, symbol_y, symbol_z)


def solution(mesh):
    return jax.shard_map(
        functools.partial(local, mesh.shape["left"], mesh.shape["right"]),
        mesh=mesh,
        in_specs=(P(None, None, "left", "right"), P(), P(), P()),
        out_specs=P(None, "left", "right", None),
        check_vma=False,
    )
```

```python
import functools
import math

import jax
import jax.numpy as jnp
import numpy as np
from jax import lax
from jax.experimental import pallas as pl
from jax.experimental.pallas import tpu as pltpu
from jax.sharding import PartitionSpec as P

MESH = pl.DeviceIdType.MESH
NEAR_BYTES = 20 * 2**20
DEPTH = 8
BAND = 16
SUBLANES = 8
LANES = 128
SLOTS = 3
NEAR_LIMIT = 50 * 2**20
SUB = 2


def transform_table(count):
    inner = 1 << ((count.bit_length() - 1) // 2)
    outer = count // inner
    column = np.arange(count)

    def angle(row):
        return 2.0 * np.pi / count * (row[:, None] * column[None, :] % count)

    low = angle(np.arange(inner))
    high = angle(np.arange(outer) * inner)
    scale = count ** (-0.5)
    cos_low = jnp.asarray(np.cos(low), jnp.float32)[None]
    sin_low = jnp.asarray(np.sin(low), jnp.float32)[None]
    plus = jnp.asarray((np.cos(high) + np.sin(high)) * scale, jnp.float32)[:, None]
    minus = jnp.asarray((np.cos(high) - np.sin(high)) * scale, jnp.float32)[:, None]
    return (cos_low * plus + sin_low * minus).reshape(count, count)


def factors_of(count):
    inner = 1 << ((count.bit_length() - 1) // 2)
    outer = count // inner
    column = np.arange(count)

    def angle(row):
        return 2.0 * np.pi / count * (row[:, None] * column[None, :] % count)

    low = angle(np.arange(inner))
    high = angle(np.arange(outer) * inner)
    scale = count ** (-0.5)
    low = np.stack([np.cos(low), np.sin(low)])
    high = np.stack([np.cos(high) + np.sin(high), np.cos(high) - np.sin(high)]) * scale
    rows = max(inner, outer)
    padded = [np.pad(part, ((0, 0), (0, rows - part.shape[1]), (0, 0))) for part in (low, high)]
    return jnp.asarray(np.concatenate(padded), jnp.float32), inner


def halves_of(table):
    upper = lax.reduce_precision(table, 8, 7)
    return jnp.stack([upper.astype(jnp.bfloat16), (table - upper).astype(jnp.bfloat16)])


def small_table(count):
    rank = np.arange(count)
    angle = 2.0 * np.pi / count * (rank[:, None] * rank[None, :] % count)
    table = ((np.cos(angle) + np.sin(angle)) * count ** (-0.5)).astype(np.float32)
    upper = table.astype(jnp.bfloat16)
    return jnp.asarray(np.stack([upper, (table - upper.astype(np.float32)).astype(jnp.bfloat16)]))


def split(values):
    upper = values.astype(jnp.bfloat16)
    return upper, (values - upper.astype(jnp.float32)).astype(jnp.bfloat16)


def product(a, b):
    dot = functools.partial(jnp.dot, preferred_element_type=jnp.float32)
    return dot(a[0], b[0]) + (dot(a[0], b[1]) + dot(a[1], b[0]))


def landed(ref, sem):
    pltpu.make_async_copy(ref, ref, sem).wait()


def far_kernel(lefts, rights, near, data, hx, hy, hz, base, sym_y, out, *rest):
    (first, second, dbuf, lines, send_a, send_b, obuf,
     d_sem, sa_sem, ra_sem, y_sem, sb_sem, rb_sem, z_sem, o_sem, *staging) = rest
    fields, share_y, share_z, _ = data.shape
    size_y, size_z = hy.shape[1], hz.shape[1]
    share_x = base.shape[0]
    bands = out.shape[1]
    pieces = share_z // DEPTH
    chunks = fields * pieces
    rows = share_y * DEPTH
    flat = DEPTH * BAND
    out_y = bands * BAND
    left, right = lax.axis_index("left"), lax.axis_index("right")

    def load(i):
        source = data.at[i // pieces, :, pl.ds(lax.rem(i, pieces) * DEPTH, DEPTH), :]
        return pltpu.make_async_copy(source, dbuf.at[lax.rem(i, 2)], d_sem.at[lax.rem(i, 2)])

    load(0).start()

    barrier = pltpu.get_barrier_semaphore()
    for k in range(1, lefts):
        pl.semaphore_signal(barrier, inc=1, device_id=(lax.rem(left + k, lefts), right), device_id_type=MESH)
    for k in range(1, rights):
        pl.semaphore_signal(barrier, inc=1, device_id=(left, lax.rem(right + k, rights)), device_id_type=MESH)
    pl.semaphore_wait(barrier, lefts + rights - 2)

    def copy_a(i, to):
        slot = lax.rem(i, SLOTS)
        return pltpu.make_async_remote_copy(
            src_ref=send_a.at[slot, to],
            dst_ref=first.at[i, pl.ds(left * rows, rows)],
            send_sem=sa_sem.at[slot, to],
            recv_sem=ra_sem.at[i, left],
            device_id=(to, right),
            device_id_type=MESH,
        )

    def copy_b(i, to, band):
        spot = right * share_z + lax.rem(i, pieces) * DEPTH
        return pltpu.make_async_remote_copy(
            src_ref=send_b.at[i, to, band],
            dst_ref=second.at[i // pieces, band, pl.ds(spot * BAND, flat)],
            send_sem=sb_sem.at[i, to, band],
            recv_sem=rb_sem.at[i, right, band],
            device_id=(left, to),
            device_id_type=MESH,
        )

    def sent_a(i):
        for k in range(1, lefts):
            copy_a(i, lax.rem(left + k, lefts)).wait_send()

    def x_step(i):
        load(i).wait()

        @pl.when(i + 1 < chunks)
        def _():
            load(i + 1).start()

        @pl.when(i >= SLOTS)
        def _():
            sent_a(i - SLOTS)

        slot = lax.rem(i, SLOTS)
        lines[0], lines[1] = split(dbuf[lax.rem(i, 2)].reshape(rows, hx.shape[1]))

        def tile(j, carry):
            cols = pl.ds(pl.multiple_of(j * 2 * share_x, 2 * share_x), 2 * share_x)
            got = product((lines[0], lines[1]), (hx[0, :, cols], hx[1, :, cols]))
            send_a[slot, 2 * j] = got[:, :share_x]
            send_a[slot, 2 * j + 1] = got[:, share_x:]
            return carry

        lax.fori_loop(0, lefts // 2, tile, 0)
        for k in range(1, lefts):
            copy_a(i, lax.rem(left + k, lefts)).start()
        pltpu.make_async_copy(
            send_a.at[slot, left], first.at[i, pl.ds(left * rows, rows)], ra_sem.at[i, left]
        ).start()

    def y_step(i):
        for k in range(lefts):
            landed(first.at[i, pl.ds(k * rows, rows)], ra_sem.at[i, k])
        if near:
            block = first.at[i]
        else:
            block = staging[0]
            fetch = pltpu.make_async_copy(first.at[i], block, y_sem)
            fetch.start()
            fetch.wait()
        for z in range(0, DEPTH, 2):
            pair = jnp.concatenate(
                [block[pl.ds(z, size_y, stride=DEPTH), :], block[pl.ds(z + 1, size_y, stride=DEPTH), :]], axis=1
            )
            got = product((hy[0], hy[1]), split(pair))
            for to in range(rights):
                for band in range(bands):
                    top = to * out_y + band * BAND
                    for half in range(2):
                        send_b[i, to, band, (z + half) * BAND:(z + half + 1) * BAND, :] = (
                            got[top:top + BAND, half * share_x:(half + 1) * share_x]
                        )
        for band in range(bands):
            for k in range(rights):
                to = jnp.where(right < rights // 2, rights - 1 - k, k)

                @pl.when(to != right)
                def _():
                    copy_b(i, to, band).start()

            spot = right * share_z + lax.rem(i, pieces) * DEPTH
            pltpu.make_async_copy(
                send_b.at[i, right, band],
                second.at[i // pieces, band, pl.ds(spot * BAND, flat)],
                rb_sem.at[i, right, band],
            ).start()

    def step(i, carry):
        @pl.when(i < chunks)
        def _():
            x_step(i)

        @pl.when(i >= 1)
        def _():
            y_step(i - 1)

        return carry

    lax.fori_loop(0, chunks + 1, step, 0)

    def put(n):
        slot = lax.rem(n, 2)
        return pltpu.make_async_copy(obuf.at[slot], out.at[n // bands, lax.rem(n, bands)], o_sem.at[slot])

    def z_step(n, carry):
        field, band = n // bands, lax.rem(n, bands)
        slot = lax.rem(n, 2)

        def arrive(p, carry):
            for k in range(rights):
                spot = k * share_z + p * DEPTH
                landed(second.at[field, band, pl.ds(spot * BAND, flat)], rb_sem.at[field * pieces + p, k, band])
            return carry

        lax.fori_loop(0, pieces, arrive, 0)
        if near:
            block = second.at[field, band]
        else:
            block = staging[1]
            fetch = pltpu.make_async_copy(second.at[field, band], block, z_sem)
            fetch.start()
            fetch.wait()

        @pl.when(n >= 2)
        def _():
            put(n - 2).wait()

        def line(y, carry):
            plane = block[pl.ds(y, size_z, stride=BAND), :].T
            got = product(split(plane), (hz[0], hz[1]))
            got = got * lax.rsqrt(base[...] + sym_y[right * out_y + band * BAND + y])
            for t in range(size_z // LANES):
                obuf[slot, t, pl.ds(y, share_x, stride=BAND), :] = got[:, t * LANES:(t + 1) * LANES]
            return carry

        lax.fori_loop(0, BAND, line, 0, unroll=2)
        put(n).start()
        return carry

    steps = fields * bands
    lax.fori_loop(0, steps, z_step, 0)

    def drain_a(i, carry):
        sent_a(i)
        return carry

    lax.fori_loop(max(chunks - SLOTS, 0), chunks, drain_a, 0)

    def drain_b(i, carry):
        for k in range(1, rights):
            for band in range(bands):
                copy_b(i, lax.rem(right + k, rights), band).wait_send()
        return carry

    lax.fori_loop(0, chunks, drain_b, 0)
    for n in range(max(steps - 2, 0), steps):
        put(n).wait()


def stacked(halves):
    upper, lower = halves[0], halves[1]
    return jnp.concatenate(
        [jnp.concatenate([upper, lower], axis=1), jnp.concatenate([upper, jnp.zeros_like(lower)], axis=1)], axis=0
    )


def near_kernel(lefts, rights, inner, data, factors_in, hy_in, hz_in, x_in, z_in, y_in, out, tail, scale, table, *rest):
    (first, second, dbuf, factors, hx, hy, hz, lines, send_a, send_b, base,
     sym_x, sym_z, sym_y, raw_out, raw_in, guest_a, guest_first, guest_b,
     d_sem, t_sem, sa_sem, ra_sem, sb_sem, rb_sem, rc_sem, raw_sem, guest_sem) = rest
    fields, share_y, share_z, size_x = data.shape
    size_y = hy.shape[1]
    share_x, size_z = base.shape
    bands = out.shape[1]
    pieces = share_z // DEPTH
    chunks = fields * pieces
    subs = DEPTH // SUB
    out_y = bands * BAND
    half = rights // 2
    left, right = lax.axis_index("left"), lax.axis_index("right")

    def load(i):
        slot = lax.rem(i, 2)
        planes = pl.ds(lax.rem(i, pieces) * DEPTH, DEPTH)
        return [pltpu.make_async_copy(
            data.at[i // pieces, :, planes, pl.ds(c * LANES, LANES)],
            dbuf.at[slot, c].reshape(share_y, DEPTH, LANES),
            d_sem.at[slot],
        ) for c in range(size_x // LANES)]

    def fetch(i):
        for copy in load(i):
            copy.start()

    def copies(pairs):
        return [pltpu.make_async_copy(a, b, t_sem.at[n]) for n, (a, b) in enumerate(pairs)]

    tables = copies([(factors_in, factors), (hy_in, hy), (hz_in, hz)])
    symbols = copies([(x_in, sym_x), (z_in, sym_z), (y_in, sym_y)])
    tables[0].start()
    fetch(0)
    tables[1].start()
    tables[2].start()

    barrier = pltpu.get_barrier_semaphore()
    for k in range(1, lefts):
        pl.semaphore_signal(barrier, inc=1, device_id=(lax.rem(left + k, lefts), right), device_id_type=MESH)
    for k in range(1, rights):
        pl.semaphore_signal(barrier, inc=1, device_id=(left, lax.rem(right + k, rights)), device_id_type=MESH)

    def copy_a(i, z, count, to, sem):
        return pltpu.make_async_remote_copy(
            src_ref=send_a.at[i, to, pl.ds(z, count)],
            dst_ref=first.at[i, pl.ds(z, count), pl.ds(left * share_y, share_y), :],
            send_sem=sa_sem,
            recv_sem=sem,
            device_id=(to, right),
            device_id_type=MESH,
        )

    def copy_b(field, spot, count, to, kind):
        return pltpu.make_async_remote_copy(
            src_ref=send_b.at[field, to, :, pl.ds(spot * BAND, count * BAND), :],
            dst_ref=second.at[field, :, pl.ds((right * share_z + spot) * BAND, count * BAND), :],
            send_sem=sb_sem.at[jnp.where(field == 0, kind, 2)],
            recv_sem=rb_sem.at[field],
            device_id=(left, to),
            device_id_type=MESH,
        )

    def copy_c(n, to):
        band, rows = n // 2, pl.ds(n % 2 * SUBLANES, SUBLANES)
        there = second.at[fields - 1, band].reshape(size_z, BAND, share_x)
        return pltpu.make_async_remote_copy(
            src_ref=send_b.at[fields - 1, to, band].reshape(share_z, BAND, share_x).at[:, rows, :],
            dst_ref=there.at[pl.ds(right * share_z, share_z), rows, :],
            send_sem=sb_sem.at[2],
            recv_sem=rc_sem.at[n],
            device_id=(left, to),
            device_id_type=MESH,
        )

    lower = right < half
    rank = jnp.where(lower, right, rights - 1 - right)
    end = rank == 0
    gate = rank == half - 1
    twin = rights - 1 - right
    guest_z = DEPTH - SUB

    def mirrored(t):
        return jnp.where(lower, t, rights - 1 - t)

    def crossing(k):
        return mirrored(jnp.where(end, rights - 1 - k, half + k))

    def beside(k):
        return mirrored(lax.rem(rank + 1 + k, half))

    def raw():
        return pltpu.make_async_remote_copy(
            src_ref=raw_out,
            dst_ref=raw_in,
            send_sem=raw_sem.at[0],
            recv_sem=raw_sem.at[1],
            device_id=(left, twin),
            device_id_type=MESH,
        )

    def copy_guest_a(to):
        return pltpu.make_async_remote_copy(
            src_ref=guest_a.at[to],
            dst_ref=guest_first.at[:, pl.ds(left * share_y, share_y), :],
            send_sem=guest_sem.at[0],
            recv_sem=guest_sem.at[1],
            device_id=(to, right),
            device_id_type=MESH,
        )

    def copy_guest_b(to):
        spot = (twin * share_z + guest_z) * BAND
        return pltpu.make_async_remote_copy(
            src_ref=guest_b.at[to],
            dst_ref=second.at[0, :, pl.ds(spot, SUB * BAND), :],
            send_sem=guest_sem.at[2],
            recv_sem=rb_sem.at[0],
            device_id=(left, to),
            device_id_type=MESH,
        )

    def widen(cols):
        for top in range(size_x // inner):
            plus, minus = factors[2, top:top + 1, cols], factors[3, top:top + 1, cols]
            made = factors[0, :inner, cols] * plus + factors[1, :inner, cols] * minus
            rows = pl.ds(top * inner, inner)
            hx[0, rows, cols], hx[1, rows, cols] = split(made)

    def arrival(i, sub):
        return ra_sem.at[lax.rem(i, SLOTS), sub]

    def partner(k):
        return left ^ k if lefts & (lefts - 1) == 0 else lax.rem(left + k, lefts)

    def x_tile(sends, j, z, count, opening):
        pair = partner(lefts - 1 - 2 * j) // 2
        cols = pl.ds(pl.multiple_of(pair * 2 * share_x, 2 * share_x), 2 * share_x)
        if opening:
            widen(cols)
        rows = pl.ds(z * share_y, count * share_y)
        got = product((lines[0, rows, :], lines[1, rows, :]), (hx[0, :, cols], hx[1, :, cols]))
        for core in range(2):
            part = got[:, core * share_x:(core + 1) * share_x].reshape(count, share_y, share_x)
            sends[2 * pair + core, z:z + count] = part
        return pair

    def x_split(i, planes):
        slot = lax.rem(i, 2)
        for c in range(size_x // LANES):
            cols = pl.ds(c * LANES, LANES)
            for z in planes:
                rows = pl.ds(z * share_y, share_y)
                lines[0, rows, cols], lines[1, rows, cols] = split(dbuf[slot, c, pl.ds(z, share_y, stride=DEPTH), :])

    def x_send(i, z, count, pair, sem):
        for core in range(2):
            @pl.when(2 * pair + core != left)
            def _():
                copy_a(i, z, count, 2 * pair + core, sem).start()

    def x_rest(i, subs_left):
        for sub in subs_left:
            for k in range(lefts - 1, 0, -1):
                copy_a(i, sub * SUB, SUB, partner(k), arrival(i, sub)).start()

    def x_own(i, z, count):
        mine = pl.ds(pl.multiple_of(left * share_y, share_y), share_y)
        first[i, z:z + count, mine, :] = send_a[i, left, z:z + count]

    def x_open():
        landed(dbuf.at[0], d_sem.at[0])
        x_split(0, range(SUB))
        for c in range(size_x // LANES):
            for z in range(SUB):
                line = dbuf[0, c, pl.ds(guest_z + z, share_y, stride=DEPTH), :]
                raw_out[z * share_y:(z + 1) * share_y, c * LANES:(c + 1) * LANES] = line
        pair = x_tile(send_a.at[0], 0, 0, SUB, True)
        pl.semaphore_wait(barrier, lefts + rights - 2)

        @pl.when(gate)
        def _():
            raw().start()

        x_send(0, 0, 1, pair, arrival(0, 0))

        def tile(j, carry):
            x_send(0, 0, 1, x_tile(send_a.at[0], j, 0, SUB, True), arrival(0, 0))
            return carry

        lax.fori_loop(1, lefts // 2, tile, 0)
        for z in range(1, SUB):
            for k in range(lefts - 1, 0, -1):
                copy_a(0, z, 1, partner(k), arrival(2 * z, 0)).start()
        x_own(0, 0, SUB)
        x_split(0, range(SUB, DEPTH))

        def more(j, carry):
            x_send(0, SUB, SUB, x_tile(send_a.at[0], j, SUB, DEPTH - SUB, False), arrival(0, 1))
            return carry

        lax.fori_loop(0, lefts // 2, more, 0)
        x_rest(0, range(2, subs))
        x_own(0, SUB, DEPTH - SUB)
        fetch(2)

    def x_step(i):
        slot = lax.rem(i, 2)
        landed(dbuf.at[slot], d_sem.at[slot])
        x_split(i, range(DEPTH))

        @pl.when(i + 2 < chunks)
        def _():
            fetch(i + 2)

        def tile(j, carry):
            x_send(i, 0, SUB, x_tile(send_a.at[i], j, 0, DEPTH, False), arrival(i, 0))
            return carry

        lax.fori_loop(0, lefts // 2, tile, 0)
        x_rest(i, range(1, subs))
        x_own(i, 0, DEPTH)

    def y_values(ready, sends, spot, count):
        got = product((hy[0], hy[1]), split(jnp.concatenate([ready[n] for n in range(count)], axis=1)))
        for to in range(rights):
            for band in range(bands):
                top = to * out_y + band * BAND
                for n in range(count):
                    rows = pl.ds(pl.multiple_of((spot + n) * BAND, BAND), BAND)
                    sends[to, band, rows, :] = got[top:top + BAND, n * share_x:(n + 1) * share_x]

    def y_own(sends, spot, field, there, count):
        for band in range(bands):
            mine = sends[right, band, pl.ds(pl.multiple_of(spot * BAND, BAND), count * BAND), :]
            second[field, band, pl.ds(pl.multiple_of(there * BAND, BAND), count * BAND), :] = mine

    def y_step(i, z, count, sem):
        landed(first.at[i, pl.ds(z, count), pl.ds(0, (lefts - 1) * share_y), :], sem)
        field, spot = i // pieces, lax.rem(i, pieces) * DEPTH + z
        y_values(first.at[i, pl.ds(z, count)], send_b.at[field], spot, count)
        hosted = jnp.logical_and(gate, jnp.logical_and(i == 0, z == guest_z))
        direct = jnp.logical_or(end, jnp.logical_and(field < fields - 1, jnp.logical_not(hosted)))
        for k in range(half):
            @pl.when(direct)
            def _():
                copy_b(field, spot, count, crossing(k), 0).start()
        for k in range(half - 1):
            copy_b(field, spot, count, beside(k), 1).start()
        y_own(send_b.at[field], spot, field, right * share_z + spot, count)

    def guest_x():
        landed(raw_in, raw_sem.at[1])
        for c in range(size_x // LANES):
            cols = pl.ds(c * LANES, LANES)
            lines[0, pl.ds(0, SUB * share_y), cols], lines[1, pl.ds(0, SUB * share_y), cols] = split(raw_in[:, cols])

        def tile(j, carry):
            x_tile(guest_a, j, 0, SUB, False)
            return carry

        lax.fori_loop(0, lefts // 2, tile, 0)
        for k in range(lefts - 1, 0, -1):
            copy_guest_a(partner(k)).start()
        guest_first[:, pl.ds(pl.multiple_of(left * share_y, share_y), share_y), :] = guest_a[left]

    def guest_y():
        landed(guest_first.at[:, pl.ds(0, (lefts - 1) * share_y), :], guest_sem.at[1])
        y_values(guest_first, guest_b, 0, SUB)
        for k in range(half - 1):
            copy_guest_b(beside(k)).start()
        y_own(guest_b, 0, 0, twin * share_z + guest_z, SUB)

    fetch(1)
    tables[0].wait()
    x_open()
    tables[1].wait()
    tables[2].wait()
    for symbol in symbols:
        symbol.start()
    for z in range(SUB):
        y_step(0, z, 1, arrival(2 * z, 0))

    def step(i, carry):
        @pl.when(i + 1 < chunks)
        def _():
            x_step(i + 1)

        @pl.when(jnp.logical_and(gate, i == min(1, chunks - 1)))
        def _():
            guest_x()

        def part(sub, carry):
            y_step(i, sub * SUB, SUB, arrival(i, sub))
            return carry

        lax.fori_loop(1, subs, part, 0)

        @pl.when(jnp.logical_and(gate, i == min(2, chunks - 1)))
        def _():
            guest_y()

        @pl.when(i + 1 < chunks)
        def _():
            y_step(i + 1, 0, SUB, arrival(i + 1, 0))

        return carry

    lax.fori_loop(0, chunks, step, 0)

    @pl.when(jnp.logical_not(end))
    def _():
        for n in range(2 * bands):
            for k in range(half):
                copy_c(n, crossing(k)).start()

    for symbol in symbols:
        symbol.wait()
    column = jnp.broadcast_to(sym_x[pl.ds(left, 1), :], (size_z, share_x)).T
    base[...] = column + sym_z[...]
    table[...] = hz[...]
    for y in range(SUBLANES):
        scale[y] = lax.rsqrt(base[...] + sym_y[right * out_y + out_y - SUBLANES + y])

    def held_in(band, part):
        block = second.at[fields - 1, band].reshape(size_z, BAND, share_x)
        rows = pl.ds(part % 2 * SUBLANES, SUBLANES)
        landed(block.at[pl.ds(0, (half - 1) * share_z), rows, :], rc_sem.at[part])

    def z_step(n, carry):
        field, part = n // (2 * bands), lax.rem(n, 2 * bands)
        band, top = part // 2, lax.rem(part, 2) * SUBLANES
        hosting = jnp.logical_and(gate, field == 0)
        everything = (rights - 1) * share_z
        for planes, chosen in (
            (everything - SUB, hosting),
            (everything, jnp.logical_and(field < fields - 1, jnp.logical_not(hosting))),
            (half * share_z, field == fields - 1),
        ):
            @pl.when(jnp.logical_and(part == 0, chosen))
            def _():
                landed(second.at[field, :, pl.ds(0, planes * BAND), :], rb_sem.at[field])

        @pl.when(field == fields - 1)
        def _():
            held_in(band, part)

        def line(step, carry):
            y = top + step
            plane = second[field, band, pl.ds(y, size_z, stride=BAND), :].T
            got = jnp.dot(jnp.concatenate(split(plane), axis=1), hz[...], preferred_element_type=jnp.float32)
            got = (got[:, :size_z] + got[:, size_z:]) * lax.rsqrt(base[...] + sym_y[right * out_y + band * BAND + y])
            out[field, band, pl.ds(y, share_x, stride=BAND), :] = got
            return carry

        lax.fori_loop(0, SUBLANES, line, 0, unroll=4)
        return carry

    lax.fori_loop(0, fields * bands * 2 - 1, z_step, 0)
    held_in(bands - 1, 2 * bands - 1)
    block = second.at[fields - 1, bands - 1].reshape(size_z, BAND, share_x)
    tail[...] = block[:, BAND - SUBLANES:, :].reshape(size_z * SUBLANES, share_x)
    landed(send_a.at[:, pl.ds(0, lefts - 1)], sa_sem)
    landed(send_b.at[0, pl.ds(0, half - 1)], sb_sem.at[1])
    landed(send_b.at[pl.ds(1, fields - 1), pl.ds(0, rights - 1)], sb_sem.at[2])

    @pl.when(gate)
    def _():
        landed(send_b.at[0, pl.ds(0, half), :, pl.ds(0, (share_z - SUB) * BAND), :], sb_sem.at[0])
        landed(raw_out, raw_sem.at[0])
        landed(guest_a.at[pl.ds(0, lefts - 1)], guest_sem.at[0])
        landed(guest_b.at[pl.ds(0, half - 1)], guest_sem.at[2])

    @pl.when(jnp.logical_not(gate))
    def _():
        landed(send_b.at[0, pl.ds(0, half)], sb_sem.at[0])


def flush_kernel(ready, tail, scale, table, out, made, sem):
    fields, bands, share_x, _, size_z = ready.shape
    for n in range(fields * bands):
        field, band = n // bands, n % bands
        rows = BAND if n < fields * bands - 1 else BAND - SUBLANES
        there = out.at[field, :, pl.ds(band * BAND, rows), :]
        pltpu.make_async_copy(ready.at[field, band, :, pl.ds(0, rows), :], there, sem).start()
    for y in range(SUBLANES):
        plane = tail[pl.ds(y, size_z, stride=SUBLANES), :].T
        got = jnp.dot(jnp.concatenate(split(plane), axis=1), table[...], preferred_element_type=jnp.float32)
        made[pl.ds(y, share_x, stride=SUBLANES), :] = (got[:, :size_z] + got[:, size_z:]) * scale[y]
    there = out.at[fields - 1, :, pl.ds(bands * BAND - SUBLANES, SUBLANES), :]
    pltpu.make_async_copy(made.reshape(share_x, SUBLANES, size_z), there, sem).start()
    landed(out, sem)


def near_local(lefts, rights, tracer, symbol_x, symbol_y, symbol_z):
    fields, size_x, share_y, share_z = tracer.shape
    size_y, size_z = symbol_y.shape[0], symbol_z.shape[0]
    share_x, out_y = size_x // lefts, size_y // rights
    bands = out_y // BAND
    chunks = fields * (share_z // DEPTH)
    data = jnp.transpose(tracer, (0, 2, 3, 1))
    factors, inner = factors_of(size_x)
    hy, hz = small_table(size_y), stacked(small_table(size_z))
    f32, bf16 = jnp.float32, jnp.bfloat16
    any_space = pl.BlockSpec(memory_space=pl.ANY)
    vmem = pl.BlockSpec(memory_space=pltpu.VMEM)
    dma = pltpu.SemaphoreType.DMA
    ready, *others = pl.pallas_call(
        functools.partial(near_kernel, lefts, rights, inner),
        name="modes",
        out_shape=[
            pltpu.VMEM((fields, bands, share_x * BAND, size_z), f32),
            pltpu.VMEM((size_z * SUBLANES, share_x), f32),
            pltpu.VMEM((SUBLANES, share_x, size_z), f32),
            pltpu.VMEM(hz.shape, bf16),
        ],
        in_specs=[any_space] * 7,
        out_specs=[vmem] * 4,
        scratch_shapes=[
            pltpu.VMEM((chunks, DEPTH, size_y, share_x), f32),
            pltpu.VMEM((fields, bands, size_z * BAND, share_x), f32),
            pltpu.VMEM((2, size_x // LANES, share_y * DEPTH, LANES), f32),
            pltpu.VMEM(factors.shape, f32),
            pltpu.VMEM((2, size_x, size_x), bf16),
            pltpu.VMEM(hy.shape, bf16),
            pltpu.VMEM(hz.shape, bf16),
            pltpu.VMEM((2, share_y * DEPTH, size_x), bf16),
            pltpu.VMEM((chunks, lefts, DEPTH, share_y, share_x), f32),
            pltpu.VMEM((fields, rights, bands, share_z * BAND, share_x), f32),
            pltpu.VMEM((share_x, size_z), f32),
            pltpu.VMEM((lefts, share_x), f32),
            pltpu.VMEM((1, size_z), f32),
            pltpu.SMEM((size_y,), f32),
            pltpu.VMEM((SUB * share_y, size_x), f32),
            pltpu.VMEM((SUB * share_y, size_x), f32),
            pltpu.VMEM((lefts, SUB, share_y, share_x), f32),
            pltpu.VMEM((SUB, size_y, share_x), f32),
            pltpu.VMEM((rights, bands, SUB * BAND, share_x), f32),
            dma((2,)),
            dma((3,)),
            dma,
            dma((SLOTS, DEPTH // SUB)),
            dma((3,)),
            dma((fields,)),
            dma((2 * bands,)),
            dma((2,)),
            dma((3,)),
        ],
        compiler_params=pltpu.CompilerParams(
            collective_id=0, has_side_effects=True, vmem_limit_bytes=NEAR_LIMIT
        ),
    )(data, factors, hy, hz, symbol_x.reshape(lefts, share_x), symbol_z.reshape(1, size_z), symbol_y)
    return pl.pallas_call(
        flush_kernel,
        name="flush",
        out_shape=jax.ShapeDtypeStruct((fields, share_x, out_y, size_z), f32),
        in_specs=[vmem] * 4,
        out_specs=any_space,
        scratch_shapes=[pltpu.VMEM((share_x * SUBLANES, size_z), f32), dma],
        compiler_params=pltpu.CompilerParams(vmem_limit_bytes=2**21),
    )(ready.reshape(fields, bands, share_x, BAND, size_z), *others)


def far_local(lefts, rights, tracer, symbol_x, symbol_y, symbol_z):
    fields, size_x, share_y, share_z = tracer.shape
    size_y, size_z = symbol_y.shape[0], symbol_z.shape[0]
    share_x, out_y = size_x // lefts, size_y // rights
    bands = out_y // BAND
    chunks = fields * (share_z // DEPTH)
    data = jnp.transpose(tracer, (0, 2, 3, 1))
    part_x = lax.dynamic_slice_in_dim(symbol_x, lax.axis_index("left") * share_x, share_x)
    base = part_x[:, None] + symbol_z[None, :]
    f32 = jnp.float32
    any_space = pl.BlockSpec(memory_space=pl.ANY)
    vmem = pl.BlockSpec(memory_space=pltpu.VMEM)
    landing = [(chunks, size_y * DEPTH, share_x), (fields, bands, size_z * BAND, share_x)]
    near = 4 * sum(map(math.prod, landing)) <= NEAR_BYTES
    staging = [] if near else [
        pltpu.VMEM((size_y * DEPTH, share_x), f32), pltpu.VMEM((size_z * BAND, share_x), f32)
    ]
    results = pl.pallas_call(
        functools.partial(far_kernel, lefts, rights, near),
        name="modes",
        out_shape=[
            jax.ShapeDtypeStruct((fields, bands, size_z // LANES, share_x * BAND, LANES), f32),
            *([] if near else [jax.ShapeDtypeStruct(shape, f32) for shape in landing]),
        ],
        in_specs=[any_space, vmem, vmem, vmem, vmem, pl.BlockSpec(memory_space=pltpu.SMEM)],
        out_specs=[any_space] * (1 if near else 3),
        scratch_shapes=[
            *([pltpu.VMEM(shape, f32) for shape in landing] if near else []),
            pltpu.VMEM((2, share_y, DEPTH, size_x), f32),
            pltpu.VMEM((2, share_y * DEPTH, size_x), jnp.bfloat16),
            pltpu.VMEM((SLOTS, lefts, share_y * DEPTH, share_x), f32),
            pltpu.VMEM((chunks, rights, bands, DEPTH * BAND, share_x), f32),
            pltpu.VMEM((2, size_z // LANES, share_x * BAND, LANES), f32),
            pltpu.SemaphoreType.DMA((2,)),
            pltpu.SemaphoreType.DMA((SLOTS, lefts)),
            pltpu.SemaphoreType.DMA((chunks, lefts)),
            pltpu.SemaphoreType.DMA,
            pltpu.SemaphoreType.DMA((chunks, rights, bands)),
            pltpu.SemaphoreType.DMA((chunks, rights, bands)),
            pltpu.SemaphoreType.DMA,
            pltpu.SemaphoreType.DMA((2,)),
            *staging,
        ],
        compiler_params=pltpu.CompilerParams(
            collective_id=0, has_side_effects=True, vmem_limit_bytes=60 * 2**20
        ),
    )(data, halves_of(transform_table(size_x)), small_table(size_y), small_table(size_z), base, symbol_y)
    out = results[0].reshape(fields, bands, size_z // LANES, share_x, BAND, LANES)
    return jnp.transpose(out, (0, 3, 1, 4, 2, 5)).reshape(fields, share_x, out_y, size_z)


def local(lefts, rights, tracer, symbol_x, symbol_y, symbol_z):
    fields, size_x, share_y, share_z = tracer.shape
    size_z, share_x = symbol_z.shape[0], size_x // lefts
    size = 4 * math.prod(tracer.shape)
    fits = size <= NEAR_BYTES // 2 and share_x == LANES and size_z == LANES and rights % 2 == 0
    fits = fits and rights > 2 and fields > 1
    run = near_local if fits else far_local
    return run(lefts, rights, tracer, symbol_x, symbol_y, symbol_z)


def solution(mesh):
    return jax.shard_map(
        functools.partial(local, mesh.shape["left"], mesh.shape["right"]),
        mesh=mesh,
        in_specs=(P(None, None, "left", "right"), P(), P(), P()),
        out_specs=P(None, "left", "right", None),
        check_vma=False,
    )
```

```python
import functools
import math

import jax
import jax.numpy as jnp
import numpy as np
from jax import lax
from jax.experimental import pallas as pl
from jax.experimental.pallas import tpu as pltpu
from jax.sharding import PartitionSpec as P

MESH = pl.DeviceIdType.MESH
NEAR_BYTES = 20 * 2**20
DEPTH = 8
BAND = 16
SUBLANES = 8
LANES = 128
SLOTS = 3
NEAR_LIMIT = 50 * 2**20
SUB = 2


def transform_table(count):
    inner = 1 << ((count.bit_length() - 1) // 2)
    outer = count // inner
    column = np.arange(count)

    def angle(row):
        return 2.0 * np.pi / count * (row[:, None] * column[None, :] % count)

    low = angle(np.arange(inner))
    high = angle(np.arange(outer) * inner)
    scale = count ** (-0.5)
    cos_low = jnp.asarray(np.cos(low), jnp.float32)[None]
    sin_low = jnp.asarray(np.sin(low), jnp.float32)[None]
    plus = jnp.asarray((np.cos(high) + np.sin(high)) * scale, jnp.float32)[:, None]
    minus = jnp.asarray((np.cos(high) - np.sin(high)) * scale, jnp.float32)[:, None]
    return (cos_low * plus + sin_low * minus).reshape(count, count)


def factors_of(count):
    inner = 1 << ((count.bit_length() - 1) // 2)
    outer = count // inner
    column = np.arange(count)

    def angle(row):
        return 2.0 * np.pi / count * (row[:, None] * column[None, :] % count)

    low = angle(np.arange(inner))
    high = angle(np.arange(outer) * inner)
    scale = count ** (-0.5)
    low = np.stack([np.cos(low), np.sin(low)])
    high = np.stack([np.cos(high) + np.sin(high), np.cos(high) - np.sin(high)]) * scale
    rows = max(inner, outer)
    padded = [np.pad(part, ((0, 0), (0, rows - part.shape[1]), (0, 0))) for part in (low, high)]
    return jnp.asarray(np.concatenate(padded), jnp.float32), inner


def halves_of(table):
    upper = lax.reduce_precision(table, 8, 7)
    return jnp.stack([upper.astype(jnp.bfloat16), (table - upper).astype(jnp.bfloat16)])


def small_table(count):
    rank = np.arange(count)
    angle = 2.0 * np.pi / count * (rank[:, None] * rank[None, :] % count)
    table = ((np.cos(angle) + np.sin(angle)) * count ** (-0.5)).astype(np.float32)
    upper = table.astype(jnp.bfloat16)
    return jnp.asarray(np.stack([upper, (table - upper.astype(np.float32)).astype(jnp.bfloat16)]))


def split(values):
    upper = values.astype(jnp.bfloat16)
    return upper, (values - upper.astype(jnp.float32)).astype(jnp.bfloat16)


def product(a, b):
    dot = functools.partial(jnp.dot, preferred_element_type=jnp.float32)
    return dot(a[0], b[0]) + (dot(a[0], b[1]) + dot(a[1], b[0]))


def landed(ref, sem):
    pltpu.make_async_copy(ref, ref, sem).wait()


def far_kernel(lefts, rights, near, data, hx, hy, hz, base, sym_y, out, *rest):
    (first, second, dbuf, lines, send_a, send_b, obuf,
     d_sem, sa_sem, ra_sem, y_sem, sb_sem, rb_sem, z_sem, o_sem, *staging) = rest
    fields, share_y, share_z, _ = data.shape
    size_y, size_z = hy.shape[1], hz.shape[1]
    share_x = base.shape[0]
    bands = out.shape[1]
    pieces = share_z // DEPTH
    chunks = fields * pieces
    rows = share_y * DEPTH
    flat = DEPTH * BAND
    out_y = bands * BAND
    left, right = lax.axis_index("left"), lax.axis_index("right")

    def load(i):
        source = data.at[i // pieces, :, pl.ds(lax.rem(i, pieces) * DEPTH, DEPTH), :]
        return pltpu.make_async_copy(source, dbuf.at[lax.rem(i, 2)], d_sem.at[lax.rem(i, 2)])

    load(0).start()

    barrier = pltpu.get_barrier_semaphore()
    for k in range(1, lefts):
        pl.semaphore_signal(barrier, inc=1, device_id=(lax.rem(left + k, lefts), right), device_id_type=MESH)
    for k in range(1, rights):
        pl.semaphore_signal(barrier, inc=1, device_id=(left, lax.rem(right + k, rights)), device_id_type=MESH)
    pl.semaphore_wait(barrier, lefts + rights - 2)

    def copy_a(i, to):
        slot = lax.rem(i, SLOTS)
        return pltpu.make_async_remote_copy(
            src_ref=send_a.at[slot, to],
            dst_ref=first.at[i, pl.ds(left * rows, rows)],
            send_sem=sa_sem.at[slot, to],
            recv_sem=ra_sem.at[i, left],
            device_id=(to, right),
            device_id_type=MESH,
        )

    def copy_b(i, to, band):
        spot = right * share_z + lax.rem(i, pieces) * DEPTH
        return pltpu.make_async_remote_copy(
            src_ref=send_b.at[i, to, band],
            dst_ref=second.at[i // pieces, band, pl.ds(spot * BAND, flat)],
            send_sem=sb_sem.at[i, to, band],
            recv_sem=rb_sem.at[i, right, band],
            device_id=(left, to),
            device_id_type=MESH,
        )

    def sent_a(i):
        for k in range(1, lefts):
            copy_a(i, lax.rem(left + k, lefts)).wait_send()

    def x_step(i):
        load(i).wait()

        @pl.when(i + 1 < chunks)
        def _():
            load(i + 1).start()

        @pl.when(i >= SLOTS)
        def _():
            sent_a(i - SLOTS)

        slot = lax.rem(i, SLOTS)
        lines[0], lines[1] = split(dbuf[lax.rem(i, 2)].reshape(rows, hx.shape[1]))

        def tile(j, carry):
            cols = pl.ds(pl.multiple_of(j * 2 * share_x, 2 * share_x), 2 * share_x)
            got = product((lines[0], lines[1]), (hx[0, :, cols], hx[1, :, cols]))
            send_a[slot, 2 * j] = got[:, :share_x]
            send_a[slot, 2 * j + 1] = got[:, share_x:]
            return carry

        lax.fori_loop(0, lefts // 2, tile, 0)
        for k in range(1, lefts):
            copy_a(i, lax.rem(left + k, lefts)).start()
        pltpu.make_async_copy(
            send_a.at[slot, left], first.at[i, pl.ds(left * rows, rows)], ra_sem.at[i, left]
        ).start()

    def y_step(i):
        for k in range(lefts):
            landed(first.at[i, pl.ds(k * rows, rows)], ra_sem.at[i, k])
        if near:
            block = first.at[i]
        else:
            block = staging[0]
            fetch = pltpu.make_async_copy(first.at[i], block, y_sem)
            fetch.start()
            fetch.wait()
        for z in range(0, DEPTH, 2):
            pair = jnp.concatenate(
                [block[pl.ds(z, size_y, stride=DEPTH), :], block[pl.ds(z + 1, size_y, stride=DEPTH), :]], axis=1
            )
            got = product((hy[0], hy[1]), split(pair))
            for to in range(rights):
                for band in range(bands):
                    top = to * out_y + band * BAND
                    for half in range(2):
                        send_b[i, to, band, (z + half) * BAND:(z + half + 1) * BAND, :] = (
                            got[top:top + BAND, half * share_x:(half + 1) * share_x]
                        )
        for band in range(bands):
            for k in range(rights):
                to = jnp.where(right < rights // 2, rights - 1 - k, k)

                @pl.when(to != right)
                def _():
                    copy_b(i, to, band).start()

            spot = right * share_z + lax.rem(i, pieces) * DEPTH
            pltpu.make_async_copy(
                send_b.at[i, right, band],
                second.at[i // pieces, band, pl.ds(spot * BAND, flat)],
                rb_sem.at[i, right, band],
            ).start()

    def step(i, carry):
        @pl.when(i < chunks)
        def _():
            x_step(i)

        @pl.when(i >= 1)
        def _():
            y_step(i - 1)

        return carry

    lax.fori_loop(0, chunks + 1, step, 0)

    def put(n):
        slot = lax.rem(n, 2)
        return pltpu.make_async_copy(obuf.at[slot], out.at[n // bands, lax.rem(n, bands)], o_sem.at[slot])

    def z_step(n, carry):
        field, band = n // bands, lax.rem(n, bands)
        slot = lax.rem(n, 2)

        def arrive(p, carry):
            for k in range(rights):
                spot = k * share_z + p * DEPTH
                landed(second.at[field, band, pl.ds(spot * BAND, flat)], rb_sem.at[field * pieces + p, k, band])
            return carry

        lax.fori_loop(0, pieces, arrive, 0)
        if near:
            block = second.at[field, band]
        else:
            block = staging[1]
            fetch = pltpu.make_async_copy(second.at[field, band], block, z_sem)
            fetch.start()
            fetch.wait()

        @pl.when(n >= 2)
        def _():
            put(n - 2).wait()

        def line(y, carry):
            plane = block[pl.ds(y, size_z, stride=BAND), :].T
            got = product(split(plane), (hz[0], hz[1]))
            got = got * lax.rsqrt(base[...] + sym_y[right * out_y + band * BAND + y])
            for t in range(size_z // LANES):
                obuf[slot, t, pl.ds(y, share_x, stride=BAND), :] = got[:, t * LANES:(t + 1) * LANES]
            return carry

        lax.fori_loop(0, BAND, line, 0, unroll=2)
        put(n).start()
        return carry

    steps = fields * bands
    lax.fori_loop(0, steps, z_step, 0)

    def drain_a(i, carry):
        sent_a(i)
        return carry

    lax.fori_loop(max(chunks - SLOTS, 0), chunks, drain_a, 0)

    def drain_b(i, carry):
        for k in range(1, rights):
            for band in range(bands):
                copy_b(i, lax.rem(right + k, rights), band).wait_send()
        return carry

    lax.fori_loop(0, chunks, drain_b, 0)
    for n in range(max(steps - 2, 0), steps):
        put(n).wait()


def stacked(halves):
    upper, lower = halves[0], halves[1]
    return jnp.concatenate(
        [jnp.concatenate([upper, lower], axis=1), jnp.concatenate([upper, jnp.zeros_like(lower)], axis=1)], axis=0
    )


def near_kernel(lefts, rights, inner, data, factors_in, hy_in, hz_in, x_in, z_in, y_in, out, tail, scale, table, *rest):
    (first, second, dbuf, factors, hx, hy, hz, lines, send_a, send_b, base,
     sym_x, sym_z, sym_y, raw_out, raw_in, guest_a, guest_first, guest_b,
     d_sem, t_sem, sa_sem, ra_sem, sb_sem, rb_sem, rc_sem, raw_sem, guest_sem) = rest
    fields, share_y, share_z, size_x = data.shape
    size_y = hy.shape[1]
    share_x, size_z = base.shape
    bands = out.shape[1]
    pieces = share_z // DEPTH
    chunks = fields * pieces
    subs = DEPTH // SUB
    out_y = bands * BAND
    half = rights // 2
    left, right = lax.axis_index("left"), lax.axis_index("right")

    def load(i):
        slot = lax.rem(i, 2)
        planes = pl.ds(lax.rem(i, pieces) * DEPTH, DEPTH)
        return [pltpu.make_async_copy(
            data.at[i // pieces, :, planes, pl.ds(c * LANES, LANES)],
            dbuf.at[slot, c].reshape(share_y, DEPTH, LANES),
            d_sem.at[slot],
        ) for c in range(size_x // LANES)]

    def fetch(i):
        for copy in load(i):
            copy.start()

    def copies(pairs):
        return [pltpu.make_async_copy(a, b, t_sem.at[n]) for n, (a, b) in enumerate(pairs)]

    tables = copies([(factors_in, factors), (hy_in, hy), (hz_in, hz)])
    symbols = copies([(x_in, sym_x), (z_in, sym_z), (y_in, sym_y)])
    tables[0].start()
    fetch(0)
    tables[1].start()
    tables[2].start()

    barrier = pltpu.get_barrier_semaphore()
    for k in range(1, lefts):
        pl.semaphore_signal(barrier, inc=1, device_id=(lax.rem(left + k, lefts), right), device_id_type=MESH)
    for k in range(1, rights):
        pl.semaphore_signal(barrier, inc=1, device_id=(left, lax.rem(right + k, rights)), device_id_type=MESH)

    def copy_a(i, z, count, to, sem):
        return pltpu.make_async_remote_copy(
            src_ref=send_a.at[i, to, pl.ds(z, count)],
            dst_ref=first.at[i, pl.ds(z, count), pl.ds(left * share_y, share_y), :],
            send_sem=sa_sem,
            recv_sem=sem,
            device_id=(to, right),
            device_id_type=MESH,
        )

    def copy_b(field, spot, count, to, kind):
        return pltpu.make_async_remote_copy(
            src_ref=send_b.at[field, to, :, pl.ds(spot * BAND, count * BAND), :],
            dst_ref=second.at[field, :, pl.ds((right * share_z + spot) * BAND, count * BAND), :],
            send_sem=sb_sem.at[jnp.where(field == 0, kind, 2)],
            recv_sem=rb_sem.at[field],
            device_id=(left, to),
            device_id_type=MESH,
        )

    def copy_c(n, to):
        band, rows = n // 2, pl.ds(n % 2 * SUBLANES, SUBLANES)
        there = second.at[fields - 1, band].reshape(size_z, BAND, share_x)
        return pltpu.make_async_remote_copy(
            src_ref=send_b.at[fields - 1, to, band].reshape(share_z, BAND, share_x).at[:, rows, :],
            dst_ref=there.at[pl.ds(right * share_z, share_z), rows, :],
            send_sem=sb_sem.at[2],
            recv_sem=rc_sem.at[n],
            device_id=(left, to),
            device_id_type=MESH,
        )

    lower = right < half
    rank = jnp.where(lower, right, rights - 1 - right)
    end = rank == 0
    gate = rank == half - 1
    twin = rights - 1 - right
    guest_z = DEPTH - SUB

    def mirrored(t):
        return jnp.where(lower, t, rights - 1 - t)

    def crossing(k):
        return mirrored(jnp.where(end, rights - 1 - k, half + k))

    def beside(k):
        return mirrored(lax.rem(rank + 1 + k, half))

    def raw():
        return pltpu.make_async_remote_copy(
            src_ref=raw_out,
            dst_ref=raw_in,
            send_sem=raw_sem.at[0],
            recv_sem=raw_sem.at[1],
            device_id=(left, twin),
            device_id_type=MESH,
        )

    def copy_guest_a(to):
        return pltpu.make_async_remote_copy(
            src_ref=guest_a.at[to],
            dst_ref=guest_first.at[:, pl.ds(left * share_y, share_y), :],
            send_sem=guest_sem.at[0],
            recv_sem=guest_sem.at[1],
            device_id=(to, right),
            device_id_type=MESH,
        )

    def copy_guest_b(to):
        spot = (twin * share_z + guest_z) * BAND
        return pltpu.make_async_remote_copy(
            src_ref=guest_b.at[to],
            dst_ref=second.at[0, :, pl.ds(spot, SUB * BAND), :],
            send_sem=guest_sem.at[2],
            recv_sem=rb_sem.at[0],
            device_id=(left, to),
            device_id_type=MESH,
        )

    def widen(cols):
        for top in range(size_x // inner):
            plus, minus = factors[2, top:top + 1, cols], factors[3, top:top + 1, cols]
            made = factors[0, :inner, cols] * plus + factors[1, :inner, cols] * minus
            rows = pl.ds(top * inner, inner)
            hx[0, rows, cols], hx[1, rows, cols] = split(made)

    def arrival(i, sub):
        return ra_sem.at[lax.rem(i, SLOTS), sub]

    def partner(k):
        return left ^ k if lefts & (lefts - 1) == 0 else lax.rem(left + k, lefts)

    def x_tile(sends, j, z, count, opening):
        pair = partner(lefts - 1 - 2 * j) // 2
        cols = pl.ds(pl.multiple_of(pair * 2 * share_x, 2 * share_x), 2 * share_x)
        if opening:
            widen(cols)
        rows = pl.ds(z * share_y, count * share_y)
        got = product((lines[0, rows, :], lines[1, rows, :]), (hx[0, :, cols], hx[1, :, cols]))
        for core in range(2):
            part = got[:, core * share_x:(core + 1) * share_x].reshape(count, share_y, share_x)
            sends[2 * pair + core, z:z + count] = part
        return pair

    def x_split(i, planes):
        slot = lax.rem(i, 2)
        for c in range(size_x // LANES):
            cols = pl.ds(c * LANES, LANES)
            for z in planes:
                rows = pl.ds(z * share_y, share_y)
                lines[0, rows, cols], lines[1, rows, cols] = split(dbuf[slot, c, pl.ds(z, share_y, stride=DEPTH), :])

    def x_send(i, z, count, pair, sem):
        for core in range(2):
            @pl.when(2 * pair + core != left)
            def _():
                copy_a(i, z, count, 2 * pair + core, sem).start()

    def x_rest(i, subs_left):
        for sub in subs_left:
            for k in range(lefts - 1, 0, -1):
                copy_a(i, sub * SUB, SUB, partner(k), arrival(i, sub)).start()

    def x_own(i, z, count):
        mine = pl.ds(pl.multiple_of(left * share_y, share_y), share_y)
        first[i, z:z + count, mine, :] = send_a[i, left, z:z + count]

    def x_open():
        landed(dbuf.at[0], d_sem.at[0])
        x_split(0, range(SUB))
        for c in range(size_x // LANES):
            for z in range(SUB):
                line = dbuf[0, c, pl.ds(guest_z + z, share_y, stride=DEPTH), :]
                raw_out[z * share_y:(z + 1) * share_y, c * LANES:(c + 1) * LANES] = line
        pair = x_tile(send_a.at[0], 0, 0, SUB, True)
        pl.semaphore_wait(barrier, lefts + rights - 2)

        @pl.when(gate)
        def _():
            raw().start()

        x_send(0, 0, 1, pair, arrival(0, 0))

        def tile(j, carry):
            x_send(0, 0, 1, x_tile(send_a.at[0], j, 0, SUB, True), arrival(0, 0))
            return carry

        lax.fori_loop(1, lefts // 2, tile, 0)
        for z in range(1, SUB):
            for k in range(lefts - 1, 0, -1):
                copy_a(0, z, 1, partner(k), arrival(2 * z, 0)).start()
        x_own(0, 0, SUB)
        x_split(0, range(SUB, DEPTH))

        def more(j, carry):
            x_send(0, SUB, SUB, x_tile(send_a.at[0], j, SUB, DEPTH - SUB, False), arrival(0, 1))
            return carry

        lax.fori_loop(0, lefts // 2, more, 0)
        x_rest(0, range(2, subs))
        x_own(0, SUB, DEPTH - SUB)
        fetch(2)

    def x_step(i):
        slot = lax.rem(i, 2)
        landed(dbuf.at[slot], d_sem.at[slot])
        x_split(i, range(DEPTH))

        @pl.when(i + 2 < chunks)
        def _():
            fetch(i + 2)

        def tile(j, carry):
            x_send(i, 0, SUB, x_tile(send_a.at[i], j, 0, DEPTH, False), arrival(i, 0))
            return carry

        lax.fori_loop(0, lefts // 2, tile, 0)
        x_rest(i, range(1, subs))
        x_own(i, 0, DEPTH)

    def y_values(ready, sends, spot, count):
        got = product((hy[0], hy[1]), split(jnp.concatenate([ready[n] for n in range(count)], axis=1)))
        for to in range(rights):
            for band in range(bands):
                top = to * out_y + band * BAND
                for n in range(count):
                    rows = pl.ds(pl.multiple_of((spot + n) * BAND, BAND), BAND)
                    sends[to, band, rows, :] = got[top:top + BAND, n * share_x:(n + 1) * share_x]

    def y_own(sends, spot, field, there, count):
        for band in range(bands):
            mine = sends[right, band, pl.ds(pl.multiple_of(spot * BAND, BAND), count * BAND), :]
            second[field, band, pl.ds(pl.multiple_of(there * BAND, BAND), count * BAND), :] = mine

    def y_step(i, z, count, sem):
        landed(first.at[i, pl.ds(z, count), pl.ds(0, (lefts - 1) * share_y), :], sem)
        field, spot = i // pieces, lax.rem(i, pieces) * DEPTH + z
        y_values(first.at[i, pl.ds(z, count)], send_b.at[field], spot, count)
        hosted = jnp.logical_and(gate, jnp.logical_and(i == 0, z == guest_z))
        direct = jnp.logical_or(end, jnp.logical_and(field < fields - 1, jnp.logical_not(hosted)))
        for k in range(half):
            @pl.when(direct)
            def _():
                copy_b(field, spot, count, crossing(k), 0).start()
        for k in range(half - 1):
            copy_b(field, spot, count, beside(k), 1).start()
        y_own(send_b.at[field], spot, field, right * share_z + spot, count)

    def guest_x():
        landed(raw_in, raw_sem.at[1])
        for c in range(size_x // LANES):
            cols = pl.ds(c * LANES, LANES)
            lines[0, pl.ds(0, SUB * share_y), cols], lines[1, pl.ds(0, SUB * share_y), cols] = split(raw_in[:, cols])

        def tile(j, carry):
            x_tile(guest_a, j, 0, SUB, False)
            return carry

        lax.fori_loop(0, lefts // 2, tile, 0)
        for k in range(lefts - 1, 0, -1):
            copy_guest_a(partner(k)).start()
        guest_first[:, pl.ds(pl.multiple_of(left * share_y, share_y), share_y), :] = guest_a[left]

    def guest_y():
        landed(guest_first.at[:, pl.ds(0, (lefts - 1) * share_y), :], guest_sem.at[1])
        y_values(guest_first, guest_b, 0, SUB)
        for k in range(half - 1):
            copy_guest_b(beside(k)).start()
        y_own(guest_b, 0, 0, twin * share_z + guest_z, SUB)

    fetch(1)
    tables[0].wait()
    x_open()
    tables[1].wait()
    tables[2].wait()
    for symbol in symbols:
        symbol.start()
    for z in range(SUB):
        y_step(0, z, 1, arrival(2 * z, 0))

    def step(i, carry):
        @pl.when(i + 1 < chunks)
        def _():
            x_step(i + 1)

        @pl.when(jnp.logical_and(gate, i == min(1, chunks - 1)))
        def _():
            guest_x()

        def part(sub, carry):
            y_step(i, sub * SUB, SUB, arrival(i, sub))
            return carry

        lax.fori_loop(1, subs, part, 0)

        @pl.when(jnp.logical_and(gate, i == min(2, chunks - 1)))
        def _():
            guest_y()

        @pl.when(i + 1 < chunks)
        def _():
            y_step(i + 1, 0, SUB, arrival(i + 1, 0))

        return carry

    lax.fori_loop(0, chunks, step, 0)

    @pl.when(jnp.logical_not(end))
    def _():
        for n in range(2 * bands):
            for k in range(half - 1, -1, -1):
                copy_c(n, crossing(k)).start()

    for symbol in symbols:
        symbol.wait()
    column = jnp.broadcast_to(sym_x[pl.ds(left, 1), :], (size_z, share_x)).T
    base[...] = column + sym_z[...]
    table[...] = hz[...]
    for y in range(SUBLANES):
        scale[y] = lax.rsqrt(base[...] + sym_y[right * out_y + out_y - SUBLANES + y])

    def held_in(band, part):
        block = second.at[fields - 1, band].reshape(size_z, BAND, share_x)
        rows = pl.ds(part % 2 * SUBLANES, SUBLANES)
        landed(block.at[pl.ds(0, (half - 1) * share_z), rows, :], rc_sem.at[part])

    def z_step(n, carry):
        field, part = n // (2 * bands), lax.rem(n, 2 * bands)
        band, top = part // 2, lax.rem(part, 2) * SUBLANES
        hosting = jnp.logical_and(gate, field == 0)
        everything = (rights - 1) * share_z
        for planes, chosen in (
            (everything - SUB, hosting),
            (everything, jnp.logical_and(field < fields - 1, jnp.logical_not(hosting))),
            (half * share_z, field == fields - 1),
        ):
            @pl.when(jnp.logical_and(part == 0, chosen))
            def _():
                landed(second.at[field, :, pl.ds(0, planes * BAND), :], rb_sem.at[field])

        @pl.when(field == fields - 1)
        def _():
            held_in(band, part)

        def line(step, carry):
            y = top + step
            plane = second[field, band, pl.ds(y, size_z, stride=BAND), :].T
            got = jnp.dot(jnp.concatenate(split(plane), axis=1), hz[...], preferred_element_type=jnp.float32)
            got = (got[:, :size_z] + got[:, size_z:]) * lax.rsqrt(base[...] + sym_y[right * out_y + band * BAND + y])
            out[field, band, pl.ds(y, share_x, stride=BAND), :] = got
            return carry

        lax.fori_loop(0, SUBLANES, line, 0, unroll=4)
        return carry

    lax.fori_loop(0, fields * bands * 2 - 1, z_step, 0)
    held_in(bands - 1, 2 * bands - 1)
    block = second.at[fields - 1, bands - 1].reshape(size_z, BAND, share_x)
    tail[...] = block[:, BAND - SUBLANES:, :].reshape(size_z * SUBLANES, share_x)
    landed(send_a.at[:, pl.ds(0, lefts - 1)], sa_sem)
    landed(send_b.at[0, pl.ds(0, half - 1)], sb_sem.at[1])
    landed(send_b.at[pl.ds(1, fields - 1), pl.ds(0, rights - 1)], sb_sem.at[2])

    @pl.when(gate)
    def _():
        landed(send_b.at[0, pl.ds(0, half), :, pl.ds(0, (share_z - SUB) * BAND), :], sb_sem.at[0])
        landed(raw_out, raw_sem.at[0])
        landed(guest_a.at[pl.ds(0, lefts - 1)], guest_sem.at[0])
        landed(guest_b.at[pl.ds(0, half - 1)], guest_sem.at[2])

    @pl.when(jnp.logical_not(gate))
    def _():
        landed(send_b.at[0, pl.ds(0, half)], sb_sem.at[0])


def flush_kernel(ready, tail, scale, table, out, made, sem):
    fields, bands, share_x, _, size_z = ready.shape
    for n in range(fields * bands):
        field, band = n // bands, n % bands
        rows = BAND if n < fields * bands - 1 else BAND - SUBLANES
        there = out.at[field, :, pl.ds(band * BAND, rows), :]
        pltpu.make_async_copy(ready.at[field, band, :, pl.ds(0, rows), :], there, sem).start()
    for y in range(SUBLANES):
        plane = tail[pl.ds(y, size_z, stride=SUBLANES), :].T
        got = jnp.dot(jnp.concatenate(split(plane), axis=1), table[...], preferred_element_type=jnp.float32)
        made[pl.ds(y, share_x, stride=SUBLANES), :] = (got[:, :size_z] + got[:, size_z:]) * scale[y]
    there = out.at[fields - 1, :, pl.ds(bands * BAND - SUBLANES, SUBLANES), :]
    pltpu.make_async_copy(made.reshape(share_x, SUBLANES, size_z), there, sem).start()
    landed(out, sem)


def near_local(lefts, rights, tracer, symbol_x, symbol_y, symbol_z):
    fields, size_x, share_y, share_z = tracer.shape
    size_y, size_z = symbol_y.shape[0], symbol_z.shape[0]
    share_x, out_y = size_x // lefts, size_y // rights
    bands = out_y // BAND
    chunks = fields * (share_z // DEPTH)
    data = jnp.transpose(tracer, (0, 2, 3, 1))
    factors, inner = factors_of(size_x)
    hy, hz = small_table(size_y), stacked(small_table(size_z))
    f32, bf16 = jnp.float32, jnp.bfloat16
    any_space = pl.BlockSpec(memory_space=pl.ANY)
    vmem = pl.BlockSpec(memory_space=pltpu.VMEM)
    dma = pltpu.SemaphoreType.DMA
    ready, *others = pl.pallas_call(
        functools.partial(near_kernel, lefts, rights, inner),
        name="modes",
        out_shape=[
            pltpu.VMEM((fields, bands, share_x * BAND, size_z), f32),
            pltpu.VMEM((size_z * SUBLANES, share_x), f32),
            pltpu.VMEM((SUBLANES, share_x, size_z), f32),
            pltpu.VMEM(hz.shape, bf16),
        ],
        in_specs=[any_space] * 7,
        out_specs=[vmem] * 4,
        scratch_shapes=[
            pltpu.VMEM((chunks, DEPTH, size_y, share_x), f32),
            pltpu.VMEM((fields, bands, size_z * BAND, share_x), f32),
            pltpu.VMEM((2, size_x // LANES, share_y * DEPTH, LANES), f32),
            pltpu.VMEM(factors.shape, f32),
            pltpu.VMEM((2, size_x, size_x), bf16),
            pltpu.VMEM(hy.shape, bf16),
            pltpu.VMEM(hz.shape, bf16),
            pltpu.VMEM((2, share_y * DEPTH, size_x), bf16),
            pltpu.VMEM((chunks, lefts, DEPTH, share_y, share_x), f32),
            pltpu.VMEM((fields, rights, bands, share_z * BAND, share_x), f32),
            pltpu.VMEM((share_x, size_z), f32),
            pltpu.VMEM((lefts, share_x), f32),
            pltpu.VMEM((1, size_z), f32),
            pltpu.SMEM((size_y,), f32),
            pltpu.VMEM((SUB * share_y, size_x), f32),
            pltpu.VMEM((SUB * share_y, size_x), f32),
            pltpu.VMEM((lefts, SUB, share_y, share_x), f32),
            pltpu.VMEM((SUB, size_y, share_x), f32),
            pltpu.VMEM((rights, bands, SUB * BAND, share_x), f32),
            dma((2,)),
            dma((3,)),
            dma,
            dma((SLOTS, DEPTH // SUB)),
            dma((3,)),
            dma((fields,)),
            dma((2 * bands,)),
            dma((2,)),
            dma((3,)),
        ],
        compiler_params=pltpu.CompilerParams(
            collective_id=0, has_side_effects=True, vmem_limit_bytes=NEAR_LIMIT
        ),
    )(data, factors, hy, hz, symbol_x.reshape(lefts, share_x), symbol_z.reshape(1, size_z), symbol_y)
    return pl.pallas_call(
        flush_kernel,
        name="flush",
        out_shape=jax.ShapeDtypeStruct((fields, share_x, out_y, size_z), f32),
        in_specs=[vmem] * 4,
        out_specs=any_space,
        scratch_shapes=[pltpu.VMEM((share_x * SUBLANES, size_z), f32), dma],
        compiler_params=pltpu.CompilerParams(vmem_limit_bytes=2**21),
    )(ready.reshape(fields, bands, share_x, BAND, size_z), *others)


def far_local(lefts, rights, tracer, symbol_x, symbol_y, symbol_z):
    fields, size_x, share_y, share_z = tracer.shape
    size_y, size_z = symbol_y.shape[0], symbol_z.shape[0]
    share_x, out_y = size_x // lefts, size_y // rights
    bands = out_y // BAND
    chunks = fields * (share_z // DEPTH)
    data = jnp.transpose(tracer, (0, 2, 3, 1))
    part_x = lax.dynamic_slice_in_dim(symbol_x, lax.axis_index("left") * share_x, share_x)
    base = part_x[:, None] + symbol_z[None, :]
    f32 = jnp.float32
    any_space = pl.BlockSpec(memory_space=pl.ANY)
    vmem = pl.BlockSpec(memory_space=pltpu.VMEM)
    landing = [(chunks, size_y * DEPTH, share_x), (fields, bands, size_z * BAND, share_x)]
    near = 4 * sum(map(math.prod, landing)) <= NEAR_BYTES
    staging = [] if near else [
        pltpu.VMEM((size_y * DEPTH, share_x), f32), pltpu.VMEM((size_z * BAND, share_x), f32)
    ]
    results = pl.pallas_call(
        functools.partial(far_kernel, lefts, rights, near),
        name="modes",
        out_shape=[
            jax.ShapeDtypeStruct((fields, bands, size_z // LANES, share_x * BAND, LANES), f32),
            *([] if near else [jax.ShapeDtypeStruct(shape, f32) for shape in landing]),
        ],
        in_specs=[any_space, vmem, vmem, vmem, vmem, pl.BlockSpec(memory_space=pltpu.SMEM)],
        out_specs=[any_space] * (1 if near else 3),
        scratch_shapes=[
            *([pltpu.VMEM(shape, f32) for shape in landing] if near else []),
            pltpu.VMEM((2, share_y, DEPTH, size_x), f32),
            pltpu.VMEM((2, share_y * DEPTH, size_x), jnp.bfloat16),
            pltpu.VMEM((SLOTS, lefts, share_y * DEPTH, share_x), f32),
            pltpu.VMEM((chunks, rights, bands, DEPTH * BAND, share_x), f32),
            pltpu.VMEM((2, size_z // LANES, share_x * BAND, LANES), f32),
            pltpu.SemaphoreType.DMA((2,)),
            pltpu.SemaphoreType.DMA((SLOTS, lefts)),
            pltpu.SemaphoreType.DMA((chunks, lefts)),
            pltpu.SemaphoreType.DMA,
            pltpu.SemaphoreType.DMA((chunks, rights, bands)),
            pltpu.SemaphoreType.DMA((chunks, rights, bands)),
            pltpu.SemaphoreType.DMA,
            pltpu.SemaphoreType.DMA((2,)),
            *staging,
        ],
        compiler_params=pltpu.CompilerParams(
            collective_id=0, has_side_effects=True, vmem_limit_bytes=60 * 2**20
        ),
    )(data, halves_of(transform_table(size_x)), small_table(size_y), small_table(size_z), base, symbol_y)
    out = results[0].reshape(fields, bands, size_z // LANES, share_x, BAND, LANES)
    return jnp.transpose(out, (0, 3, 1, 4, 2, 5)).reshape(fields, share_x, out_y, size_z)


def local(lefts, rights, tracer, symbol_x, symbol_y, symbol_z):
    fields, size_x, share_y, share_z = tracer.shape
    size_z, share_x = symbol_z.shape[0], size_x // lefts
    size = 4 * math.prod(tracer.shape)
    fits = size <= NEAR_BYTES // 2 and share_x == LANES and size_z == LANES and rights % 2 == 0
    fits = fits and rights > 2 and fields > 1
    run = near_local if fits else far_local
    return run(lefts, rights, tracer, symbol_x, symbol_y, symbol_z)


def solution(mesh):
    return jax.shard_map(
        functools.partial(local, mesh.shape["left"], mesh.shape["right"]),
        mesh=mesh,
        in_specs=(P(None, None, "left", "right"), P(), P(), P()),
        out_specs=P(None, "left", "right", None),
        check_vma=False,
    )
```

```python
import functools
import math

import jax
import jax.numpy as jnp
import numpy as np
from jax import lax
from jax.experimental import pallas as pl
from jax.experimental.pallas import tpu as pltpu
from jax.sharding import PartitionSpec as P

MESH = pl.DeviceIdType.MESH
NEAR_BYTES = 20 * 2**20
DEPTH = 8
BAND = 16
SUBLANES = 8
LANES = 128
SLOTS = 3
NEAR_LIMIT = 50 * 2**20
SUB = 2


def transform_table(count):
    inner = 1 << ((count.bit_length() - 1) // 2)
    outer = count // inner
    column = np.arange(count)

    def angle(row):
        return 2.0 * np.pi / count * (row[:, None] * column[None, :] % count)

    low = angle(np.arange(inner))
    high = angle(np.arange(outer) * inner)
    scale = count ** (-0.5)
    cos_low = jnp.asarray(np.cos(low), jnp.float32)[None]
    sin_low = jnp.asarray(np.sin(low), jnp.float32)[None]
    plus = jnp.asarray((np.cos(high) + np.sin(high)) * scale, jnp.float32)[:, None]
    minus = jnp.asarray((np.cos(high) - np.sin(high)) * scale, jnp.float32)[:, None]
    return (cos_low * plus + sin_low * minus).reshape(count, count)


def factors_of(count):
    inner = 1 << ((count.bit_length() - 1) // 2)
    outer = count // inner
    column = np.arange(count)

    def angle(row):
        return 2.0 * np.pi / count * (row[:, None] * column[None, :] % count)

    low = angle(np.arange(inner))
    high = angle(np.arange(outer) * inner)
    scale = count ** (-0.5)
    low = np.stack([np.cos(low), np.sin(low)])
    high = np.stack([np.cos(high) + np.sin(high), np.cos(high) - np.sin(high)]) * scale
    rows = max(inner, outer)
    padded = [np.pad(part, ((0, 0), (0, rows - part.shape[1]), (0, 0))) for part in (low, high)]
    return jnp.asarray(np.concatenate(padded), jnp.float32), inner


def halves_of(table):
    upper = lax.reduce_precision(table, 8, 7)
    return jnp.stack([upper.astype(jnp.bfloat16), (table - upper).astype(jnp.bfloat16)])


def small_table(count):
    rank = np.arange(count)
    angle = 2.0 * np.pi / count * (rank[:, None] * rank[None, :] % count)
    table = ((np.cos(angle) + np.sin(angle)) * count ** (-0.5)).astype(np.float32)
    upper = table.astype(jnp.bfloat16)
    return jnp.asarray(np.stack([upper, (table - upper.astype(np.float32)).astype(jnp.bfloat16)]))


def split(values):
    upper = values.astype(jnp.bfloat16)
    return upper, (values - upper.astype(jnp.float32)).astype(jnp.bfloat16)


def product(a, b):
    dot = functools.partial(jnp.dot, preferred_element_type=jnp.float32)
    return dot(a[0], b[0]) + (dot(a[0], b[1]) + dot(a[1], b[0]))


def landed(ref, sem):
    pltpu.make_async_copy(ref, ref, sem).wait()


def far_kernel(lefts, rights, near, data, hx, hy, hz, base, sym_y, out, *rest):
    (first, second, dbuf, lines, send_a, send_b, obuf,
     d_sem, sa_sem, ra_sem, y_sem, sb_sem, rb_sem, z_sem, o_sem, *staging) = rest
    fields, share_y, share_z, _ = data.shape
    size_y, size_z = hy.shape[1], hz.shape[1]
    share_x = base.shape[0]
    bands = out.shape[1]
    pieces = share_z // DEPTH
    chunks = fields * pieces
    rows = share_y * DEPTH
    flat = DEPTH * BAND
    out_y = bands * BAND
    left, right = lax.axis_index("left"), lax.axis_index("right")

    def load(i):
        source = data.at[i // pieces, :, pl.ds(lax.rem(i, pieces) * DEPTH, DEPTH), :]
        return pltpu.make_async_copy(source, dbuf.at[lax.rem(i, 2)], d_sem.at[lax.rem(i, 2)])

    load(0).start()

    barrier = pltpu.get_barrier_semaphore()
    for k in range(1, lefts):
        pl.semaphore_signal(barrier, inc=1, device_id=(lax.rem(left + k, lefts), right), device_id_type=MESH)
    for k in range(1, rights):
        pl.semaphore_signal(barrier, inc=1, device_id=(left, lax.rem(right + k, rights)), device_id_type=MESH)
    pl.semaphore_wait(barrier, lefts + rights - 2)

    def copy_a(i, to):
        slot = lax.rem(i, SLOTS)
        return pltpu.make_async_remote_copy(
            src_ref=send_a.at[slot, to],
            dst_ref=first.at[i, pl.ds(left * rows, rows)],
            send_sem=sa_sem.at[slot, to],
            recv_sem=ra_sem.at[i, left],
            device_id=(to, right),
            device_id_type=MESH,
        )

    def copy_b(i, to, band):
        spot = right * share_z + lax.rem(i, pieces) * DEPTH
        return pltpu.make_async_remote_copy(
            src_ref=send_b.at[i, to, band],
            dst_ref=second.at[i // pieces, band, pl.ds(spot * BAND, flat)],
            send_sem=sb_sem.at[i, to, band],
            recv_sem=rb_sem.at[i, right, band],
            device_id=(left, to),
            device_id_type=MESH,
        )

    def sent_a(i):
        for k in range(1, lefts):
            copy_a(i, lax.rem(left + k, lefts)).wait_send()

    def x_step(i):
        load(i).wait()

        @pl.when(i + 1 < chunks)
        def _():
            load(i + 1).start()

        @pl.when(i >= SLOTS)
        def _():
            sent_a(i - SLOTS)

        slot = lax.rem(i, SLOTS)
        lines[0], lines[1] = split(dbuf[lax.rem(i, 2)].reshape(rows, hx.shape[1]))

        def tile(j, carry):
            cols = pl.ds(pl.multiple_of(j * 2 * share_x, 2 * share_x), 2 * share_x)
            got = product((lines[0], lines[1]), (hx[0, :, cols], hx[1, :, cols]))
            send_a[slot, 2 * j] = got[:, :share_x]
            send_a[slot, 2 * j + 1] = got[:, share_x:]
            return carry

        lax.fori_loop(0, lefts // 2, tile, 0)
        for k in range(1, lefts):
            copy_a(i, lax.rem(left + k, lefts)).start()
        pltpu.make_async_copy(
            send_a.at[slot, left], first.at[i, pl.ds(left * rows, rows)], ra_sem.at[i, left]
        ).start()

    def y_step(i):
        for k in range(lefts):
            landed(first.at[i, pl.ds(k * rows, rows)], ra_sem.at[i, k])
        if near:
            block = first.at[i]
        else:
            block = staging[0]
            fetch = pltpu.make_async_copy(first.at[i], block, y_sem)
            fetch.start()
            fetch.wait()
        for z in range(0, DEPTH, 2):
            pair = jnp.concatenate(
                [block[pl.ds(z, size_y, stride=DEPTH), :], block[pl.ds(z + 1, size_y, stride=DEPTH), :]], axis=1
            )
            got = product((hy[0], hy[1]), split(pair))
            for to in range(rights):
                for band in range(bands):
                    top = to * out_y + band * BAND
                    for half in range(2):
                        send_b[i, to, band, (z + half) * BAND:(z + half + 1) * BAND, :] = (
                            got[top:top + BAND, half * share_x:(half + 1) * share_x]
                        )
        for band in range(bands):
            for k in range(rights):
                to = jnp.where(right < rights // 2, rights - 1 - k, k)

                @pl.when(to != right)
                def _():
                    copy_b(i, to, band).start()

            spot = right * share_z + lax.rem(i, pieces) * DEPTH
            pltpu.make_async_copy(
                send_b.at[i, right, band],
                second.at[i // pieces, band, pl.ds(spot * BAND, flat)],
                rb_sem.at[i, right, band],
            ).start()

    def step(i, carry):
        @pl.when(i < chunks)
        def _():
            x_step(i)

        @pl.when(i >= 1)
        def _():
            y_step(i - 1)

        return carry

    lax.fori_loop(0, chunks + 1, step, 0)

    def put(n):
        slot = lax.rem(n, 2)
        return pltpu.make_async_copy(obuf.at[slot], out.at[n // bands, lax.rem(n, bands)], o_sem.at[slot])

    def z_step(n, carry):
        field, band = n // bands, lax.rem(n, bands)
        slot = lax.rem(n, 2)

        def arrive(p, carry):
            for k in range(rights):
                spot = k * share_z + p * DEPTH
                landed(second.at[field, band, pl.ds(spot * BAND, flat)], rb_sem.at[field * pieces + p, k, band])
            return carry

        lax.fori_loop(0, pieces, arrive, 0)
        if near:
            block = second.at[field, band]
        else:
            block = staging[1]
            fetch = pltpu.make_async_copy(second.at[field, band], block, z_sem)
            fetch.start()
            fetch.wait()

        @pl.when(n >= 2)
        def _():
            put(n - 2).wait()

        def line(y, carry):
            plane = block[pl.ds(y, size_z, stride=BAND), :].T
            got = product(split(plane), (hz[0], hz[1]))
            got = got * lax.rsqrt(base[...] + sym_y[right * out_y + band * BAND + y])
            for t in range(size_z // LANES):
                obuf[slot, t, pl.ds(y, share_x, stride=BAND), :] = got[:, t * LANES:(t + 1) * LANES]
            return carry

        lax.fori_loop(0, BAND, line, 0, unroll=2)
        put(n).start()
        return carry

    steps = fields * bands
    lax.fori_loop(0, steps, z_step, 0)

    def drain_a(i, carry):
        sent_a(i)
        return carry

    lax.fori_loop(max(chunks - SLOTS, 0), chunks, drain_a, 0)

    def drain_b(i, carry):
        for k in range(1, rights):
            for band in range(bands):
                copy_b(i, lax.rem(right + k, rights), band).wait_send()
        return carry

    lax.fori_loop(0, chunks, drain_b, 0)
    for n in range(max(steps - 2, 0), steps):
        put(n).wait()


def stacked(halves):
    upper, lower = halves[0], halves[1]
    return jnp.concatenate(
        [jnp.concatenate([upper, lower], axis=1), jnp.concatenate([upper, jnp.zeros_like(lower)], axis=1)], axis=0
    )


def near_kernel(lefts, rights, inner, data, factors_in, hy_in, hz_in, x_in, z_in, y_in, out, tail, scale, table, *rest):
    (first, second, dbuf, factors, hx, hy, hz, lines, send_a, send_b, base,
     sym_x, sym_z, sym_y, raw_out, raw_in, guest_a, guest_first, guest_b,
     d_sem, t_sem, sa_sem, ra_sem, sb_sem, rb_sem, rc_sem, raw_sem, guest_sem) = rest
    fields, share_y, share_z, size_x = data.shape
    size_y = hy.shape[1]
    share_x, size_z = base.shape
    bands = out.shape[1]
    pieces = share_z // DEPTH
    chunks = fields * pieces
    subs = DEPTH // SUB
    out_y = bands * BAND
    half = rights // 2
    left, right = lax.axis_index("left"), lax.axis_index("right")

    def load(i):
        slot = lax.rem(i, 2)
        planes = pl.ds(lax.rem(i, pieces) * DEPTH, DEPTH)
        return [pltpu.make_async_copy(
            data.at[i // pieces, :, planes, pl.ds(c * LANES, LANES)],
            dbuf.at[slot, c].reshape(share_y, DEPTH, LANES),
            d_sem.at[slot],
        ) for c in range(size_x // LANES)]

    def fetch(i):
        for copy in load(i):
            copy.start()

    def copies(pairs):
        return [pltpu.make_async_copy(a, b, t_sem.at[n]) for n, (a, b) in enumerate(pairs)]

    tables = copies([(factors_in, factors), (hy_in, hy), (hz_in, hz)])
    symbols = copies([(x_in, sym_x), (z_in, sym_z), (y_in, sym_y)])
    barrier = pltpu.get_barrier_semaphore()
    for k in range(1, lefts):
        pl.semaphore_signal(barrier, inc=1, device_id=(lax.rem(left + k, lefts), right), device_id_type=MESH)
    for k in range(1, rights):
        pl.semaphore_signal(barrier, inc=1, device_id=(left, lax.rem(right + k, rights)), device_id_type=MESH)

    tables[0].start()
    fetch(0)
    tables[1].start()
    tables[2].start()

    def copy_a(i, z, count, to, sem):
        return pltpu.make_async_remote_copy(
            src_ref=send_a.at[i, to, pl.ds(z, count)],
            dst_ref=first.at[i, pl.ds(z, count), pl.ds(left * share_y, share_y), :],
            send_sem=sa_sem,
            recv_sem=sem,
            device_id=(to, right),
            device_id_type=MESH,
        )

    def copy_b(field, spot, count, to, kind):
        return pltpu.make_async_remote_copy(
            src_ref=send_b.at[field, to, :, pl.ds(spot * BAND, count * BAND), :],
            dst_ref=second.at[field, :, pl.ds((right * share_z + spot) * BAND, count * BAND), :],
            send_sem=sb_sem.at[jnp.where(field == 0, kind, 2)],
            recv_sem=rb_sem.at[field],
            device_id=(left, to),
            device_id_type=MESH,
        )

    def copy_c(n, to):
        band, rows = n // 2, pl.ds(n % 2 * SUBLANES, SUBLANES)
        there = second.at[fields - 1, band].reshape(size_z, BAND, share_x)
        return pltpu.make_async_remote_copy(
            src_ref=send_b.at[fields - 1, to, band].reshape(share_z, BAND, share_x).at[:, rows, :],
            dst_ref=there.at[pl.ds(right * share_z, share_z), rows, :],
            send_sem=sb_sem.at[2],
            recv_sem=rc_sem.at[n],
            device_id=(left, to),
            device_id_type=MESH,
        )

    lower = right < half
    rank = jnp.where(lower, right, rights - 1 - right)
    end = rank == 0
    gate = rank == half - 1
    twin = rights - 1 - right
    guest_z = DEPTH - SUB

    def mirrored(t):
        return jnp.where(lower, t, rights - 1 - t)

    def crossing(k):
        return mirrored(jnp.where(end, rights - 1 - k, half + k))

    def beside(k):
        return mirrored(lax.rem(rank + 1 + k, half))

    def raw():
        return pltpu.make_async_remote_copy(
            src_ref=raw_out,
            dst_ref=raw_in,
            send_sem=raw_sem.at[0],
            recv_sem=raw_sem.at[1],
            device_id=(left, twin),
            device_id_type=MESH,
        )

    def copy_guest_a(to):
        return pltpu.make_async_remote_copy(
            src_ref=guest_a.at[to],
            dst_ref=guest_first.at[:, pl.ds(left * share_y, share_y), :],
            send_sem=guest_sem.at[0],
            recv_sem=guest_sem.at[1],
            device_id=(to, right),
            device_id_type=MESH,
        )

    def copy_guest_b(to):
        spot = (twin * share_z + guest_z) * BAND
        return pltpu.make_async_remote_copy(
            src_ref=guest_b.at[to],
            dst_ref=second.at[0, :, pl.ds(spot, SUB * BAND), :],
            send_sem=guest_sem.at[2],
            recv_sem=rb_sem.at[0],
            device_id=(left, to),
            device_id_type=MESH,
        )

    def widen(cols):
        for top in range(size_x // inner):
            plus, minus = factors[2, top:top + 1, cols], factors[3, top:top + 1, cols]
            made = factors[0, :inner, cols] * plus + factors[1, :inner, cols] * minus
            rows = pl.ds(top * inner, inner)
            hx[0, rows, cols], hx[1, rows, cols] = split(made)

    def arrival(i, sub):
        return ra_sem.at[lax.rem(i, SLOTS), sub]

    def partner(k):
        return left ^ k if lefts & (lefts - 1) == 0 else lax.rem(left + k, lefts)

    def x_tile(sends, j, z, count, opening):
        pair = partner(lefts - 1 - 2 * j) // 2
        cols = pl.ds(pl.multiple_of(pair * 2 * share_x, 2 * share_x), 2 * share_x)
        if opening:
            widen(cols)
        rows = pl.ds(z * share_y, count * share_y)
        got = product((lines[0, rows, :], lines[1, rows, :]), (hx[0, :, cols], hx[1, :, cols]))
        for core in range(2):
            part = got[:, core * share_x:(core + 1) * share_x].reshape(count, share_y, share_x)
            sends[2 * pair + core, z:z + count] = part
        return pair

    def x_split(i, planes):
        slot = lax.rem(i, 2)
        for c in range(size_x // LANES):
            cols = pl.ds(c * LANES, LANES)
            for z in planes:
                rows = pl.ds(z * share_y, share_y)
                lines[0, rows, cols], lines[1, rows, cols] = split(dbuf[slot, c, pl.ds(z, share_y, stride=DEPTH), :])

    def x_send(i, z, count, pair, sem):
        for core in range(2):
            @pl.when(2 * pair + core != left)
            def _():
                copy_a(i, z, count, 2 * pair + core, sem).start()

    def x_rest(i, subs_left):
        for sub in subs_left:
            for k in range(lefts - 1, 0, -1):
                copy_a(i, sub * SUB, SUB, partner(k), arrival(i, sub)).start()

    def x_own(i, z, count):
        mine = pl.ds(pl.multiple_of(left * share_y, share_y), share_y)
        first[i, z:z + count, mine, :] = send_a[i, left, z:z + count]

    def x_open():
        landed(dbuf.at[0], d_sem.at[0])
        for c in range(size_x // LANES):
            for z in range(SUB):
                line = dbuf[0, c, pl.ds(guest_z + z, share_y, stride=DEPTH), :]
                raw_out[z * share_y:(z + 1) * share_y, c * LANES:(c + 1) * LANES] = line
        x_split(0, range(SUB))
        pl.semaphore_wait(barrier, lefts + rights - 2)

        @pl.when(gate)
        def _():
            raw().start()

        pair = x_tile(send_a.at[0], 0, 0, SUB, True)
        x_send(0, 0, 1, pair, arrival(0, 0))

        def tile(j, carry):
            x_send(0, 0, 1, x_tile(send_a.at[0], j, 0, SUB, True), arrival(0, 0))
            return carry

        lax.fori_loop(1, lefts // 2, tile, 0)
        for z in range(1, SUB):
            for k in range(lefts - 1, 0, -1):
                copy_a(0, z, 1, partner(k), arrival(2 * z, 0)).start()
        x_own(0, 0, SUB)
        x_split(0, range(SUB, DEPTH))

        def more(j, carry):
            x_send(0, SUB, SUB, x_tile(send_a.at[0], j, SUB, DEPTH - SUB, False), arrival(0, 1))
            return carry

        lax.fori_loop(0, lefts // 2, more, 0)
        x_rest(0, range(2, subs))
        x_own(0, SUB, DEPTH - SUB)
        fetch(2)

    def x_step(i):
        slot = lax.rem(i, 2)
        landed(dbuf.at[slot], d_sem.at[slot])
        x_split(i, range(DEPTH))

        @pl.when(i + 2 < chunks)
        def _():
            fetch(i + 2)

        def tile(j, carry):
            x_send(i, 0, SUB, x_tile(send_a.at[i], j, 0, DEPTH, False), arrival(i, 0))
            return carry

        lax.fori_loop(0, lefts // 2, tile, 0)
        x_rest(i, range(1, subs))
        x_own(i, 0, DEPTH)

    def y_values(ready, sends, spot, count):
        got = product((hy[0], hy[1]), split(jnp.concatenate([ready[n] for n in range(count)], axis=1)))
        for to in range(rights):
            for band in range(bands):
                top = to * out_y + band * BAND
                for n in range(count):
                    rows = pl.ds(pl.multiple_of((spot + n) * BAND, BAND), BAND)
                    sends[to, band, rows, :] = got[top:top + BAND, n * share_x:(n + 1) * share_x]

    def y_own(sends, spot, field, there, count):
        for band in range(bands):
            mine = sends[right, band, pl.ds(pl.multiple_of(spot * BAND, BAND), count * BAND), :]
            second[field, band, pl.ds(pl.multiple_of(there * BAND, BAND), count * BAND), :] = mine

    def y_step(i, z, count, sem):
        landed(first.at[i, pl.ds(z, count), pl.ds(0, (lefts - 1) * share_y), :], sem)
        field, spot = i // pieces, lax.rem(i, pieces) * DEPTH + z
        y_values(first.at[i, pl.ds(z, count)], send_b.at[field], spot, count)
        hosted = jnp.logical_and(gate, jnp.logical_and(i == 0, z == guest_z))
        direct = jnp.logical_or(end, jnp.logical_and(field < fields - 1, jnp.logical_not(hosted)))
        for k in range(half):
            @pl.when(direct)
            def _():
                copy_b(field, spot, count, crossing(k), 0).start()
        for k in range(half - 1):
            @pl.when(jnp.logical_not(field == fields - 1))
            def _():
                copy_b(field, spot, count, beside(k), 1).start()
        y_own(send_b.at[field], spot, field, right * share_z + spot, count)

    def guest_x():
        landed(raw_in, raw_sem.at[1])
        for c in range(size_x // LANES):
            cols = pl.ds(c * LANES, LANES)
            lines[0, pl.ds(0, SUB * share_y), cols], lines[1, pl.ds(0, SUB * share_y), cols] = split(raw_in[:, cols])

        def tile(j, carry):
            x_tile(guest_a, j, 0, SUB, False)
            return carry

        lax.fori_loop(0, lefts // 2, tile, 0)
        for k in range(lefts - 1, 0, -1):
            copy_guest_a(partner(k)).start()
        guest_first[:, pl.ds(pl.multiple_of(left * share_y, share_y), share_y), :] = guest_a[left]

    def guest_y():
        landed(guest_first.at[:, pl.ds(0, (lefts - 1) * share_y), :], guest_sem.at[1])
        y_values(guest_first, guest_b, 0, SUB)
        for k in range(half - 1):
            copy_guest_b(beside(k)).start()
        y_own(guest_b, 0, 0, twin * share_z + guest_z, SUB)

    fetch(1)
    tables[0].wait()
    x_open()
    tables[1].wait()
    tables[2].wait()
    for symbol in symbols:
        symbol.start()
    for z in range(SUB):
        y_step(0, z, 1, arrival(2 * z, 0))

    def step(i, carry):
        @pl.when(i + 1 < chunks)
        def _():
            x_step(i + 1)

        @pl.when(jnp.logical_and(gate, i == min(1, chunks - 1)))
        def _():
            guest_x()

        def part(sub, carry):
            y_step(i, sub * SUB, SUB, arrival(i, sub))
            return carry

        lax.fori_loop(1, subs, part, 0)

        @pl.when(jnp.logical_and(gate, i == min(2, chunks - 1)))
        def _():
            guest_y()

        @pl.when(i + 1 < chunks)
        def _():
            y_step(i + 1, 0, SUB, arrival(i + 1, 0))

        return carry

    lax.fori_loop(0, chunks, step, 0)

    for k in range(half - 1):
        copy_b(fields - 1, 0, share_z, beside(k), 1).start()

    @pl.when(jnp.logical_not(end))
    def _():
        for n in range(2 * bands):
            for k in range(half - 1, -1, -1):
                copy_c(n, crossing(k)).start()

    for symbol in symbols:
        symbol.wait()
    column = jnp.broadcast_to(sym_x[pl.ds(left, 1), :], (size_z, share_x)).T
    base[...] = column + sym_z[...]
    table[...] = hz[...]
    for y in range(SUBLANES):
        scale[y] = lax.rsqrt(base[...] + sym_y[right * out_y + out_y - SUBLANES + y])

    def held_in(band, part):
        block = second.at[fields - 1, band].reshape(size_z, BAND, share_x)
        rows = pl.ds(part % 2 * SUBLANES, SUBLANES)
        landed(block.at[pl.ds(0, (half - 1) * share_z), rows, :], rc_sem.at[part])

    def z_step(n, carry):
        field, part = n // (2 * bands), lax.rem(n, 2 * bands)
        band, top = part // 2, lax.rem(part, 2) * SUBLANES
        hosting = jnp.logical_and(gate, field == 0)
        everything = (rights - 1) * share_z
        for planes, chosen in (
            (everything - SUB, hosting),
            (everything, jnp.logical_and(field < fields - 1, jnp.logical_not(hosting))),
            (half * share_z, field == fields - 1),
        ):
            @pl.when(jnp.logical_and(part == 0, chosen))
            def _():
                landed(second.at[field, :, pl.ds(0, planes * BAND), :], rb_sem.at[field])

        @pl.when(field == fields - 1)
        def _():
            held_in(band, part)

        def line(step, carry):
            y = top + step
            plane = second[field, band, pl.ds(y, size_z, stride=BAND), :].T
            got = jnp.dot(jnp.concatenate(split(plane), axis=1), hz[...], preferred_element_type=jnp.float32)
            got = (got[:, :size_z] + got[:, size_z:]) * lax.rsqrt(base[...] + sym_y[right * out_y + band * BAND + y])
            out[field, band, pl.ds(y, share_x, stride=BAND), :] = got
            return carry

        lax.fori_loop(0, SUBLANES, line, 0, unroll=4)
        return carry

    lax.fori_loop(0, fields * bands * 2 - 1, z_step, 0)
    held_in(bands - 1, 2 * bands - 1)
    block = second.at[fields - 1, bands - 1].reshape(size_z, BAND, share_x)
    tail[...] = block[:, BAND - SUBLANES:, :].reshape(size_z * SUBLANES, share_x)
    landed(send_a.at[:, pl.ds(0, lefts - 1)], sa_sem)
    landed(send_b.at[0, pl.ds(0, half - 1)], sb_sem.at[1])
    landed(send_b.at[pl.ds(1, fields - 1), pl.ds(0, rights - 1)], sb_sem.at[2])

    @pl.when(gate)
    def _():
        landed(send_b.at[0, pl.ds(0, half), :, pl.ds(0, (share_z - SUB) * BAND), :], sb_sem.at[0])
        landed(raw_out, raw_sem.at[0])
        landed(guest_a.at[pl.ds(0, lefts - 1)], guest_sem.at[0])
        landed(guest_b.at[pl.ds(0, half - 1)], guest_sem.at[2])

    @pl.when(jnp.logical_not(gate))
    def _():
        landed(send_b.at[0, pl.ds(0, half)], sb_sem.at[0])


def flush_kernel(ready, tail, scale, table, out, made, sem):
    fields, bands, share_x, _, size_z = ready.shape
    for n in range(fields * bands):
        field, band = n // bands, n % bands
        rows = BAND if n < fields * bands - 1 else BAND - SUBLANES
        there = out.at[field, :, pl.ds(band * BAND, rows), :]
        pltpu.make_async_copy(ready.at[field, band, :, pl.ds(0, rows), :], there, sem).start()
    for y in range(SUBLANES):
        plane = tail[pl.ds(y, size_z, stride=SUBLANES), :].T
        got = jnp.dot(jnp.concatenate(split(plane), axis=1), table[...], preferred_element_type=jnp.float32)
        made[pl.ds(y, share_x, stride=SUBLANES), :] = (got[:, :size_z] + got[:, size_z:]) * scale[y]
    there = out.at[fields - 1, :, pl.ds(bands * BAND - SUBLANES, SUBLANES), :]
    pltpu.make_async_copy(made.reshape(share_x, SUBLANES, size_z), there, sem).start()
    landed(out, sem)


def near_local(lefts, rights, tracer, symbol_x, symbol_y, symbol_z):
    fields, size_x, share_y, share_z = tracer.shape
    size_y, size_z = symbol_y.shape[0], symbol_z.shape[0]
    share_x, out_y = size_x // lefts, size_y // rights
    bands = out_y // BAND
    chunks = fields * (share_z // DEPTH)
    data = jnp.transpose(tracer, (0, 2, 3, 1))
    factors, inner = factors_of(size_x)
    hy, hz = small_table(size_y), stacked(small_table(size_z))
    f32, bf16 = jnp.float32, jnp.bfloat16
    any_space = pl.BlockSpec(memory_space=pl.ANY)
    vmem = pl.BlockSpec(memory_space=pltpu.VMEM)
    dma = pltpu.SemaphoreType.DMA
    ready, *others = pl.pallas_call(
        functools.partial(near_kernel, lefts, rights, inner),
        name="modes",
        out_shape=[
            pltpu.VMEM((fields, bands, share_x * BAND, size_z), f32),
            pltpu.VMEM((size_z * SUBLANES, share_x), f32),
            pltpu.VMEM((SUBLANES, share_x, size_z), f32),
            pltpu.VMEM(hz.shape, bf16),
        ],
        in_specs=[any_space] * 7,
        out_specs=[vmem] * 4,
        scratch_shapes=[
            pltpu.VMEM((chunks, DEPTH, size_y, share_x), f32),
            pltpu.VMEM((fields, bands, size_z * BAND, share_x), f32),
            pltpu.VMEM((2, size_x // LANES, share_y * DEPTH, LANES), f32),
            pltpu.VMEM(factors.shape, f32),
            pltpu.VMEM((2, size_x, size_x), bf16),
            pltpu.VMEM(hy.shape, bf16),
            pltpu.VMEM(hz.shape, bf16),
            pltpu.VMEM((2, share_y * DEPTH, size_x), bf16),
            pltpu.VMEM((chunks, lefts, DEPTH, share_y, share_x), f32),
            pltpu.VMEM((fields, rights, bands, share_z * BAND, share_x), f32),
            pltpu.VMEM((share_x, size_z), f32),
            pltpu.VMEM((lefts, share_x), f32),
            pltpu.VMEM((1, size_z), f32),
            pltpu.SMEM((size_y,), f32),
            pltpu.VMEM((SUB * share_y, size_x), f32),
            pltpu.VMEM((SUB * share_y, size_x), f32),
            pltpu.VMEM((lefts, SUB, share_y, share_x), f32),
            pltpu.VMEM((SUB, size_y, share_x), f32),
            pltpu.VMEM((rights, bands, SUB * BAND, share_x), f32),
            dma((2,)),
            dma((3,)),
            dma,
            dma((SLOTS, DEPTH // SUB)),
            dma((3,)),
            dma((fields,)),
            dma((2 * bands,)),
            dma((2,)),
            dma((3,)),
        ],
        compiler_params=pltpu.CompilerParams(
            collective_id=0, has_side_effects=True, vmem_limit_bytes=NEAR_LIMIT
        ),
    )(data, factors, hy, hz, symbol_x.reshape(lefts, share_x), symbol_z.reshape(1, size_z), symbol_y)
    return pl.pallas_call(
        flush_kernel,
        name="flush",
        out_shape=jax.ShapeDtypeStruct((fields, share_x, out_y, size_z), f32),
        in_specs=[vmem] * 4,
        out_specs=any_space,
        scratch_shapes=[pltpu.VMEM((share_x * SUBLANES, size_z), f32), dma],
        compiler_params=pltpu.CompilerParams(vmem_limit_bytes=2**21),
    )(ready.reshape(fields, bands, share_x, BAND, size_z), *others)


def far_local(lefts, rights, tracer, symbol_x, symbol_y, symbol_z):
    fields, size_x, share_y, share_z = tracer.shape
    size_y, size_z = symbol_y.shape[0], symbol_z.shape[0]
    share_x, out_y = size_x // lefts, size_y // rights
    bands = out_y // BAND
    chunks = fields * (share_z // DEPTH)
    data = jnp.transpose(tracer, (0, 2, 3, 1))
    part_x = lax.dynamic_slice_in_dim(symbol_x, lax.axis_index("left") * share_x, share_x)
    base = part_x[:, None] + symbol_z[None, :]
    f32 = jnp.float32
    any_space = pl.BlockSpec(memory_space=pl.ANY)
    vmem = pl.BlockSpec(memory_space=pltpu.VMEM)
    landing = [(chunks, size_y * DEPTH, share_x), (fields, bands, size_z * BAND, share_x)]
    near = 4 * sum(map(math.prod, landing)) <= NEAR_BYTES
    staging = [] if near else [
        pltpu.VMEM((size_y * DEPTH, share_x), f32), pltpu.VMEM((size_z * BAND, share_x), f32)
    ]
    results = pl.pallas_call(
        functools.partial(far_kernel, lefts, rights, near),
        name="modes",
        out_shape=[
            jax.ShapeDtypeStruct((fields, bands, size_z // LANES, share_x * BAND, LANES), f32),
            *([] if near else [jax.ShapeDtypeStruct(shape, f32) for shape in landing]),
        ],
        in_specs=[any_space, vmem, vmem, vmem, vmem, pl.BlockSpec(memory_space=pltpu.SMEM)],
        out_specs=[any_space] * (1 if near else 3),
        scratch_shapes=[
            *([pltpu.VMEM(shape, f32) for shape in landing] if near else []),
            pltpu.VMEM((2, share_y, DEPTH, size_x), f32),
            pltpu.VMEM((2, share_y * DEPTH, size_x), jnp.bfloat16),
            pltpu.VMEM((SLOTS, lefts, share_y * DEPTH, share_x), f32),
            pltpu.VMEM((chunks, rights, bands, DEPTH * BAND, share_x), f32),
            pltpu.VMEM((2, size_z // LANES, share_x * BAND, LANES), f32),
            pltpu.SemaphoreType.DMA((2,)),
            pltpu.SemaphoreType.DMA((SLOTS, lefts)),
            pltpu.SemaphoreType.DMA((chunks, lefts)),
            pltpu.SemaphoreType.DMA,
            pltpu.SemaphoreType.DMA((chunks, rights, bands)),
            pltpu.SemaphoreType.DMA((chunks, rights, bands)),
            pltpu.SemaphoreType.DMA,
            pltpu.SemaphoreType.DMA((2,)),
            *staging,
        ],
        compiler_params=pltpu.CompilerParams(
            collective_id=0, has_side_effects=True, vmem_limit_bytes=60 * 2**20
        ),
    )(data, halves_of(transform_table(size_x)), small_table(size_y), small_table(size_z), base, symbol_y)
    out = results[0].reshape(fields, bands, size_z // LANES, share_x, BAND, LANES)
    return jnp.transpose(out, (0, 3, 1, 4, 2, 5)).reshape(fields, share_x, out_y, size_z)


def local(lefts, rights, tracer, symbol_x, symbol_y, symbol_z):
    fields, size_x, share_y, share_z = tracer.shape
    size_z, share_x = symbol_z.shape[0], size_x // lefts
    size = 4 * math.prod(tracer.shape)
    fits = size <= NEAR_BYTES // 2 and share_x == LANES and size_z == LANES and rights % 2 == 0
    fits = fits and rights > 2 and fields > 1
    run = near_local if fits else far_local
    return run(lefts, rights, tracer, symbol_x, symbol_y, symbol_z)


def solution(mesh):
    return jax.shard_map(
        functools.partial(local, mesh.shape["left"], mesh.shape["right"]),
        mesh=mesh,
        in_specs=(P(None, None, "left", "right"), P(), P(), P()),
        out_specs=P(None, "left", "right", None),
        check_vma=False,
    )
```

```python
import functools
import math

import jax
import jax.numpy as jnp
import numpy as np
from jax import lax
from jax.experimental import pallas as pl
from jax.experimental.pallas import tpu as pltpu
from jax.sharding import PartitionSpec as P

MESH = pl.DeviceIdType.MESH
NEAR_BYTES = 20 * 2**20
DEPTH = 8
BAND = 16
SUBLANES = 8
LANES = 128
SLOTS = 3
NEAR_LIMIT = 50 * 2**20
SUB = 2


def transform_table(count):
    inner = 1 << ((count.bit_length() - 1) // 2)
    outer = count // inner
    column = np.arange(count)

    def angle(row):
        return 2.0 * np.pi / count * (row[:, None] * column[None, :] % count)

    low = angle(np.arange(inner))
    high = angle(np.arange(outer) * inner)
    scale = count ** (-0.5)
    cos_low = jnp.asarray(np.cos(low), jnp.float32)[None]
    sin_low = jnp.asarray(np.sin(low), jnp.float32)[None]
    plus = jnp.asarray((np.cos(high) + np.sin(high)) * scale, jnp.float32)[:, None]
    minus = jnp.asarray((np.cos(high) - np.sin(high)) * scale, jnp.float32)[:, None]
    return (cos_low * plus + sin_low * minus).reshape(count, count)


def factors_of(count):
    inner = 1 << ((count.bit_length() - 1) // 2)
    outer = count // inner
    column = np.arange(count)

    def angle(row):
        return 2.0 * np.pi / count * (row[:, None] * column[None, :] % count)

    low = angle(np.arange(inner))
    high = angle(np.arange(outer) * inner)
    scale = count ** (-0.5)
    low = np.stack([np.cos(low), np.sin(low)])
    high = np.stack([np.cos(high) + np.sin(high), np.cos(high) - np.sin(high)]) * scale
    rows = max(inner, outer)
    padded = [np.pad(part, ((0, 0), (0, rows - part.shape[1]), (0, 0))) for part in (low, high)]
    return jnp.asarray(np.concatenate(padded), jnp.float32), inner


def halves_of(table):
    upper = lax.reduce_precision(table, 8, 7)
    return jnp.stack([upper.astype(jnp.bfloat16), (table - upper).astype(jnp.bfloat16)])


def small_table(count):
    rank = np.arange(count)
    angle = 2.0 * np.pi / count * (rank[:, None] * rank[None, :] % count)
    table = ((np.cos(angle) + np.sin(angle)) * count ** (-0.5)).astype(np.float32)
    upper = table.astype(jnp.bfloat16)
    return jnp.asarray(np.stack([upper, (table - upper.astype(np.float32)).astype(jnp.bfloat16)]))


def split(values):
    upper = values.astype(jnp.bfloat16)
    return upper, (values - upper.astype(jnp.float32)).astype(jnp.bfloat16)


def product(a, b):
    dot = functools.partial(jnp.dot, preferred_element_type=jnp.float32)
    return dot(a[0], b[0]) + (dot(a[0], b[1]) + dot(a[1], b[0]))


def landed(ref, sem):
    pltpu.make_async_copy(ref, ref, sem).wait()


def far_kernel(lefts, rights, near, data, hx, hy, hz, base, sym_y, out, *rest):
    (first, second, dbuf, lines, send_a, send_b, obuf,
     d_sem, sa_sem, ra_sem, y_sem, sb_sem, rb_sem, z_sem, o_sem, *staging) = rest
    fields, share_y, share_z, _ = data.shape
    size_y, size_z = hy.shape[1], hz.shape[1]
    share_x = base.shape[0]
    bands = out.shape[1]
    pieces = share_z // DEPTH
    chunks = fields * pieces
    rows = share_y * DEPTH
    flat = DEPTH * BAND
    out_y = bands * BAND
    left, right = lax.axis_index("left"), lax.axis_index("right")

    def load(i):
        source = data.at[i // pieces, :, pl.ds(lax.rem(i, pieces) * DEPTH, DEPTH), :]
        return pltpu.make_async_copy(source, dbuf.at[lax.rem(i, 2)], d_sem.at[lax.rem(i, 2)])

    load(0).start()

    barrier = pltpu.get_barrier_semaphore()
    for k in range(1, lefts):
        pl.semaphore_signal(barrier, inc=1, device_id=(lax.rem(left + k, lefts), right), device_id_type=MESH)
    for k in range(1, rights):
        pl.semaphore_signal(barrier, inc=1, device_id=(left, lax.rem(right + k, rights)), device_id_type=MESH)
    pl.semaphore_wait(barrier, lefts + rights - 2)

    def copy_a(i, to):
        slot = lax.rem(i, SLOTS)
        return pltpu.make_async_remote_copy(
            src_ref=send_a.at[slot, to],
            dst_ref=first.at[i, pl.ds(left * rows, rows)],
            send_sem=sa_sem.at[slot, to],
            recv_sem=ra_sem.at[i, left],
            device_id=(to, right),
            device_id_type=MESH,
        )

    def copy_b(i, to, band):
        spot = right * share_z + lax.rem(i, pieces) * DEPTH
        return pltpu.make_async_remote_copy(
            src_ref=send_b.at[i, to, band],
            dst_ref=second.at[i // pieces, band, pl.ds(spot * BAND, flat)],
            send_sem=sb_sem.at[i, to, band],
            recv_sem=rb_sem.at[i, right, band],
            device_id=(left, to),
            device_id_type=MESH,
        )

    def sent_a(i):
        for k in range(1, lefts):
            copy_a(i, lax.rem(left + k, lefts)).wait_send()

    def x_step(i):
        load(i).wait()

        @pl.when(i + 1 < chunks)
        def _():
            load(i + 1).start()

        @pl.when(i >= SLOTS)
        def _():
            sent_a(i - SLOTS)

        slot = lax.rem(i, SLOTS)
        lines[0], lines[1] = split(dbuf[lax.rem(i, 2)].reshape(rows, hx.shape[1]))

        def tile(j, carry):
            cols = pl.ds(pl.multiple_of(j * 2 * share_x, 2 * share_x), 2 * share_x)
            got = product((lines[0], lines[1]), (hx[0, :, cols], hx[1, :, cols]))
            send_a[slot, 2 * j] = got[:, :share_x]
            send_a[slot, 2 * j + 1] = got[:, share_x:]
            return carry

        lax.fori_loop(0, lefts // 2, tile, 0)
        for k in range(1, lefts):
            copy_a(i, lax.rem(left + k, lefts)).start()
        pltpu.make_async_copy(
            send_a.at[slot, left], first.at[i, pl.ds(left * rows, rows)], ra_sem.at[i, left]
        ).start()

    def y_step(i):
        for k in range(lefts):
            landed(first.at[i, pl.ds(k * rows, rows)], ra_sem.at[i, k])
        if near:
            block = first.at[i]
        else:
            block = staging[0]
            fetch = pltpu.make_async_copy(first.at[i], block, y_sem)
            fetch.start()
            fetch.wait()
        for z in range(0, DEPTH, 2):
            pair = jnp.concatenate(
                [block[pl.ds(z, size_y, stride=DEPTH), :], block[pl.ds(z + 1, size_y, stride=DEPTH), :]], axis=1
            )
            got = product((hy[0], hy[1]), split(pair))
            for to in range(rights):
                for band in range(bands):
                    top = to * out_y + band * BAND
                    for half in range(2):
                        send_b[i, to, band, (z + half) * BAND:(z + half + 1) * BAND, :] = (
                            got[top:top + BAND, half * share_x:(half + 1) * share_x]
                        )
        for band in range(bands):
            for k in range(rights):
                to = jnp.where(right < rights // 2, rights - 1 - k, k)

                @pl.when(to != right)
                def _():
                    copy_b(i, to, band).start()

            spot = right * share_z + lax.rem(i, pieces) * DEPTH
            pltpu.make_async_copy(
                send_b.at[i, right, band],
                second.at[i // pieces, band, pl.ds(spot * BAND, flat)],
                rb_sem.at[i, right, band],
            ).start()

    def step(i, carry):
        @pl.when(i < chunks)
        def _():
            x_step(i)

        @pl.when(i >= 1)
        def _():
            y_step(i - 1)

        return carry

    lax.fori_loop(0, chunks + 1, step, 0)

    def put(n):
        slot = lax.rem(n, 2)
        return pltpu.make_async_copy(obuf.at[slot], out.at[n // bands, lax.rem(n, bands)], o_sem.at[slot])

    def z_step(n, carry):
        field, band = n // bands, lax.rem(n, bands)
        slot = lax.rem(n, 2)

        def arrive(p, carry):
            for k in range(rights):
                spot = k * share_z + p * DEPTH
                landed(second.at[field, band, pl.ds(spot * BAND, flat)], rb_sem.at[field * pieces + p, k, band])
            return carry

        lax.fori_loop(0, pieces, arrive, 0)
        if near:
            block = second.at[field, band]
        else:
            block = staging[1]
            fetch = pltpu.make_async_copy(second.at[field, band], block, z_sem)
            fetch.start()
            fetch.wait()

        @pl.when(n >= 2)
        def _():
            put(n - 2).wait()

        def line(y, carry):
            plane = block[pl.ds(y, size_z, stride=BAND), :].T
            got = product(split(plane), (hz[0], hz[1]))
            got = got * lax.rsqrt(base[...] + sym_y[right * out_y + band * BAND + y])
            for t in range(size_z // LANES):
                obuf[slot, t, pl.ds(y, share_x, stride=BAND), :] = got[:, t * LANES:(t + 1) * LANES]
            return carry

        lax.fori_loop(0, BAND, line, 0, unroll=2)
        put(n).start()
        return carry

    steps = fields * bands
    lax.fori_loop(0, steps, z_step, 0)

    def drain_a(i, carry):
        sent_a(i)
        return carry

    lax.fori_loop(max(chunks - SLOTS, 0), chunks, drain_a, 0)

    def drain_b(i, carry):
        for k in range(1, rights):
            for band in range(bands):
                copy_b(i, lax.rem(right + k, rights), band).wait_send()
        return carry

    lax.fori_loop(0, chunks, drain_b, 0)
    for n in range(max(steps - 2, 0), steps):
        put(n).wait()


def stacked(halves):
    upper, lower = halves[0], halves[1]
    return jnp.concatenate(
        [jnp.concatenate([upper, lower], axis=1), jnp.concatenate([upper, jnp.zeros_like(lower)], axis=1)], axis=0
    )


def near_kernel(lefts, rights, inner, data, factors_in, hy_in, hz_in, x_in, z_in, y_in, out, tail, scale, table, *rest):
    (first, second, dbuf, factors, hx, hy, hz, lines, send_a, send_b, base,
     sym_x, sym_z, sym_y, raw_out, raw_in, guest_a, guest_first, guest_b,
     d_sem, t_sem, sa_sem, ra_sem, sb_sem, rb_sem, rc_sem, raw_sem, guest_sem) = rest
    fields, share_y, share_z, size_x = data.shape
    size_y = hy.shape[1]
    share_x, size_z = base.shape
    bands = out.shape[1]
    pieces = share_z // DEPTH
    chunks = fields * pieces
    subs = DEPTH // SUB
    out_y = bands * BAND
    half = rights // 2
    left, right = lax.axis_index("left"), lax.axis_index("right")

    def load(i):
        slot = lax.rem(i, 2)
        planes = pl.ds(lax.rem(i, pieces) * DEPTH, DEPTH)
        return [pltpu.make_async_copy(
            data.at[i // pieces, :, planes, pl.ds(c * LANES, LANES)],
            dbuf.at[slot, c].reshape(share_y, DEPTH, LANES),
            d_sem.at[slot],
        ) for c in range(size_x // LANES)]

    def fetch(i):
        for copy in load(i):
            copy.start()

    def copies(pairs):
        return [pltpu.make_async_copy(a, b, t_sem.at[n]) for n, (a, b) in enumerate(pairs)]

    tables = copies([(factors_in, factors), (hy_in, hy), (hz_in, hz)])
    symbols = copies([(x_in, sym_x), (z_in, sym_z), (y_in, sym_y)])
    barrier = pltpu.get_barrier_semaphore()
    for k in range(1, lefts):
        pl.semaphore_signal(barrier, inc=1, device_id=(lax.rem(left + k, lefts), right), device_id_type=MESH)
    for k in range(1, rights):
        pl.semaphore_signal(barrier, inc=1, device_id=(left, lax.rem(right + k, rights)), device_id_type=MESH)

    tables[0].start()
    fetch(0)
    tables[1].start()
    tables[2].start()

    def copy_a(i, z, count, to, sem):
        return pltpu.make_async_remote_copy(
            src_ref=send_a.at[i, to, pl.ds(z, count)],
            dst_ref=first.at[i, pl.ds(z, count), pl.ds(left * share_y, share_y), :],
            send_sem=sa_sem,
            recv_sem=sem,
            device_id=(to, right),
            device_id_type=MESH,
        )

    def copy_b(field, spot, count, to, kind):
        return pltpu.make_async_remote_copy(
            src_ref=send_b.at[field, to, :, pl.ds(spot * BAND, count * BAND), :],
            dst_ref=second.at[field, :, pl.ds((right * share_z + spot) * BAND, count * BAND), :],
            send_sem=sb_sem.at[jnp.where(field == 0, kind, 2)],
            recv_sem=rb_sem.at[field],
            device_id=(left, to),
            device_id_type=MESH,
        )

    def copy_c(n, to):
        band, rows = n // 2, pl.ds(n % 2 * SUBLANES, SUBLANES)
        there = second.at[fields - 1, band].reshape(size_z, BAND, share_x)
        return pltpu.make_async_remote_copy(
            src_ref=send_b.at[fields - 1, to, band].reshape(share_z, BAND, share_x).at[:, rows, :],
            dst_ref=there.at[pl.ds(right * share_z, share_z), rows, :],
            send_sem=sb_sem.at[2],
            recv_sem=rc_sem.at[n],
            device_id=(left, to),
            device_id_type=MESH,
        )

    lower = right < half
    rank = jnp.where(lower, right, rights - 1 - right)
    end = rank == 0
    gate = rank == half - 1
    twin = rights - 1 - right
    guest_z = DEPTH - SUB

    def mirrored(t):
        return jnp.where(lower, t, rights - 1 - t)

    def crossing(k):
        return mirrored(jnp.where(end, rights - 1 - k, half + k))

    def beside(k):
        return mirrored(lax.rem(rank + 1 + k, half))

    def raw():
        return pltpu.make_async_remote_copy(
            src_ref=raw_out,
            dst_ref=raw_in,
            send_sem=raw_sem.at[0],
            recv_sem=raw_sem.at[1],
            device_id=(left, twin),
            device_id_type=MESH,
        )

    def copy_guest_a(to):
        return pltpu.make_async_remote_copy(
            src_ref=guest_a.at[to],
            dst_ref=guest_first.at[:, pl.ds(left * share_y, share_y), :],
            send_sem=guest_sem.at[0],
            recv_sem=guest_sem.at[1],
            device_id=(to, right),
            device_id_type=MESH,
        )

    def copy_guest_b(to):
        spot = (twin * share_z + guest_z) * BAND
        return pltpu.make_async_remote_copy(
            src_ref=guest_b.at[to],
            dst_ref=second.at[0, :, pl.ds(spot, SUB * BAND), :],
            send_sem=guest_sem.at[2],
            recv_sem=rb_sem.at[0],
            device_id=(left, to),
            device_id_type=MESH,
        )

    def widen(cols):
        for top in range(size_x // inner):
            plus, minus = factors[2, top:top + 1, cols], factors[3, top:top + 1, cols]
            made = factors[0, :inner, cols] * plus + factors[1, :inner, cols] * minus
            rows = pl.ds(top * inner, inner)
            hx[0, rows, cols], hx[1, rows, cols] = split(made)

    def arrival(i, sub):
        return ra_sem.at[lax.rem(i, SLOTS), sub]

    def partner(k):
        return left ^ k if lefts & (lefts - 1) == 0 else lax.rem(left + k, lefts)

    def x_tile(sends, j, z, count, opening):
        pair = partner(lefts - 1 - 2 * j) // 2
        cols = pl.ds(pl.multiple_of(pair * 2 * share_x, 2 * share_x), 2 * share_x)
        if opening:
            widen(cols)
        rows = pl.ds(z * share_y, count * share_y)
        got = product((lines[0, rows, :], lines[1, rows, :]), (hx[0, :, cols], hx[1, :, cols]))
        for core in range(2):
            part = got[:, core * share_x:(core + 1) * share_x].reshape(count, share_y, share_x)
            sends[2 * pair + core, z:z + count] = part
        return pair

    def x_split(i, planes):
        slot = lax.rem(i, 2)
        for c in range(size_x // LANES):
            cols = pl.ds(c * LANES, LANES)
            for z in planes:
                rows = pl.ds(z * share_y, share_y)
                lines[0, rows, cols], lines[1, rows, cols] = split(dbuf[slot, c, pl.ds(z, share_y, stride=DEPTH), :])

    def x_send(i, z, count, pair, sem):
        for core in range(2):
            @pl.when(2 * pair + core != left)
            def _():
                copy_a(i, z, count, 2 * pair + core, sem).start()

    def x_rest(i, subs_left):
        for sub in subs_left:
            for k in range(lefts - 1, 0, -1):
                copy_a(i, sub * SUB, SUB, partner(k), arrival(i, sub)).start()

    def x_own(i, z, count):
        mine = pl.ds(pl.multiple_of(left * share_y, share_y), share_y)
        first[i, z:z + count, mine, :] = send_a[i, left, z:z + count]

    def x_open():
        landed(dbuf.at[0], d_sem.at[0])
        for c in range(size_x // LANES):
            for z in range(SUB):
                line = dbuf[0, c, pl.ds(guest_z + z, share_y, stride=DEPTH), :]
                raw_out[z * share_y:(z + 1) * share_y, c * LANES:(c + 1) * LANES] = line
        x_split(0, range(SUB))
        pl.semaphore_wait(barrier, lefts + rights - 2)

        @pl.when(gate)
        def _():
            raw().start()

        pair = x_tile(send_a.at[0], 0, 0, SUB, True)
        x_send(0, 0, 1, pair, arrival(0, 0))

        def tile(j, carry):
            x_send(0, 0, 1, x_tile(send_a.at[0], j, 0, SUB, True), arrival(0, 0))
            return carry

        lax.fori_loop(1, lefts // 2, tile, 0)
        for z in range(1, SUB):
            for k in range(lefts - 1, 0, -1):
                copy_a(0, z, 1, partner(k), arrival(2 * z, 0)).start()
        x_own(0, 0, SUB)
        x_split(0, range(SUB, DEPTH))

        def more(j, carry):
            x_send(0, SUB, SUB, x_tile(send_a.at[0], j, SUB, DEPTH - SUB, False), arrival(0, 1))
            return carry

        lax.fori_loop(0, lefts // 2, more, 0)
        x_rest(0, range(2, subs))
        x_own(0, SUB, DEPTH - SUB)
        fetch(2)

    def x_step(i):
        slot = lax.rem(i, 2)
        landed(dbuf.at[slot], d_sem.at[slot])
        x_split(i, range(DEPTH))

        @pl.when(i + 2 < chunks)
        def _():
            fetch(i + 2)

        def tile(j, carry):
            x_send(i, 0, SUB, x_tile(send_a.at[i], j, 0, DEPTH, False), arrival(i, 0))
            return carry

        lax.fori_loop(0, lefts // 2, tile, 0)
        x_rest(i, range(1, subs))
        x_own(i, 0, DEPTH)

    def y_values(ready, sends, spot, count):
        got = product((hy[0], hy[1]), split(jnp.concatenate([ready[n] for n in range(count)], axis=1)))
        for to in range(rights):
            for band in range(bands):
                top = to * out_y + band * BAND
                for n in range(count):
                    rows = pl.ds(pl.multiple_of((spot + n) * BAND, BAND), BAND)
                    sends[to, band, rows, :] = got[top:top + BAND, n * share_x:(n + 1) * share_x]

    def y_own(sends, spot, field, there, count):
        for band in range(bands):
            mine = sends[right, band, pl.ds(pl.multiple_of(spot * BAND, BAND), count * BAND), :]
            second[field, band, pl.ds(pl.multiple_of(there * BAND, BAND), count * BAND), :] = mine

    def y_step(i, z, count, sem):
        landed(first.at[i, pl.ds(z, count), pl.ds(0, (lefts - 1) * share_y), :], sem)
        field, spot = i // pieces, lax.rem(i, pieces) * DEPTH + z
        y_values(first.at[i, pl.ds(z, count)], send_b.at[field], spot, count)
        hosted = jnp.logical_and(gate, jnp.logical_and(i == 0, z == guest_z))
        direct = jnp.logical_or(end, jnp.logical_and(field < fields - 1, jnp.logical_not(hosted)))
        for k in range(half):
            @pl.when(direct)
            def _():
                copy_b(field, spot, count, crossing(k), 0).start()
        for k in range(half - 1):
            @pl.when(jnp.logical_not(field == fields - 1))
            def _():
                copy_b(field, spot, count, beside(k), 1).start()
        y_own(send_b.at[field], spot, field, right * share_z + spot, count)

    def guest_x():
        landed(raw_in, raw_sem.at[1])
        for c in range(size_x // LANES):
            cols = pl.ds(c * LANES, LANES)
            lines[0, pl.ds(0, SUB * share_y), cols], lines[1, pl.ds(0, SUB * share_y), cols] = split(raw_in[:, cols])

        def tile(j, carry):
            x_tile(guest_a, j, 0, SUB, False)
            return carry

        lax.fori_loop(0, lefts // 2, tile, 0)
        for k in range(lefts - 1, 0, -1):
            copy_guest_a(partner(k)).start()
        guest_first[:, pl.ds(pl.multiple_of(left * share_y, share_y), share_y), :] = guest_a[left]

    def guest_y():
        landed(guest_first.at[:, pl.ds(0, (lefts - 1) * share_y), :], guest_sem.at[1])
        y_values(guest_first, guest_b, 0, SUB)
        for k in range(half - 1):
            copy_guest_b(beside(k)).start()
        y_own(guest_b, 0, 0, twin * share_z + guest_z, SUB)

    fetch(1)
    tables[0].wait()
    x_open()
    tables[1].wait()
    tables[2].wait()
    for symbol in symbols:
        symbol.start()
    for z in range(SUB):
        y_step(0, z, 1, arrival(2 * z, 0))

    def step(i, carry):
        @pl.when(i + 1 < chunks)
        def _():
            x_step(i + 1)

        @pl.when(jnp.logical_and(gate, i == min(1, chunks - 1)))
        def _():
            guest_x()

        def part(sub, carry):
            y_step(i, sub * SUB, SUB, arrival(i, sub))
            return carry

        lax.fori_loop(1, subs, part, 0)

        @pl.when(jnp.logical_and(gate, i == min(2, chunks - 1)))
        def _():
            guest_y()

        @pl.when(i + 1 < chunks)
        def _():
            y_step(i + 1, 0, SUB, arrival(i + 1, 0))

        return carry

    lax.fori_loop(0, chunks, step, 0)

    for k in range(half - 1):
        copy_b(fields - 1, 0, share_z, beside(k), 1).start()

    @pl.when(jnp.logical_not(end))
    def _():
        for parts in (*((n,) for n in range(2 * bands - 2)), (2 * bands - 2, 2 * bands - 1)):
            for k in range(half - 1, -1, -1):
                for n in parts:
                    copy_c(n, crossing(k)).start()

    for symbol in symbols:
        symbol.wait()
    column = jnp.broadcast_to(sym_x[pl.ds(left, 1), :], (size_z, share_x)).T
    base[...] = column + sym_z[...]
    table[...] = hz[...]
    for y in range(SUBLANES):
        scale[y] = lax.rsqrt(base[...] + sym_y[right * out_y + out_y - SUBLANES + y])

    def held_in(band, part):
        block = second.at[fields - 1, band].reshape(size_z, BAND, share_x)
        rows = pl.ds(part % 2 * SUBLANES, SUBLANES)
        landed(block.at[pl.ds(0, (half - 1) * share_z), rows, :], rc_sem.at[part])

    def z_step(n, carry):
        field, part = n // (2 * bands), lax.rem(n, 2 * bands)
        band, top = part // 2, lax.rem(part, 2) * SUBLANES
        hosting = jnp.logical_and(gate, field == 0)
        everything = (rights - 1) * share_z
        for planes, chosen in (
            (everything - SUB, hosting),
            (everything, jnp.logical_and(field < fields - 1, jnp.logical_not(hosting))),
            (half * share_z, field == fields - 1),
        ):
            @pl.when(jnp.logical_and(part == 0, chosen))
            def _():
                landed(second.at[field, :, pl.ds(0, planes * BAND), :], rb_sem.at[field])

        @pl.when(field == fields - 1)
        def _():
            held_in(band, part)

        def line(step, carry):
            y = top + step
            plane = second[field, band, pl.ds(y, size_z, stride=BAND), :].T
            got = jnp.dot(jnp.concatenate(split(plane), axis=1), hz[...], preferred_element_type=jnp.float32)
            got = (got[:, :size_z] + got[:, size_z:]) * lax.rsqrt(base[...] + sym_y[right * out_y + band * BAND + y])
            out[field, band, pl.ds(y, share_x, stride=BAND), :] = got
            return carry

        lax.fori_loop(0, SUBLANES, line, 0, unroll=4)
        return carry

    lax.fori_loop(0, fields * bands * 2 - 1, z_step, 0)
    held_in(bands - 1, 2 * bands - 1)
    block = second.at[fields - 1, bands - 1].reshape(size_z, BAND, share_x)
    tail[...] = block[:, BAND - SUBLANES:, :].reshape(size_z * SUBLANES, share_x)
    landed(send_a.at[:, pl.ds(0, lefts - 1)], sa_sem)
    landed(send_b.at[0, pl.ds(0, half - 1)], sb_sem.at[1])
    landed(send_b.at[pl.ds(1, fields - 1), pl.ds(0, rights - 1)], sb_sem.at[2])

    @pl.when(gate)
    def _():
        landed(send_b.at[0, pl.ds(0, half), :, pl.ds(0, (share_z - SUB) * BAND), :], sb_sem.at[0])
        landed(raw_out, raw_sem.at[0])
        landed(guest_a.at[pl.ds(0, lefts - 1)], guest_sem.at[0])
        landed(guest_b.at[pl.ds(0, half - 1)], guest_sem.at[2])

    @pl.when(jnp.logical_not(gate))
    def _():
        landed(send_b.at[0, pl.ds(0, half)], sb_sem.at[0])


def flush_kernel(ready, tail, scale, table, out, made, sem):
    fields, bands, share_x, _, size_z = ready.shape
    for n in range(fields * bands):
        field, band = n // bands, n % bands
        rows = BAND if n < fields * bands - 1 else BAND - SUBLANES
        there = out.at[field, :, pl.ds(band * BAND, rows), :]
        pltpu.make_async_copy(ready.at[field, band, :, pl.ds(0, rows), :], there, sem).start()
    for y in range(SUBLANES):
        plane = tail[pl.ds(y, size_z, stride=SUBLANES), :].T
        got = jnp.dot(jnp.concatenate(split(plane), axis=1), table[...], preferred_element_type=jnp.float32)
        made[pl.ds(y, share_x, stride=SUBLANES), :] = (got[:, :size_z] + got[:, size_z:]) * scale[y]
    there = out.at[fields - 1, :, pl.ds(bands * BAND - SUBLANES, SUBLANES), :]
    pltpu.make_async_copy(made.reshape(share_x, SUBLANES, size_z), there, sem).start()
    landed(out, sem)


def near_local(lefts, rights, tracer, symbol_x, symbol_y, symbol_z):
    fields, size_x, share_y, share_z = tracer.shape
    size_y, size_z = symbol_y.shape[0], symbol_z.shape[0]
    share_x, out_y = size_x // lefts, size_y // rights
    bands = out_y // BAND
    chunks = fields * (share_z // DEPTH)
    data = jnp.transpose(tracer, (0, 2, 3, 1))
    factors, inner = factors_of(size_x)
    hy, hz = small_table(size_y), stacked(small_table(size_z))
    f32, bf16 = jnp.float32, jnp.bfloat16
    any_space = pl.BlockSpec(memory_space=pl.ANY)
    vmem = pl.BlockSpec(memory_space=pltpu.VMEM)
    dma = pltpu.SemaphoreType.DMA
    ready, *others = pl.pallas_call(
        functools.partial(near_kernel, lefts, rights, inner),
        name="modes",
        out_shape=[
            pltpu.VMEM((fields, bands, share_x * BAND, size_z), f32),
            pltpu.VMEM((size_z * SUBLANES, share_x), f32),
            pltpu.VMEM((SUBLANES, share_x, size_z), f32),
            pltpu.VMEM(hz.shape, bf16),
        ],
        in_specs=[any_space] * 7,
        out_specs=[vmem] * 4,
        scratch_shapes=[
            pltpu.VMEM((chunks, DEPTH, size_y, share_x), f32),
            pltpu.VMEM((fields, bands, size_z * BAND, share_x), f32),
            pltpu.VMEM((2, size_x // LANES, share_y * DEPTH, LANES), f32),
            pltpu.VMEM(factors.shape, f32),
            pltpu.VMEM((2, size_x, size_x), bf16),
            pltpu.VMEM(hy.shape, bf16),
            pltpu.VMEM(hz.shape, bf16),
            pltpu.VMEM((2, share_y * DEPTH, size_x), bf16),
            pltpu.VMEM((chunks, lefts, DEPTH, share_y, share_x), f32),
            pltpu.VMEM((fields, rights, bands, share_z * BAND, share_x), f32),
            pltpu.VMEM((share_x, size_z), f32),
            pltpu.VMEM((lefts, share_x), f32),
            pltpu.VMEM((1, size_z), f32),
            pltpu.SMEM((size_y,), f32),
            pltpu.VMEM((SUB * share_y, size_x), f32),
            pltpu.VMEM((SUB * share_y, size_x), f32),
            pltpu.VMEM((lefts, SUB, share_y, share_x), f32),
            pltpu.VMEM((SUB, size_y, share_x), f32),
            pltpu.VMEM((rights, bands, SUB * BAND, share_x), f32),
            dma((2,)),
            dma((3,)),
            dma,
            dma((SLOTS, DEPTH // SUB)),
            dma((3,)),
            dma((fields,)),
            dma((2 * bands,)),
            dma((2,)),
            dma((3,)),
        ],
        compiler_params=pltpu.CompilerParams(
            collective_id=0, has_side_effects=True, vmem_limit_bytes=NEAR_LIMIT
        ),
    )(data, factors, hy, hz, symbol_x.reshape(lefts, share_x), symbol_z.reshape(1, size_z), symbol_y)
    return pl.pallas_call(
        flush_kernel,
        name="flush",
        out_shape=jax.ShapeDtypeStruct((fields, share_x, out_y, size_z), f32),
        in_specs=[vmem] * 4,
        out_specs=any_space,
        scratch_shapes=[pltpu.VMEM((share_x * SUBLANES, size_z), f32), dma],
        compiler_params=pltpu.CompilerParams(vmem_limit_bytes=2**21),
    )(ready.reshape(fields, bands, share_x, BAND, size_z), *others)


def far_local(lefts, rights, tracer, symbol_x, symbol_y, symbol_z):
    fields, size_x, share_y, share_z = tracer.shape
    size_y, size_z = symbol_y.shape[0], symbol_z.shape[0]
    share_x, out_y = size_x // lefts, size_y // rights
    bands = out_y // BAND
    chunks = fields * (share_z // DEPTH)
    data = jnp.transpose(tracer, (0, 2, 3, 1))
    part_x = lax.dynamic_slice_in_dim(symbol_x, lax.axis_index("left") * share_x, share_x)
    base = part_x[:, None] + symbol_z[None, :]
    f32 = jnp.float32
    any_space = pl.BlockSpec(memory_space=pl.ANY)
    vmem = pl.BlockSpec(memory_space=pltpu.VMEM)
    landing = [(chunks, size_y * DEPTH, share_x), (fields, bands, size_z * BAND, share_x)]
    near = 4 * sum(map(math.prod, landing)) <= NEAR_BYTES
    staging = [] if near else [
        pltpu.VMEM((size_y * DEPTH, share_x), f32), pltpu.VMEM((size_z * BAND, share_x), f32)
    ]
    results = pl.pallas_call(
        functools.partial(far_kernel, lefts, rights, near),
        name="modes",
        out_shape=[
            jax.ShapeDtypeStruct((fields, bands, size_z // LANES, share_x * BAND, LANES), f32),
            *([] if near else [jax.ShapeDtypeStruct(shape, f32) for shape in landing]),
        ],
        in_specs=[any_space, vmem, vmem, vmem, vmem, pl.BlockSpec(memory_space=pltpu.SMEM)],
        out_specs=[any_space] * (1 if near else 3),
        scratch_shapes=[
            *([pltpu.VMEM(shape, f32) for shape in landing] if near else []),
            pltpu.VMEM((2, share_y, DEPTH, size_x), f32),
            pltpu.VMEM((2, share_y * DEPTH, size_x), jnp.bfloat16),
            pltpu.VMEM((SLOTS, lefts, share_y * DEPTH, share_x), f32),
            pltpu.VMEM((chunks, rights, bands, DEPTH * BAND, share_x), f32),
            pltpu.VMEM((2, size_z // LANES, share_x * BAND, LANES), f32),
            pltpu.SemaphoreType.DMA((2,)),
            pltpu.SemaphoreType.DMA((SLOTS, lefts)),
            pltpu.SemaphoreType.DMA((chunks, lefts)),
            pltpu.SemaphoreType.DMA,
            pltpu.SemaphoreType.DMA((chunks, rights, bands)),
            pltpu.SemaphoreType.DMA((chunks, rights, bands)),
            pltpu.SemaphoreType.DMA,
            pltpu.SemaphoreType.DMA((2,)),
            *staging,
        ],
        compiler_params=pltpu.CompilerParams(
            collective_id=0, has_side_effects=True, vmem_limit_bytes=60 * 2**20
        ),
    )(data, halves_of(transform_table(size_x)), small_table(size_y), small_table(size_z), base, symbol_y)
    out = results[0].reshape(fields, bands, size_z // LANES, share_x, BAND, LANES)
    return jnp.transpose(out, (0, 3, 1, 4, 2, 5)).reshape(fields, share_x, out_y, size_z)


def local(lefts, rights, tracer, symbol_x, symbol_y, symbol_z):
    fields, size_x, share_y, share_z = tracer.shape
    size_z, share_x = symbol_z.shape[0], size_x // lefts
    size = 4 * math.prod(tracer.shape)
    fits = size <= NEAR_BYTES // 2 and share_x == LANES and size_z == LANES and rights % 2 == 0
    fits = fits and rights > 2 and fields > 1
    run = near_local if fits else far_local
    return run(lefts, rights, tracer, symbol_x, symbol_y, symbol_z)


def solution(mesh):
    return jax.shard_map(
        functools.partial(local, mesh.shape["left"], mesh.shape["right"]),
        mesh=mesh,
        in_specs=(P(None, None, "left", "right"), P(), P(), P()),
        out_specs=P(None, "left", "right", None),
        check_vma=False,
    )
```

```python
import functools
import math

import jax
import jax.numpy as jnp
import numpy as np
from jax import lax
from jax.experimental import pallas as pl
from jax.experimental.pallas import tpu as pltpu
from jax.sharding import PartitionSpec as P

MESH = pl.DeviceIdType.MESH
NEAR_BYTES = 20 * 2**20
DEPTH = 8
BAND = 16
SUBLANES = 8
LANES = 128
SLOTS = 3
NEAR_LIMIT = 50 * 2**20
SUB = 2


def transform_table(count):
    inner = 1 << ((count.bit_length() - 1) // 2)
    outer = count // inner
    column = np.arange(count)

    def angle(row):
        return 2.0 * np.pi / count * (row[:, None] * column[None, :] % count)

    low = angle(np.arange(inner))
    high = angle(np.arange(outer) * inner)
    scale = count ** (-0.5)
    cos_low = jnp.asarray(np.cos(low), jnp.float32)[None]
    sin_low = jnp.asarray(np.sin(low), jnp.float32)[None]
    plus = jnp.asarray((np.cos(high) + np.sin(high)) * scale, jnp.float32)[:, None]
    minus = jnp.asarray((np.cos(high) - np.sin(high)) * scale, jnp.float32)[:, None]
    return (cos_low * plus + sin_low * minus).reshape(count, count)


def factors_of(count):
    inner = 1 << ((count.bit_length() - 1) // 2)
    outer = count // inner
    column = np.arange(count)

    def angle(row):
        return 2.0 * np.pi / count * (row[:, None] * column[None, :] % count)

    low = angle(np.arange(inner))
    high = angle(np.arange(outer) * inner)
    scale = count ** (-0.5)
    low = np.stack([np.cos(low), np.sin(low)])
    high = np.stack([np.cos(high) + np.sin(high), np.cos(high) - np.sin(high)]) * scale
    rows = max(inner, outer)
    padded = [np.pad(part, ((0, 0), (0, rows - part.shape[1]), (0, 0))) for part in (low, high)]
    return jnp.asarray(np.concatenate(padded), jnp.float32), inner


def halves_of(table):
    upper = lax.reduce_precision(table, 8, 7)
    return jnp.stack([upper.astype(jnp.bfloat16), (table - upper).astype(jnp.bfloat16)])


def small_table(count):
    rank = np.arange(count)
    angle = 2.0 * np.pi / count * (rank[:, None] * rank[None, :] % count)
    table = ((np.cos(angle) + np.sin(angle)) * count ** (-0.5)).astype(np.float32)
    upper = table.astype(jnp.bfloat16)
    return jnp.asarray(np.stack([upper, (table - upper.astype(np.float32)).astype(jnp.bfloat16)]))


def split(values):
    upper = values.astype(jnp.bfloat16)
    return upper, (values - upper.astype(jnp.float32)).astype(jnp.bfloat16)


def product(a, b):
    dot = functools.partial(jnp.dot, preferred_element_type=jnp.float32)
    return dot(a[0], b[0]) + (dot(a[0], b[1]) + dot(a[1], b[0]))


def landed(ref, sem):
    pltpu.make_async_copy(ref, ref, sem).wait()


def far_kernel(lefts, rights, near, data, hx, hy, hz, base, sym_y, out, *rest):
    (first, second, dbuf, lines, send_a, send_b, obuf,
     d_sem, sa_sem, ra_sem, y_sem, sb_sem, rb_sem, z_sem, o_sem, *staging) = rest
    fields, share_y, share_z, _ = data.shape
    size_y, size_z = hy.shape[1], hz.shape[1]
    share_x = base.shape[0]
    bands = out.shape[1]
    pieces = share_z // DEPTH
    chunks = fields * pieces
    rows = share_y * DEPTH
    flat = DEPTH * BAND
    out_y = bands * BAND
    left, right = lax.axis_index("left"), lax.axis_index("right")

    def load(i):
        source = data.at[i // pieces, :, pl.ds(lax.rem(i, pieces) * DEPTH, DEPTH), :]
        return pltpu.make_async_copy(source, dbuf.at[lax.rem(i, 2)], d_sem.at[lax.rem(i, 2)])

    load(0).start()

    barrier = pltpu.get_barrier_semaphore()
    for k in range(1, lefts):
        pl.semaphore_signal(barrier, inc=1, device_id=(lax.rem(left + k, lefts), right), device_id_type=MESH)
    for k in range(1, rights):
        pl.semaphore_signal(barrier, inc=1, device_id=(left, lax.rem(right + k, rights)), device_id_type=MESH)
    pl.semaphore_wait(barrier, lefts + rights - 2)

    def copy_a(i, to):
        slot = lax.rem(i, SLOTS)
        return pltpu.make_async_remote_copy(
            src_ref=send_a.at[slot, to],
            dst_ref=first.at[i, pl.ds(left * rows, rows)],
            send_sem=sa_sem.at[slot, to],
            recv_sem=ra_sem.at[i, left],
            device_id=(to, right),
            device_id_type=MESH,
        )

    def copy_b(i, to, band):
        spot = right * share_z + lax.rem(i, pieces) * DEPTH
        return pltpu.make_async_remote_copy(
            src_ref=send_b.at[i, to, band],
            dst_ref=second.at[i // pieces, band, pl.ds(spot * BAND, flat)],
            send_sem=sb_sem.at[i, to, band],
            recv_sem=rb_sem.at[i, right, band],
            device_id=(left, to),
            device_id_type=MESH,
        )

    def sent_a(i):
        for k in range(1, lefts):
            copy_a(i, lax.rem(left + k, lefts)).wait_send()

    def x_step(i):
        load(i).wait()

        @pl.when(i + 1 < chunks)
        def _():
            load(i + 1).start()

        @pl.when(i >= SLOTS)
        def _():
            sent_a(i - SLOTS)

        slot = lax.rem(i, SLOTS)
        lines[0], lines[1] = split(dbuf[lax.rem(i, 2)].reshape(rows, hx.shape[1]))

        def tile(j, carry):
            cols = pl.ds(pl.multiple_of(j * 2 * share_x, 2 * share_x), 2 * share_x)
            got = product((lines[0], lines[1]), (hx[0, :, cols], hx[1, :, cols]))
            send_a[slot, 2 * j] = got[:, :share_x]
            send_a[slot, 2 * j + 1] = got[:, share_x:]
            return carry

        lax.fori_loop(0, lefts // 2, tile, 0)
        for k in range(1, lefts):
            copy_a(i, lax.rem(left + k, lefts)).start()
        pltpu.make_async_copy(
            send_a.at[slot, left], first.at[i, pl.ds(left * rows, rows)], ra_sem.at[i, left]
        ).start()

    def y_step(i):
        for k in range(lefts):
            landed(first.at[i, pl.ds(k * rows, rows)], ra_sem.at[i, k])
        if near:
            block = first.at[i]
        else:
            block = staging[0]
            fetch = pltpu.make_async_copy(first.at[i], block, y_sem)
            fetch.start()
            fetch.wait()
        for z in range(0, DEPTH, 2):
            pair = jnp.concatenate(
                [block[pl.ds(z, size_y, stride=DEPTH), :], block[pl.ds(z + 1, size_y, stride=DEPTH), :]], axis=1
            )
            got = product((hy[0], hy[1]), split(pair))
            for to in range(rights):
                for band in range(bands):
                    top = to * out_y + band * BAND
                    for half in range(2):
                        send_b[i, to, band, (z + half) * BAND:(z + half + 1) * BAND, :] = (
                            got[top:top + BAND, half * share_x:(half + 1) * share_x]
                        )
        for band in range(bands):
            for k in range(rights):
                to = jnp.where(right < rights // 2, rights - 1 - k, k)

                @pl.when(to != right)
                def _():
                    copy_b(i, to, band).start()

            spot = right * share_z + lax.rem(i, pieces) * DEPTH
            pltpu.make_async_copy(
                send_b.at[i, right, band],
                second.at[i // pieces, band, pl.ds(spot * BAND, flat)],
                rb_sem.at[i, right, band],
            ).start()

    def step(i, carry):
        @pl.when(i < chunks)
        def _():
            x_step(i)

        @pl.when(i >= 1)
        def _():
            y_step(i - 1)

        return carry

    lax.fori_loop(0, chunks + 1, step, 0)

    def put(n):
        slot = lax.rem(n, 2)
        return pltpu.make_async_copy(obuf.at[slot], out.at[n // bands, lax.rem(n, bands)], o_sem.at[slot])

    def z_step(n, carry):
        field, band = n // bands, lax.rem(n, bands)
        slot = lax.rem(n, 2)

        def arrive(p, carry):
            for k in range(rights):
                spot = k * share_z + p * DEPTH
                landed(second.at[field, band, pl.ds(spot * BAND, flat)], rb_sem.at[field * pieces + p, k, band])
            return carry

        lax.fori_loop(0, pieces, arrive, 0)
        if near:
            block = second.at[field, band]
        else:
            block = staging[1]
            fetch = pltpu.make_async_copy(second.at[field, band], block, z_sem)
            fetch.start()
            fetch.wait()

        @pl.when(n >= 2)
        def _():
            put(n - 2).wait()

        def line(y, carry):
            plane = block[pl.ds(y, size_z, stride=BAND), :].T
            got = product(split(plane), (hz[0], hz[1]))
            got = got * lax.rsqrt(base[...] + sym_y[right * out_y + band * BAND + y])
            for t in range(size_z // LANES):
                obuf[slot, t, pl.ds(y, share_x, stride=BAND), :] = got[:, t * LANES:(t + 1) * LANES]
            return carry

        lax.fori_loop(0, BAND, line, 0, unroll=2)
        put(n).start()
        return carry

    steps = fields * bands
    lax.fori_loop(0, steps, z_step, 0)

    def drain_a(i, carry):
        sent_a(i)
        return carry

    lax.fori_loop(max(chunks - SLOTS, 0), chunks, drain_a, 0)

    def drain_b(i, carry):
        for k in range(1, rights):
            for band in range(bands):
                copy_b(i, lax.rem(right + k, rights), band).wait_send()
        return carry

    lax.fori_loop(0, chunks, drain_b, 0)
    for n in range(max(steps - 2, 0), steps):
        put(n).wait()


def stacked(halves):
    upper, lower = halves[0], halves[1]
    return jnp.concatenate(
        [jnp.concatenate([upper, lower], axis=1), jnp.concatenate([upper, jnp.zeros_like(lower)], axis=1)], axis=0
    )


def near_kernel(lefts, rights, inner, data, factors_in, hy_in, hz_in, x_in, z_in, y_in, out, tail, scale, table, *rest):
    (first, second, dbuf, factors, hx, hy, hz, lines, send_a, send_b, base,
     sym_x, sym_z, sym_y, raw_out, raw_in, guest_a, guest_first, guest_b,
     d_sem, t_sem, sa_sem, ra_sem, sb_sem, rb_sem, rc_sem, raw_sem, guest_sem) = rest
    fields, share_y, share_z, size_x = data.shape
    size_y = hy.shape[1]
    share_x, size_z = base.shape
    bands = out.shape[1]
    pieces = share_z // DEPTH
    chunks = fields * pieces
    subs = DEPTH // SUB
    out_y = bands * BAND
    half = rights // 2
    left, right = lax.axis_index("left"), lax.axis_index("right")

    def load(i):
        slot = lax.rem(i, 2)
        planes = pl.ds(lax.rem(i, pieces) * DEPTH, DEPTH)
        return [pltpu.make_async_copy(
            data.at[i // pieces, :, planes, pl.ds(c * LANES, LANES)],
            dbuf.at[slot, c].reshape(share_y, DEPTH, LANES),
            d_sem.at[slot],
        ) for c in range(size_x // LANES)]

    def fetch(i):
        for copy in load(i):
            copy.start()

    def copies(pairs):
        return [pltpu.make_async_copy(a, b, t_sem.at[n]) for n, (a, b) in enumerate(pairs)]

    tables = copies([(factors_in, factors), (hy_in, hy), (hz_in, hz)])
    symbols = copies([(x_in, sym_x), (z_in, sym_z), (y_in, sym_y)])
    barrier = pltpu.get_barrier_semaphore()
    for k in range(1, lefts):
        pl.semaphore_signal(barrier, inc=1, device_id=(lax.rem(left + k, lefts), right), device_id_type=MESH)
    for k in range(1, rights):
        pl.semaphore_signal(barrier, inc=1, device_id=(left, lax.rem(right + k, rights)), device_id_type=MESH)

    tables[0].start()
    fetch(0)
    tables[1].start()
    tables[2].start()

    def copy_a(i, z, count, to, sem):
        return pltpu.make_async_remote_copy(
            src_ref=send_a.at[i, to, pl.ds(z, count)],
            dst_ref=first.at[i, pl.ds(z, count), pl.ds(left * share_y, share_y), :],
            send_sem=sa_sem,
            recv_sem=sem,
            device_id=(to, right),
            device_id_type=MESH,
        )

    def copy_b(field, spot, count, to, kind):
        return pltpu.make_async_remote_copy(
            src_ref=send_b.at[field, to, :, pl.ds(spot * BAND, count * BAND), :],
            dst_ref=second.at[field, :, pl.ds((right * share_z + spot) * BAND, count * BAND), :],
            send_sem=sb_sem.at[jnp.where(field == 0, kind, 2)],
            recv_sem=rb_sem.at[field],
            device_id=(left, to),
            device_id_type=MESH,
        )

    def copy_c(n, to):
        band, rows = n // 2, pl.ds(n % 2 * SUBLANES, SUBLANES)
        there = second.at[fields - 1, band].reshape(size_z, BAND, share_x)
        return pltpu.make_async_remote_copy(
            src_ref=send_b.at[fields - 1, to, band].reshape(share_z, BAND, share_x).at[:, rows, :],
            dst_ref=there.at[pl.ds(right * share_z, share_z), rows, :],
            send_sem=sb_sem.at[2],
            recv_sem=rc_sem.at[n],
            device_id=(left, to),
            device_id_type=MESH,
        )

    lower = right < half
    rank = jnp.where(lower, right, rights - 1 - right)
    end = rank == 0
    gate = rank == half - 1
    twin = rights - 1 - right
    guest_z = DEPTH - SUB

    def mirrored(t):
        return jnp.where(lower, t, rights - 1 - t)

    def crossing(k):
        return mirrored(jnp.where(end, rights - 1 - k, half + k))

    def beside(k):
        return mirrored(lax.rem(rank + 1 + k, half))

    def raw():
        return pltpu.make_async_remote_copy(
            src_ref=raw_out,
            dst_ref=raw_in,
            send_sem=raw_sem.at[0],
            recv_sem=raw_sem.at[1],
            device_id=(left, twin),
            device_id_type=MESH,
        )

    def copy_guest_a(to):
        return pltpu.make_async_remote_copy(
            src_ref=guest_a.at[to],
            dst_ref=guest_first.at[:, pl.ds(left * share_y, share_y), :],
            send_sem=guest_sem.at[0],
            recv_sem=guest_sem.at[1],
            device_id=(to, right),
            device_id_type=MESH,
        )

    def copy_guest_b(to):
        spot = (twin * share_z + guest_z) * BAND
        return pltpu.make_async_remote_copy(
            src_ref=guest_b.at[to],
            dst_ref=second.at[0, :, pl.ds(spot, SUB * BAND), :],
            send_sem=guest_sem.at[2],
            recv_sem=rb_sem.at[0],
            device_id=(left, to),
            device_id_type=MESH,
        )

    def widen(cols):
        for top in range(size_x // inner):
            plus, minus = factors[2, top:top + 1, cols], factors[3, top:top + 1, cols]
            made = factors[0, :inner, cols] * plus + factors[1, :inner, cols] * minus
            rows = pl.ds(top * inner, inner)
            hx[0, rows, cols], hx[1, rows, cols] = split(made)

    def arrival(i, sub):
        return ra_sem.at[lax.rem(i, SLOTS), sub]

    def partner(k):
        return left ^ k if lefts & (lefts - 1) == 0 else lax.rem(left + k, lefts)

    def x_tile(sends, j, z, count, opening):
        pair = partner(lefts - 1 - 2 * j) // 2
        cols = pl.ds(pl.multiple_of(pair * 2 * share_x, 2 * share_x), 2 * share_x)
        if opening:
            widen(cols)
        rows = pl.ds(z * share_y, count * share_y)
        got = product((lines[0, rows, :], lines[1, rows, :]), (hx[0, :, cols], hx[1, :, cols]))
        for core in range(2):
            part = got[:, core * share_x:(core + 1) * share_x].reshape(count, share_y, share_x)
            sends[2 * pair + core, z:z + count] = part
        return pair

    def x_split(i, planes):
        slot = lax.rem(i, 2)
        for c in range(size_x // LANES):
            cols = pl.ds(c * LANES, LANES)
            for z in planes:
                rows = pl.ds(z * share_y, share_y)
                lines[0, rows, cols], lines[1, rows, cols] = split(dbuf[slot, c, pl.ds(z, share_y, stride=DEPTH), :])

    def x_send(i, z, count, pair, sem):
        for core in range(2):
            @pl.when(2 * pair + core != left)
            def _():
                copy_a(i, z, count, 2 * pair + core, sem).start()

    def x_rest(i, subs_left):
        for sub in subs_left:
            for k in range(lefts - 1, 0, -1):
                copy_a(i, sub * SUB, SUB, partner(k), arrival(i, sub)).start()

    def x_own(i, z, count):
        mine = pl.ds(pl.multiple_of(left * share_y, share_y), share_y)
        first[i, z:z + count, mine, :] = send_a[i, left, z:z + count]

    def x_open():
        landed(dbuf.at[0], d_sem.at[0])
        for c in range(size_x // LANES):
            for z in range(SUB):
                line = dbuf[0, c, pl.ds(guest_z + z, share_y, stride=DEPTH), :]
                raw_out[z * share_y:(z + 1) * share_y, c * LANES:(c + 1) * LANES] = line
        x_split(0, range(SUB))
        pl.semaphore_wait(barrier, lefts + rights - 2)

        @pl.when(gate)
        def _():
            raw().start()

        pair = x_tile(send_a.at[0], 0, 0, SUB, True)
        x_send(0, 0, 1, pair, arrival(0, 0))

        def tile(j, carry):
            x_send(0, 0, 1, x_tile(send_a.at[0], j, 0, SUB, True), arrival(0, 0))
            return carry

        lax.fori_loop(1, lefts // 2, tile, 0)
        for z in range(1, SUB):
            for k in range(lefts - 1, 0, -1):
                copy_a(0, z, 1, partner(k), arrival(2 * z, 0)).start()
        x_own(0, 0, SUB)
        x_split(0, range(SUB, DEPTH))

        def more(j, carry):
            x_send(0, SUB, SUB, x_tile(send_a.at[0], j, SUB, DEPTH - SUB, False), arrival(0, 1))
            return carry

        lax.fori_loop(0, lefts // 2, more, 0)
        x_rest(0, range(2, subs))
        x_own(0, SUB, DEPTH - SUB)
        fetch(2)

    def x_step(i):
        slot = lax.rem(i, 2)
        landed(dbuf.at[slot], d_sem.at[slot])
        x_split(i, range(DEPTH))

        @pl.when(i + 2 < chunks)
        def _():
            fetch(i + 2)

        def tile(j, carry):
            x_send(i, 0, SUB, x_tile(send_a.at[i], j, 0, DEPTH, False), arrival(i, 0))
            return carry

        lax.fori_loop(0, lefts // 2, tile, 0)
        x_rest(i, range(1, subs))
        x_own(i, 0, DEPTH)

    def y_values(ready, sends, spot, count):
        got = product((hy[0], hy[1]), split(jnp.concatenate([ready[n] for n in range(count)], axis=1)))
        for to in range(rights):
            for band in range(bands):
                top = to * out_y + band * BAND
                for n in range(count):
                    rows = pl.ds(pl.multiple_of((spot + n) * BAND, BAND), BAND)
                    sends[to, band, rows, :] = got[top:top + BAND, n * share_x:(n + 1) * share_x]

    def y_own(sends, spot, field, there, count):
        for band in range(bands):
            mine = sends[right, band, pl.ds(pl.multiple_of(spot * BAND, BAND), count * BAND), :]
            second[field, band, pl.ds(pl.multiple_of(there * BAND, BAND), count * BAND), :] = mine

    def y_step(i, z, count, sem):
        landed(first.at[i, pl.ds(z, count), pl.ds(0, (lefts - 1) * share_y), :], sem)
        field, spot = i // pieces, lax.rem(i, pieces) * DEPTH + z
        y_values(first.at[i, pl.ds(z, count)], send_b.at[field], spot, count)
        hosted = jnp.logical_and(gate, jnp.logical_and(i == 0, z == guest_z))
        direct = jnp.logical_or(end, jnp.logical_and(field < fields - 1, jnp.logical_not(hosted)))
        for k in range(half):
            @pl.when(direct)
            def _():
                copy_b(field, spot, count, crossing(k), 0).start()
        for k in range(half - 1):
            @pl.when(jnp.logical_not(field == fields - 1))
            def _():
                copy_b(field, spot, count, beside(k), 1).start()
        y_own(send_b.at[field], spot, field, right * share_z + spot, count)

    def guest_x():
        landed(raw_in, raw_sem.at[1])
        for c in range(size_x // LANES):
            cols = pl.ds(c * LANES, LANES)
            lines[0, pl.ds(0, SUB * share_y), cols], lines[1, pl.ds(0, SUB * share_y), cols] = split(raw_in[:, cols])

        def tile(j, carry):
            x_tile(guest_a, j, 0, SUB, False)
            return carry

        lax.fori_loop(0, lefts // 2, tile, 0)
        for k in range(lefts - 1, 0, -1):
            copy_guest_a(partner(k)).start()
        guest_first[:, pl.ds(pl.multiple_of(left * share_y, share_y), share_y), :] = guest_a[left]

    def guest_y():
        landed(guest_first.at[:, pl.ds(0, (lefts - 1) * share_y), :], guest_sem.at[1])
        y_values(guest_first, guest_b, 0, SUB)
        for k in range(half - 1):
            copy_guest_b(beside(k)).start()
        y_own(guest_b, 0, 0, twin * share_z + guest_z, SUB)

    fetch(1)
    tables[0].wait()
    x_open()
    tables[1].wait()
    tables[2].wait()
    for symbol in symbols:
        symbol.start()
    for z in range(SUB):
        y_step(0, z, 1, arrival(2 * z, 0))
    y_step(0, SUB, SUB, arrival(0, 1))

    def step(i, carry):
        @pl.when(i + 1 < chunks)
        def _():
            x_step(i + 1)

        @pl.when(jnp.logical_and(gate, i == min(1, chunks - 1)))
        def _():
            guest_x()

        def part(sub, carry):
            y_step(i, sub * SUB, SUB, arrival(i, sub))
            return carry

        lax.fori_loop(jnp.where(i == 0, 2, 1), subs, part, 0)

        @pl.when(jnp.logical_and(gate, i == min(2, chunks - 1)))
        def _():
            guest_y()

        @pl.when(i + 1 < chunks)
        def _():
            y_step(i + 1, 0, SUB, arrival(i + 1, 0))

        return carry

    lax.fori_loop(0, chunks, step, 0)

    for k in range(half - 1):
        copy_b(fields - 1, 0, share_z, beside(k), 1).start()

    @pl.when(jnp.logical_not(end))
    def _():
        for parts in (*((n,) for n in range(2 * bands - 2)), (2 * bands - 2, 2 * bands - 1)):
            for k in range(half - 1, -1, -1):
                for n in parts:
                    copy_c(n, crossing(k)).start()

    for symbol in symbols:
        symbol.wait()
    column = jnp.broadcast_to(sym_x[pl.ds(left, 1), :], (size_z, share_x)).T
    base[...] = column + sym_z[...]
    table[...] = hz[...]
    for y in range(SUBLANES):
        scale[y] = lax.rsqrt(base[...] + sym_y[right * out_y + out_y - SUBLANES + y])

    def held_in(band, part):
        block = second.at[fields - 1, band].reshape(size_z, BAND, share_x)
        rows = pl.ds(part % 2 * SUBLANES, SUBLANES)
        landed(block.at[pl.ds(0, (half - 1) * share_z), rows, :], rc_sem.at[part])

    def z_step(n, carry):
        field, part = n // (2 * bands), lax.rem(n, 2 * bands)
        band, top = part // 2, lax.rem(part, 2) * SUBLANES
        hosting = jnp.logical_and(gate, field == 0)
        everything = (rights - 1) * share_z
        for planes, chosen in (
            (everything - SUB, hosting),
            (everything, jnp.logical_and(field < fields - 1, jnp.logical_not(hosting))),
            (half * share_z, field == fields - 1),
        ):
            @pl.when(jnp.logical_and(part == 0, chosen))
            def _():
                landed(second.at[field, :, pl.ds(0, planes * BAND), :], rb_sem.at[field])

        @pl.when(field == fields - 1)
        def _():
            held_in(band, part)

        def line(step, carry):
            y = top + step
            plane = second[field, band, pl.ds(y, size_z, stride=BAND), :].T
            got = jnp.dot(jnp.concatenate(split(plane), axis=1), hz[...], preferred_element_type=jnp.float32)
            got = (got[:, :size_z] + got[:, size_z:]) * lax.rsqrt(base[...] + sym_y[right * out_y + band * BAND + y])
            out[field, band, pl.ds(y, share_x, stride=BAND), :] = got
            return carry

        lax.fori_loop(0, SUBLANES, line, 0, unroll=4)
        return carry

    lax.fori_loop(0, fields * bands * 2 - 1, z_step, 0)
    held_in(bands - 1, 2 * bands - 1)
    block = second.at[fields - 1, bands - 1].reshape(size_z, BAND, share_x)
    tail[...] = block[:, BAND - SUBLANES:, :].reshape(size_z * SUBLANES, share_x)
    landed(send_a.at[:, pl.ds(0, lefts - 1)], sa_sem)
    landed(send_b.at[0, pl.ds(0, half - 1)], sb_sem.at[1])
    landed(send_b.at[pl.ds(1, fields - 1), pl.ds(0, rights - 1)], sb_sem.at[2])

    @pl.when(gate)
    def _():
        landed(send_b.at[0, pl.ds(0, half), :, pl.ds(0, (share_z - SUB) * BAND), :], sb_sem.at[0])
        landed(raw_out, raw_sem.at[0])
        landed(guest_a.at[pl.ds(0, lefts - 1)], guest_sem.at[0])
        landed(guest_b.at[pl.ds(0, half - 1)], guest_sem.at[2])

    @pl.when(jnp.logical_not(gate))
    def _():
        landed(send_b.at[0, pl.ds(0, half)], sb_sem.at[0])


def flush_kernel(ready, tail, scale, table, out, made, sem):
    fields, bands, share_x, _, size_z = ready.shape
    for n in range(fields * bands):
        field, band = n // bands, n % bands
        rows = BAND if n < fields * bands - 1 else BAND - SUBLANES
        there = out.at[field, :, pl.ds(band * BAND, rows), :]
        pltpu.make_async_copy(ready.at[field, band, :, pl.ds(0, rows), :], there, sem).start()
    for y in range(SUBLANES):
        plane = tail[pl.ds(y, size_z, stride=SUBLANES), :].T
        got = jnp.dot(jnp.concatenate(split(plane), axis=1), table[...], preferred_element_type=jnp.float32)
        made[pl.ds(y, share_x, stride=SUBLANES), :] = (got[:, :size_z] + got[:, size_z:]) * scale[y]
    there = out.at[fields - 1, :, pl.ds(bands * BAND - SUBLANES, SUBLANES), :]
    pltpu.make_async_copy(made.reshape(share_x, SUBLANES, size_z), there, sem).start()
    landed(out, sem)


def near_local(lefts, rights, tracer, symbol_x, symbol_y, symbol_z):
    fields, size_x, share_y, share_z = tracer.shape
    size_y, size_z = symbol_y.shape[0], symbol_z.shape[0]
    share_x, out_y = size_x // lefts, size_y // rights
    bands = out_y // BAND
    chunks = fields * (share_z // DEPTH)
    data = jnp.transpose(tracer, (0, 2, 3, 1))
    factors, inner = factors_of(size_x)
    hy, hz = small_table(size_y), stacked(small_table(size_z))
    f32, bf16 = jnp.float32, jnp.bfloat16
    any_space = pl.BlockSpec(memory_space=pl.ANY)
    vmem = pl.BlockSpec(memory_space=pltpu.VMEM)
    dma = pltpu.SemaphoreType.DMA
    ready, *others = pl.pallas_call(
        functools.partial(near_kernel, lefts, rights, inner),
        name="modes",
        out_shape=[
            pltpu.VMEM((fields, bands, share_x * BAND, size_z), f32),
            pltpu.VMEM((size_z * SUBLANES, share_x), f32),
            pltpu.VMEM((SUBLANES, share_x, size_z), f32),
            pltpu.VMEM(hz.shape, bf16),
        ],
        in_specs=[any_space] * 7,
        out_specs=[vmem] * 4,
        scratch_shapes=[
            pltpu.VMEM((chunks, DEPTH, size_y, share_x), f32),
            pltpu.VMEM((fields, bands, size_z * BAND, share_x), f32),
            pltpu.VMEM((2, size_x // LANES, share_y * DEPTH, LANES), f32),
            pltpu.VMEM(factors.shape, f32),
            pltpu.VMEM((2, size_x, size_x), bf16),
            pltpu.VMEM(hy.shape, bf16),
            pltpu.VMEM(hz.shape, bf16),
            pltpu.VMEM((2, share_y * DEPTH, size_x), bf16),
            pltpu.VMEM((chunks, lefts, DEPTH, share_y, share_x), f32),
            pltpu.VMEM((fields, rights, bands, share_z * BAND, share_x), f32),
            pltpu.VMEM((share_x, size_z), f32),
            pltpu.VMEM((lefts, share_x), f32),
            pltpu.VMEM((1, size_z), f32),
            pltpu.SMEM((size_y,), f32),
            pltpu.VMEM((SUB * share_y, size_x), f32),
            pltpu.VMEM((SUB * share_y, size_x), f32),
            pltpu.VMEM((lefts, SUB, share_y, share_x), f32),
            pltpu.VMEM((SUB, size_y, share_x), f32),
            pltpu.VMEM((rights, bands, SUB * BAND, share_x), f32),
            dma((2,)),
            dma((3,)),
            dma,
            dma((SLOTS, DEPTH // SUB)),
            dma((3,)),
            dma((fields,)),
            dma((2 * bands,)),
            dma((2,)),
            dma((3,)),
        ],
        compiler_params=pltpu.CompilerParams(
            collective_id=0, has_side_effects=True, vmem_limit_bytes=NEAR_LIMIT
        ),
    )(data, factors, hy, hz, symbol_x.reshape(lefts, share_x), symbol_z.reshape(1, size_z), symbol_y)
    return pl.pallas_call(
        flush_kernel,
        name="flush",
        out_shape=jax.ShapeDtypeStruct((fields, share_x, out_y, size_z), f32),
        in_specs=[vmem] * 4,
        out_specs=any_space,
        scratch_shapes=[pltpu.VMEM((share_x * SUBLANES, size_z), f32), dma],
        compiler_params=pltpu.CompilerParams(vmem_limit_bytes=2**21),
    )(ready.reshape(fields, bands, share_x, BAND, size_z), *others)


def far_local(lefts, rights, tracer, symbol_x, symbol_y, symbol_z):
    fields, size_x, share_y, share_z = tracer.shape
    size_y, size_z = symbol_y.shape[0], symbol_z.shape[0]
    share_x, out_y = size_x // lefts, size_y // rights
    bands = out_y // BAND
    chunks = fields * (share_z // DEPTH)
    data = jnp.transpose(tracer, (0, 2, 3, 1))
    part_x = lax.dynamic_slice_in_dim(symbol_x, lax.axis_index("left") * share_x, share_x)
    base = part_x[:, None] + symbol_z[None, :]
    f32 = jnp.float32
    any_space = pl.BlockSpec(memory_space=pl.ANY)
    vmem = pl.BlockSpec(memory_space=pltpu.VMEM)
    landing = [(chunks, size_y * DEPTH, share_x), (fields, bands, size_z * BAND, share_x)]
    near = 4 * sum(map(math.prod, landing)) <= NEAR_BYTES
    staging = [] if near else [
        pltpu.VMEM((size_y * DEPTH, share_x), f32), pltpu.VMEM((size_z * BAND, share_x), f32)
    ]
    results = pl.pallas_call(
        functools.partial(far_kernel, lefts, rights, near),
        name="modes",
        out_shape=[
            jax.ShapeDtypeStruct((fields, bands, size_z // LANES, share_x * BAND, LANES), f32),
            *([] if near else [jax.ShapeDtypeStruct(shape, f32) for shape in landing]),
        ],
        in_specs=[any_space, vmem, vmem, vmem, vmem, pl.BlockSpec(memory_space=pltpu.SMEM)],
        out_specs=[any_space] * (1 if near else 3),
        scratch_shapes=[
            *([pltpu.VMEM(shape, f32) for shape in landing] if near else []),
            pltpu.VMEM((2, share_y, DEPTH, size_x), f32),
            pltpu.VMEM((2, share_y * DEPTH, size_x), jnp.bfloat16),
            pltpu.VMEM((SLOTS, lefts, share_y * DEPTH, share_x), f32),
            pltpu.VMEM((chunks, rights, bands, DEPTH * BAND, share_x), f32),
            pltpu.VMEM((2, size_z // LANES, share_x * BAND, LANES), f32),
            pltpu.SemaphoreType.DMA((2,)),
            pltpu.SemaphoreType.DMA((SLOTS, lefts)),
            pltpu.SemaphoreType.DMA((chunks, lefts)),
            pltpu.SemaphoreType.DMA,
            pltpu.SemaphoreType.DMA((chunks, rights, bands)),
            pltpu.SemaphoreType.DMA((chunks, rights, bands)),
            pltpu.SemaphoreType.DMA,
            pltpu.SemaphoreType.DMA((2,)),
            *staging,
        ],
        compiler_params=pltpu.CompilerParams(
            collective_id=0, has_side_effects=True, vmem_limit_bytes=60 * 2**20
        ),
    )(data, halves_of(transform_table(size_x)), small_table(size_y), small_table(size_z), base, symbol_y)
    out = results[0].reshape(fields, bands, size_z // LANES, share_x, BAND, LANES)
    return jnp.transpose(out, (0, 3, 1, 4, 2, 5)).reshape(fields, share_x, out_y, size_z)


def local(lefts, rights, tracer, symbol_x, symbol_y, symbol_z):
    fields, size_x, share_y, share_z = tracer.shape
    size_z, share_x = symbol_z.shape[0], size_x // lefts
    size = 4 * math.prod(tracer.shape)
    fits = size <= NEAR_BYTES // 2 and share_x == LANES and size_z == LANES and rights % 2 == 0
    fits = fits and rights > 2 and fields > 1
    run = near_local if fits else far_local
    return run(lefts, rights, tracer, symbol_x, symbol_y, symbol_z)


def solution(mesh):
    return jax.shard_map(
        functools.partial(local, mesh.shape["left"], mesh.shape["right"]),
        mesh=mesh,
        in_specs=(P(None, None, "left", "right"), P(), P(), P()),
        out_specs=P(None, "left", "right", None),
        check_vma=False,
    )
```
